128 devices in a mesh: chord: 8 (over y_lo, z), span: 16 (over x, y_hi, core).
Axes of the slice: x: 4, y: 4 (y_hi: 2, y_lo: 2; y = y_hi * 2 + y_lo), z: 4, core: 2. Of those that a mesh axis runs over, the one named last changes fastest.
Arguments:
- state: float32 [5, 125, 32, 32, 128], P(None, None, 'chord', 'span'), may hold values from -10 to 10
Outputs:
- residual: float32 [5, 125, 32, 32, 128], P(None, None, 'chord', 'span')
- viscosity: float32 [125, 32, 32, 128], P(None, 'chord', 'span')
The draws below stay inside these ranges and needn't reach their ends.
All inputs are finite; a program needn't handle non-finite values.
Results may differ from the reference program's by a relative error of at most 0.0001.
Values sent between devices are 32-bit elements; how exact they have to be, the bound alone decides.
A program may use at most 128 MiB of HBM per device.

```python
import math
import jax
import jax.numpy as jnp
import numpy as np
from jax import lax

NVAR = 5
NPTS = 125
NORMAL_ELEMENTS = 128
CHORD_ELEMENTS = 32
SPAN_ELEMENTS = 32


def draw_state(key, part):
    element_lattice = (CHORD_ELEMENTS, SPAN_ELEMENTS, NORMAL_ELEMENTS)
    variable = jnp.arange(NVAR).reshape(NVAR, 1, 1, 1, 1)
    level_base = jax.random.normal(jax.random.fold_in(key, 1), (NVAR, 1) + element_lattice, jnp.float32)
    density_base = jax.random.uniform(jax.random.fold_in(key, 2), (NVAR, 1) + element_lattice, jnp.float32, 0.5, 1.5)
    base = jnp.where(variable == 0, density_base, level_base)
    log_amp = jax.random.uniform(jax.random.fold_in(key, 3), (NVAR, 1) + element_lattice, jnp.float32, math.log(0.001), math.log(1.0))
    noise = jax.random.normal(jax.random.fold_in(key, 4), (NVAR, NPTS) + element_lattice, jnp.float32)
    return jnp.clip(base + jnp.exp(log_amp) * noise, -10.0, 10.0)


def setup_inputs(seed: int = 0) -> dict:
    key_of = jax.random.split(jax.random.key(seed), 2)
    return {
        "state": draw_state(jax.random.fold_in(key_of[1], 71), 0),
    }


EPS_SCALE = 0.01
SENSOR_CENTRE = -3.0
SENSOR_WIDTH = 1.5
RATIO_FLOOR = 1e-06
ENERGY_EPS = 1e-06
GAUSS_NODES = [-0.906179845938664, -0.5384693101056831, 0.0, 0.5384693101056831, 0.906179845938664]
GAUSS_WEIGHTS = [0.2369268850561891, 0.4786286704993665, 0.5688888888888889, 0.4786286704993665, 0.2369268850561891]

def legendre_values(points):
    values = [np.ones(points.shape), np.array(points)]
    for order in range(1, 5):
        values.append(((2 * order + 1) * points * values[order] - order * values[order - 1]) / (order + 1))
    return values

def line_tables():
    line_nodes = np.array(GAUSS_NODES)
    quadrature_weights = np.array(GAUSS_WEIGHTS)
    barycentric = np.array([1.0 / np.prod([line_nodes[j] - line_nodes[k] for k in range(5) if k != j]) for j in range(5)])
    derivative = np.zeros((5, 5))
    for i in range(5):
        for j in range(5):
            if i != j:
                derivative[i, j] = barycentric[j] / barycentric[i] / (line_nodes[i] - line_nodes[j])
        derivative[i, i] = -np.sum(derivative[i])
    left_values = np.ones(5)
    right_values = np.ones(5)
    for j in range(5):
        for k in range(5):
            if k != j:
                left_values[j] *= (-1.0 - line_nodes[k]) / (line_nodes[j] - line_nodes[k])
                right_values[j] *= (1.0 - line_nodes[k]) / (line_nodes[j] - line_nodes[k])
    legendre = legendre_values(line_nodes)
    fourth_slope = 7.0 * legendre[3] + 3.0 * legendre[1]
    fifth_slope = 9.0 * legendre[4] + 5.0 * legendre[2] + legendre[0]
    left_corr = 0.5 * (fourth_slope - fifth_slope)
    right_corr = 0.5 * (fourth_slope + fifth_slope)
    modal = np.zeros((5, 5))
    for k in range(5):
        modal[k, :] = quadrature_weights * math.sqrt((2 * k + 1) / 2.0) * legendre[k]
    return (line_nodes, derivative, left_values, right_values, left_corr, right_corr, modal)

def along_axis(operator_matrix, axis):
    factors = [np.eye(5), np.eye(5), np.eye(5)]
    factors[axis] = operator_matrix
    return np.kron(np.kron(factors[0], factors[1]), factors[2])

def build_tables():
    line_nodes, derivative, left_values, right_values, left_corr, right_corr, modal = line_tables()
    operators = []
    for axis in range(3):
        group = (along_axis(derivative, axis), along_axis(left_values[None, :], axis), along_axis(right_values[None, :], axis), along_axis(left_corr[:, None], axis), along_axis(right_corr[:, None], axis))
        operators.append(tuple((jnp.asarray(entry, dtype=jnp.float32) for entry in group)))
    modal_3d = jnp.asarray(np.kron(np.kron(modal, modal), modal), dtype=jnp.float32)
    point_index = np.arange(125)
    high_np = np.where((point_index // 25 == 4) | (point_index // 5 % 5 == 4) | (point_index % 5 == 4), 1.0, 0.0)
    high_mask = jnp.asarray(high_np, dtype=jnp.float32)
    halves = [(1.0 - line_nodes) / 2.0, (1.0 + line_nodes) / 2.0]
    trilinear_np = np.zeros((125, 8))
    for corner in range(8):
        trilinear_np[:, corner] = np.kron(np.kron(halves[corner // 4], halves[corner // 2 % 2]), halves[corner % 2])
    trilinear = jnp.asarray(trilinear_np, dtype=jnp.float32)
    return (operators, modal_3d, high_mask, trilinear)

def single_points(operator_matrix, field):
    return jnp.einsum('qp,pxyz->qxyz', operator_matrix, field, precision=lax.Precision.HIGHEST)

def sensor_viscosity(density, modal_3d, high_mask):
    coeffs = single_points(modal_3d, density)
    energy = coeffs * coeffs
    high_part = lax.optimization_barrier(jnp.sum(energy * high_mask[:, None, None, None], axis=0))
    total = lax.optimization_barrier(jnp.sum(energy, axis=0)) + ENERGY_EPS
    level = jnp.log10(jnp.maximum(high_part / total, RATIO_FLOOR))
    ramp = jnp.clip((level - SENSOR_CENTRE) / SENSOR_WIDTH, -1.0, 1.0)
    return EPS_SCALE * 0.5 * (1.0 + jnp.sin(0.5 * math.pi * ramp))

def boundary_masks(length, dim, rank, is_first, is_last):
    shape = [1] * rank
    shape[dim] = length
    place = lax.broadcasted_iota(jnp.int32, tuple(shape), dim)
    lower_open = jnp.logical_or(place > 0, jnp.logical_not(is_first))
    upper_open = jnp.logical_or(place < length - 1, jnp.logical_not(is_last))
    return (lower_open.astype(jnp.float32), upper_open.astype(jnp.float32))

def variable_residual(field, viscosity, operators):
    total = jnp.zeros_like(field)
    for axis in range(3):
        derivative, to_left, to_right, lift_left, lift_right = operators[axis]
        dim = axis + 1
        closed = axis != 1
        lower_open, upper_open = boundary_masks(field.shape[dim], dim, 4, closed, closed)
        left_tr = single_points(to_left, field)
        right_tr = single_points(to_right, field)
        prev_right = jnp.roll(right_tr, 1, axis=dim)
        following_left = jnp.roll(left_tr, -1, axis=dim)
        gradient = single_points(derivative, field) + single_points(lift_left, 0.5 * (prev_right - left_tr) * lower_open) + single_points(lift_right, 0.5 * (following_left - right_tr) * upper_open)
        flux = viscosity * gradient
        flux_left = single_points(to_left, flux)
        flux_right = single_points(to_right, flux)
        flux_prev = jnp.roll(flux_right, 1, axis=dim)
        flux_next = jnp.roll(flux_left, -1, axis=dim)
        total = total + single_points(derivative, flux) + single_points(lift_left, 0.5 * (flux_prev + flux_left) * lower_open - flux_left) + single_points(lift_right, 0.5 * (flux_next + flux_right) * upper_open - flux_right)
    return total

def reference(state):
    operators, modal_3d, high_mask, trilinear = build_tables()
    element_eps = sensor_viscosity(state[0], modal_3d, high_mask)
    padded = jnp.pad(element_eps, ((1, 1), (0, 0), (1, 1)))
    along_chord = jnp.maximum(padded[:-1], padded[1:])
    along_span = jnp.maximum(along_chord, jnp.roll(along_chord, 1, axis=1))
    vertex = jnp.maximum(along_span[:, :, :-1], along_span[:, :, 1:])
    shifted = jnp.roll(vertex, -1, axis=1)
    chord_count = element_eps.shape[0]
    normal_count = element_eps.shape[2]
    corner_list = []
    for corner in range(8):
        step_x = corner // 4
        step_y = corner // 2 % 2
        step_z = corner % 2
        source = shifted if step_y == 1 else vertex
        corner_list.append(source[step_x:step_x + chord_count, :, step_z:step_z + normal_count])
    corners = jnp.stack(corner_list, axis=0)
    viscosity = jnp.einsum('qc,cxyz->qxyz', trilinear, corners, precision=lax.Precision.HIGHEST)

    def one_variable(field):
        return variable_residual(field, viscosity, operators)
    residual = lax.map(one_variable, state)
    return (residual, viscosity)
```

```python
import functools
import math

import jax
import jax.numpy as jnp
import numpy as np
from jax import lax
from jax.experimental import pallas as pl
from jax.experimental.pallas import tpu as pltpu
from jax.sharding import PartitionSpec as P

VMEM_BYTES = 52_500_000
EPS_SCALE = 0.01
SENSOR_CENTRE = -3.0
SENSOR_WIDTH = 1.5
RATIO_FLOOR = 1e-06
ENERGY_EPS = 1e-06
GAUSS_NODES = [-0.906179845938664, -0.5384693101056831, 0.0, 0.5384693101056831, 0.906179845938664]
GAUSS_WEIGHTS = [
    0.2369268850561891,
    0.4786286704993665,
    0.5688888888888889,
    0.4786286704993665,
    0.2369268850561891,
]


def legendre_values(points):
    values = [np.ones(points.shape), np.array(points)]
    for order in range(1, 5):
        values.append(
            ((2 * order + 1) * points * values[order] - order * values[order - 1]) / (order + 1)
        )
    return values


def line_tables():
    line_nodes = np.array(GAUSS_NODES)
    quadrature_weights = np.array(GAUSS_WEIGHTS)
    barycentric = np.array(
        [
            1.0 / np.prod([line_nodes[j] - line_nodes[k] for k in range(5) if k != j])
            for j in range(5)
        ]
    )
    derivative = np.zeros((5, 5))
    for i in range(5):
        for j in range(5):
            if i != j:
                derivative[i, j] = barycentric[j] / barycentric[i] / (line_nodes[i] - line_nodes[j])
        derivative[i, i] = -np.sum(derivative[i])
    left_values = np.ones(5)
    right_values = np.ones(5)
    for j in range(5):
        for k in range(5):
            if k != j:
                left_values[j] *= (-1.0 - line_nodes[k]) / (line_nodes[j] - line_nodes[k])
                right_values[j] *= (1.0 - line_nodes[k]) / (line_nodes[j] - line_nodes[k])
    legendre = legendre_values(line_nodes)
    fourth_slope = 7.0 * legendre[3] + 3.0 * legendre[1]
    fifth_slope = 9.0 * legendre[4] + 5.0 * legendre[2] + legendre[0]
    left_corr = 0.5 * (fourth_slope - fifth_slope)
    right_corr = 0.5 * (fourth_slope + fifth_slope)
    modal = np.zeros((5, 5))
    for k in range(5):
        modal[k, :] = quadrature_weights * math.sqrt((2 * k + 1) / 2.0) * legendre[k]
    return (line_nodes, derivative, left_values, right_values, left_corr, right_corr, modal)


NODES, DERIV, LEFT, RIGHT, LIFT_LEFT, LIFT_RIGHT, MODAL = line_tables()
HALF_LEFT = 0.5 * LIFT_LEFT
HALF_RIGHT = 0.5 * LIFT_RIGHT


def fold(u):
    return (u[0] + u[4], u[1] + u[3], u[2], u[0] - u[4], u[1] - u[3])


def traces(parts):
    s0, s1, mid, d0, d1 = parts
    r = [float(x) for x in RIGHT]
    even = 0.5 * (r[0] + r[4]) * s0 + 0.5 * (r[1] + r[3]) * s1 + r[2] * mid
    odd = 0.5 * (r[0] - r[4]) * d0 + 0.5 * (r[1] - r[3]) * d1
    return even - odd, even + odd


def slope(parts, before, after):
    s0, s1, mid, d0, d1 = parts
    h = [float(x) for x in HALF_LEFT]
    r = [float(x) for x in RIGHT]
    if before is not None:
        diff, both = before - after, before + after
    even, odd = [], []
    for i in range(3):
        lift = 0.5 * (h[i] + h[4 - i])
        value = (
            float(0.5 * (DERIV[i, 0] - DERIV[i, 4]) + lift * (r[0] - r[4])) * d0
            + float(0.5 * (DERIV[i, 1] - DERIV[i, 3]) + lift * (r[1] - r[3])) * d1
        )
        even.append(value if before is None else value + lift * diff)
    for i in range(2):
        lift = 0.5 * (h[i] - h[4 - i])
        value = (
            float(0.5 * (DERIV[i, 0] + DERIV[i, 4]) - lift * (r[0] + r[4])) * s0
            + float(0.5 * (DERIV[i, 1] + DERIV[i, 3]) - lift * (r[1] + r[3])) * s1
            + float(DERIV[i, 2] - 2.0 * lift * r[2]) * mid
        )
        odd.append(value if before is None else value + lift * both)
    return [even[0] + odd[0], even[1] + odd[1], even[2], even[1] - odd[1], even[0] - odd[0]]


def points(axis, q, j):
    if axis == 0:
        return [25 * i + 5 * q + j for i in range(5)]
    if axis == 1:
        return [25 * q + 5 * i + j for i in range(5)]
    return [25 * q + 5 * j + i for i in range(5)]


def modal_line(u):
    s0, s1, mid, d0, d1 = fold(u)
    out = []
    for k in range(5):
        m = [float(x) for x in MODAL[k]]
        out.append(m[0] * s0 + m[1] * s1 + m[2] * mid if k % 2 == 0 else m[0] * d0 + m[1] * d1)
    return out


def sensor(load, work):
    def first(q, carry):
        for j in range(5):
            pts = points(0, q, j)
            for i, value in zip(pts, modal_line([load(p) for p in pts])):
                work[i] = value
        return carry

    lax.fori_loop(0, 5, first, 0)

    def second(q, carry):
        total, high = carry
        plane = {}
        for c in range(5):
            for b, value in enumerate(modal_line([work[25 * q + 5 * b + c] for b in range(5)])):
                plane[b, c] = value
        low = jnp.zeros_like(total)
        edge = jnp.zeros_like(total)
        for b in range(5):
            line = modal_line([plane[b, c] for c in range(5)])
            squares = [x * x for x in line]
            if b < 4:
                low = low + ((squares[0] + squares[1]) + (squares[2] + squares[3]))
                edge = edge + squares[4]
            else:
                edge = edge + ((squares[0] + squares[1]) + (squares[2] + squares[3])) + squares[4]
        plane_total = low + edge
        return total + plane_total, high + jnp.where(q == 4, plane_total, edge)

    zero = jnp.zeros(work.shape[1:], jnp.float32)
    total, high = lax.fori_loop(0, 5, second, (zero, zero))
    level = jnp.log(jnp.maximum(high / (total + ENERGY_EPS), RATIO_FLOOR)) * (1.0 / math.log(10.0))
    ramp = jnp.clip((level - SENSOR_CENTRE) / SENSOR_WIDTH, -1.0, 1.0)
    return EPS_SCALE * 0.5 * (1.0 + jnp.sin(0.5 * math.pi * ramp))


def rolled(value, shift, axis):
    size = value.shape[axis]
    return pltpu.roll(value, shift % size, axis)


LOWER = [float((1.0 - x) / 2.0) for x in NODES]
UPPER = [float((1.0 + x) / 2.0) for x in NODES]


def along_lanes(line):
    lanes = line.shape[1]
    lane = lax.broadcasted_iota(jnp.int32, line.shape, 1)
    before = jnp.where(lane == 0, 0.0, rolled(line, 1, 1))
    after = jnp.where(lane == lanes - 1, 0.0, rolled(line, -1, 1))
    return jnp.maximum(line, before), jnp.maximum(line, after)


def interpolate(neighbours, nu):
    corner = {}
    for x in range(2):
        for y in range(2):
            line = jnp.maximum(
                jnp.maximum(neighbours[x][y], neighbours[x + 1][y]),
                jnp.maximum(neighbours[x][y + 1], neighbours[x + 1][y + 1]),
            )
            corner[x, y, 0], corner[x, y, 1] = along_lanes(line)
    lower, upper = LOWER, UPPER
    for a in range(5):
        face = {
            (y, z): lower[a] * corner[0, y, z] + upper[a] * corner[1, y, z]
            for y in range(2)
            for z in range(2)
        }
        for b in range(5):
            edge = [lower[b] * face[0, z] + upper[b] * face[1, z] for z in range(2)]
            for c in range(5):
                nu[25 * a + 5 * b + c] = lower[c] * edge[0] + upper[c] * edge[1]


def row_masks(axis, chords, spans, lanes):
    row = lax.broadcasted_iota(jnp.int32, (chords * spans, lanes), 0)
    if axis == 0:
        return row < spans, row >= (chords - 1) * spans
    place = row % spans
    return place == 0, place == spans - 1


def outer_rows(axis, chords, spans, last):
    if axis == 0:
        return pl.ds((chords - 1) * spans if last else 0, spans)
    return pl.ds(spans - 1 if last else 0, chords, spans)


def weights(axis, masks):
    low, high = masks[axis]
    return [
        jnp.where(low, float(HALF_LEFT[i]), jnp.where(high, float(HALF_RIGHT[i]), 0.0))
        for i in range(5)
    ]


def local_kernel(sizes, count, chords, spans, *refs):
    state_hbm = refs[0]
    nu, acc = refs[1:3]
    state, grad, around, work, eps_out, faces, outside, lifted, t0, t1, t2, t3, f0, f1, f2, f3 = refs[3:19]
    ghosts, flux_ghosts = refs[19:23], refs[23:27]
    load_sem, eps_send, eps_recv, send_sem, recv_sem = refs[27:]
    sends = ((t0, t1, t2, t3), (f0, f1, f2, f3))
    lands = (ghosts, flux_ghosts)
    rows, lanes = nu.shape[1:]
    chord_size, span_size = sizes
    me_c, me_s = lax.axis_index("chord"), lax.axis_index("span")
    mesh_id = pl.DeviceIdType.MESH

    def reachable(dx):
        if dx == 0:
            return None
        return me_c + 1 < chord_size if dx == 1 else me_c > 0

    def guarded(cond, run):
        if cond is None:
            run()
        else:
            pl.when(cond)(run)

    def partner(dx, dy):
        return (me_c + dx, lax.rem(me_s + dy + span_size, span_size))

    offsets = [(dx, dy) for dx in (0, -1, 1) for dy in (-1, 0, 1) if (dx, dy) != (0, 0)]
    barrier = pltpu.get_barrier_semaphore()
    for dx, dy in offsets:

        def greet(dx=dx, dy=dy):
            pl.semaphore_signal(barrier, inc=1, device_id=partner(dx, dy), device_id_type=mesh_id)

        guarded(reachable(dx), greet)

    def load(v):
        return pltpu.make_async_copy(state_hbm.at[v], state.at[v], load_sem.at[v])

    for v in range(count):
        load(v).start()

    def eps_copy(dx, dy):
        slot = 3 * (dx + 1) + dy + 1
        return pltpu.make_async_remote_copy(
            src_ref=eps_out, dst_ref=around.at[1 - dx, 1 - dy],
            send_sem=eps_send.at[slot], recv_sem=eps_recv.at[8 - slot],
            device_id=partner(dx, dy), device_id_type=mesh_id,
        )

    ways = ((1, 0), (-1, 0), (0, 1), (0, -1))

    def message(stage, k, v):
        dx, dy = ways[k]
        return pltpu.make_async_remote_copy(
            src_ref=sends[stage][k].at[v], dst_ref=lands[stage][k].at[v],
            send_sem=send_sem.at[stage, k], recv_sem=recv_sem.at[stage, k, v],
            device_id=partner(dx, dy), device_id_type=mesh_id,
        )

    def sent(stage, k):
        dx, dy = ways[k]
        return pltpu.make_async_remote_copy(
            src_ref=sends[stage][k], dst_ref=lands[stage][k],
            send_sem=send_sem.at[stage, k], recv_sem=recv_sem.at[stage, k, 0],
            device_id=partner(dx, dy), device_id_type=mesh_id,
        )

    def launch(stage, axis, v):
        sign = 1.0 if stage == 0 else -1.0
        for k in (2 * axis, 2 * axis + 1):
            guarded(reachable(ways[k][0]), lambda k=k: message(stage, k, v).start())
        if axis == 0:
            for k in range(2):

                def mirror(k=k):
                    lands[stage][1 - k][v] = sign * sends[stage][k][v]

                pl.when(jnp.logical_not(reachable(ways[k][0])))(mirror)

    def arrived(stage, axis, v):
        for k in (2 * axis, 2 * axis + 1):
            guarded(reachable(-ways[k][0]), lambda k=k: message(stage, k, v).wait_recv())

    masks = [row_masks(axis, chords, spans, lanes) for axis in range(2)]
    outer = [[outer_rows(axis, chords, spans, last) for last in (False, True)] for axis in range(2)]

    def extract(stage, axis, v, f, ref, index):
        up, down = sends[stage][2 * axis], sends[stage][2 * axis + 1]
        down[v, f] = ref[index + (outer[axis][0],)]
        up[v, f] = ref[index[:-1] + (index[-1] + 1, outer[axis][1])]

    def gather(stage, axis, v, f, ref):
        up, down = lands[stage][2 * axis], lands[stage][2 * axis + 1]
        ref[axis, f, outer[axis][0]] = up[v, f]
        ref[axis, f, outer[axis][1]] = down[v, f]
        return ref[axis, f]

    def send_traces(axis, v):
        def body(q, carry):
            for j in range(5):
                f = 5 * q + j
                left, right = traces(fold([state[v, p] for p in points(axis, q, j)]))
                faces[axis, v, 2 * f] = left
                faces[axis, v, 2 * f + 1] = right
                extract(0, axis, v, f, faces, (axis, v, 2 * f))
            return carry

        lax.fori_loop(0, 5, body, 0)

    for f in range(25):
        lifted[0, f] = jnp.zeros((rows, lanes), jnp.float32)
    load(0).wait()
    eps = sensor(lambda p: state[0, p], work)
    eps_out[...] = eps
    around[1, 1] = eps
    send_traces(1, 0)
    send_traces(0, 0)
    sides = jnp.where(me_c > 0, 1, 0) + jnp.where(me_c + 1 < chord_size, 1, 0)
    pl.semaphore_wait(barrier, 2 + 3 * sides)
    for dx, dy in offsets:
        guarded(reachable(dx), lambda dx=dx, dy=dy: eps_copy(dx, dy).start())
    launch(0, 0, 0)
    launch(0, 1, 0)

    def later_traces(v, carry):
        load(v).wait()
        for axis in range(2):
            send_traces(axis, v)
            launch(0, axis, v)
        return carry

    lax.fori_loop(1, count, later_traces, 0)

    lane = lax.broadcasted_iota(jnp.int32, (rows, lanes), 1)
    first, last = lane == 0, lane == lanes - 1

    def normal_gradient(v, carry):
        def body(q, carry):
            for j in range(5):
                pts = points(2, q, j)
                parts = fold([state[v, p] for p in pts])
                left, right = traces(parts)
                before = jnp.where(first, left, rolled(right, 1, 1))
                after = jnp.where(last, right, rolled(left, -1, 1))
                for p, value in zip(pts, slope(parts, before, after)):
                    grad[v, p] = value
            return carry

        lax.fori_loop(0, 5, body, 0, unroll=True)
        return carry

    lax.fori_loop(0, count, normal_gradient, 0)

    row = lax.broadcasted_iota(jnp.int32, (rows, lanes), 0)
    for dx, dy in offsets:
        guarded(reachable(-dx), lambda dx=dx, dy=dy: eps_copy(dx, dy).wait_recv())

    have_low = jnp.where(me_c > 0, spans, 0)
    have_high = jnp.where(me_c + 1 < chord_size, rows, rows - spans)
    low_s, high_s = masks[1]
    low_c, high_c = masks[0]
    column = []
    for x in range(3):
        mine, left, right = around[x, 1], around[x, 0], around[x, 2]
        column.append([
            jnp.where(low_s, rolled(left, 1 - spans, 0), rolled(mine, 1, 0)),
            mine,
            jnp.where(high_s, rolled(right, spans - 1, 0), rolled(mine, -1, 0)),
        ])
    closed_low = row < spans - have_low
    closed_high = row >= have_high
    neighbours = [[], [], []]
    for y in range(3):
        inner = column[1][y]
        below = jnp.where(low_c, rolled(column[0][y], spans, 0), rolled(inner, spans, 0))
        above = jnp.where(high_c, rolled(column[2][y], -spans, 0), rolled(inner, -spans, 0))
        neighbours[0].append(jnp.where(closed_low, 0.0, below))
        neighbours[1].append(inner)
        neighbours[2].append(jnp.where(closed_high, 0.0, above))
    interpolate(neighbours, nu)

    def flux(axis, v):
        low, high = masks[axis]
        step = spans if axis == 0 else 1

        def body(q, carry):
            for j in range(5):
                f = 5 * q + j
                pts = points(axis, q, j)
                parts = fold([state[v, p] for p in pts])
                left, right = faces[axis, v, 2 * f], faces[axis, v, 2 * f + 1]
                ghost = gather(0, axis, v, f, outside)
                before = jnp.where(low, ghost, rolled(right, step, 0))
                after = jnp.where(high, ghost, rolled(left, -step, 0))
                gradient = slope(parts, before, after)
                parts = fold([nu[p] * g for p, g in zip(pts, gradient)])
                left, right = traces(parts)
                work[2 * f] = left
                work[2 * f + 1] = right
                extract(1, axis, v, f, work, (2 * f,))
                before = jnp.where(low, 0.0, rolled(right, step, 0))
                after = jnp.where(high, 0.0, rolled(left, -step, 0))
                for p, value in zip(pts, slope(parts, before, after)):
                    if axis == 0:
                        acc[v, p] = value
                    else:
                        acc[v, p] += value
            return carry

        lax.fori_loop(0, 5, body, 0, unroll=True)

    def variable(v, carry):
        for axis in range(2):
            arrived(0, axis, v)
            flux(axis, v)
            launch(1, axis, v)
        return carry

    lax.fori_loop(0, count, variable, 0)

    def normal(v, carry):
        def body(q, carry):
            for j in range(5):
                pts = points(2, q, j)
                parts = fold([nu[p] * grad[v, p] for p in pts])
                left, right = traces(parts)
                before = jnp.where(first, -left, rolled(right, 1, 1))
                after = jnp.where(last, -right, rolled(left, -1, 1))
                for p, value in zip(pts, slope(parts, before, after)):
                    acc[v, p] += value
            return carry

        lax.fori_loop(0, 5, body, 0, unroll=True)
        return carry

    lax.fori_loop(0, count, normal, 0)

    weight_c, weight_s = weights(0, masks), weights(1, masks)

    def correct(v, carry):
        for axis in range(2):
            arrived(1, axis, v)
        for f in range(25):
            for axis in range(2):
                gather(1, axis, v, f, lifted)
        for c in range(5):
            across = [lifted[0, 5 * b + c] for b in range(5)]
            for a in range(5):
                along = lifted[1, 5 * a + c]
                for b in range(5):
                    acc[v, 25 * a + 5 * b + c] += weight_c[a] * across[b] + weight_s[b] * along
        return carry

    lax.fori_loop(0, count, correct, 0)

    for dx, dy in offsets:
        guarded(reachable(dx), lambda dx=dx, dy=dy: eps_copy(dx, dy).wait_send())
    for stage in range(2):
        for k in range(4):
            guarded(reachable(ways[k][0]), lambda stage=stage, k=k: sent(stage, k).wait_send())


def shards(state):
    count, npts, chords, spans, lanes = state.shape
    rows = chords * spans
    flat = state.reshape(count, npts, rows, lanes)
    f32 = jnp.float32
    sizes = (lax.axis_size("chord"), lax.axis_size("span"))

    def message(n, k):
        return (n, 25, spans if k < 2 else chords, lanes)

    def full(*shape):
        return jax.ShapeDtypeStruct(shape, f32)

    vmem = pl.BlockSpec(memory_space=pltpu.VMEM)
    nu, residual = pl.pallas_call(
        functools.partial(local_kernel, sizes, count, chords, spans),
        in_specs=[pl.BlockSpec(memory_space=pltpu.HBM)],
        out_specs=[vmem, vmem],
        out_shape=[full(npts, rows, lanes), full(count, npts, rows, lanes)],
        scratch_shapes=[
            pltpu.VMEM(shape, f32)
            for shape in [
                (count, npts, rows, lanes),
                (count, npts, rows, lanes),
                (3, 3, rows, lanes),
                (npts, rows, lanes),
                (rows, lanes),
                (2, count, 50, rows, lanes),
                (2, 25, rows, lanes),
                (2, 25, rows, lanes),
            ]
            + [message(count, k) for k in range(4)] * 4
        ]
        + [
            pltpu.SemaphoreType.DMA((count,)),
            pltpu.SemaphoreType.DMA((9,)),
            pltpu.SemaphoreType.DMA((9,)),
            pltpu.SemaphoreType.DMA((2, 4)),
            pltpu.SemaphoreType.DMA((2, 4, count)),
        ],
        compiler_params=pltpu.CompilerParams(
            collective_id=0, has_side_effects=True, vmem_limit_bytes=VMEM_BYTES
        ),
    )(flat)
    return residual.reshape(state.shape), nu.reshape(npts, chords, spans, lanes)


def solution(mesh):
    in_specs = (P(None, None, "chord", "span", None),)
    out_specs = (P(None, None, "chord", "span", None), P(None, "chord", "span", None))
    return jax.shard_map(shards, mesh=mesh, in_specs=in_specs, out_specs=out_specs, check_vma=False)
```

```python
import functools
import math

import jax
import jax.numpy as jnp
import numpy as np
from jax import lax
from jax.experimental import pallas as pl
from jax.experimental.pallas import tpu as pltpu
from jax.sharding import PartitionSpec as P

VMEM_BYTES = 52_500_000
EPS_SCALE = 0.01
SENSOR_CENTRE = -3.0
SENSOR_WIDTH = 1.5
RATIO_FLOOR = 1e-06
ENERGY_EPS = 1e-06
GAUSS_NODES = [-0.906179845938664, -0.5384693101056831, 0.0, 0.5384693101056831, 0.906179845938664]
GAUSS_WEIGHTS = [
    0.2369268850561891,
    0.4786286704993665,
    0.5688888888888889,
    0.4786286704993665,
    0.2369268850561891,
]


def legendre_values(points):
    values = [np.ones(points.shape), np.array(points)]
    for order in range(1, 5):
        values.append(
            ((2 * order + 1) * points * values[order] - order * values[order - 1]) / (order + 1)
        )
    return values


def line_tables():
    line_nodes = np.array(GAUSS_NODES)
    quadrature_weights = np.array(GAUSS_WEIGHTS)
    barycentric = np.array(
        [
            1.0 / np.prod([line_nodes[j] - line_nodes[k] for k in range(5) if k != j])
            for j in range(5)
        ]
    )
    derivative = np.zeros((5, 5))
    for i in range(5):
        for j in range(5):
            if i != j:
                derivative[i, j] = barycentric[j] / barycentric[i] / (line_nodes[i] - line_nodes[j])
        derivative[i, i] = -np.sum(derivative[i])
    left_values = np.ones(5)
    right_values = np.ones(5)
    for j in range(5):
        for k in range(5):
            if k != j:
                left_values[j] *= (-1.0 - line_nodes[k]) / (line_nodes[j] - line_nodes[k])
                right_values[j] *= (1.0 - line_nodes[k]) / (line_nodes[j] - line_nodes[k])
    legendre = legendre_values(line_nodes)
    fourth_slope = 7.0 * legendre[3] + 3.0 * legendre[1]
    fifth_slope = 9.0 * legendre[4] + 5.0 * legendre[2] + legendre[0]
    left_corr = 0.5 * (fourth_slope - fifth_slope)
    right_corr = 0.5 * (fourth_slope + fifth_slope)
    modal = np.zeros((5, 5))
    for k in range(5):
        modal[k, :] = quadrature_weights * math.sqrt((2 * k + 1) / 2.0) * legendre[k]
    return (line_nodes, derivative, left_values, right_values, left_corr, right_corr, modal)


NODES, DERIV, LEFT, RIGHT, LIFT_LEFT, LIFT_RIGHT, MODAL = line_tables()
HALF_LEFT = 0.5 * LIFT_LEFT
HALF_RIGHT = 0.5 * LIFT_RIGHT


def fold(u):
    return (u[0] + u[4], u[1] + u[3], u[2], u[0] - u[4], u[1] - u[3])


def traces(parts):
    s0, s1, mid, d0, d1 = parts
    r = [float(x) for x in RIGHT]
    even = 0.5 * (r[0] + r[4]) * s0 + 0.5 * (r[1] + r[3]) * s1 + r[2] * mid
    odd = 0.5 * (r[0] - r[4]) * d0 + 0.5 * (r[1] - r[3]) * d1
    return even - odd, even + odd


def slope(parts, before, after):
    s0, s1, mid, d0, d1 = parts
    h = [float(x) for x in HALF_LEFT]
    r = [float(x) for x in RIGHT]
    if before is not None:
        diff, both = before - after, before + after
    even, odd = [], []
    for i in range(3):
        lift = 0.5 * (h[i] + h[4 - i])
        value = (
            float(0.5 * (DERIV[i, 0] - DERIV[i, 4]) + lift * (r[0] - r[4])) * d0
            + float(0.5 * (DERIV[i, 1] - DERIV[i, 3]) + lift * (r[1] - r[3])) * d1
        )
        even.append(value if before is None else value + lift * diff)
    for i in range(2):
        lift = 0.5 * (h[i] - h[4 - i])
        value = (
            float(0.5 * (DERIV[i, 0] + DERIV[i, 4]) - lift * (r[0] + r[4])) * s0
            + float(0.5 * (DERIV[i, 1] + DERIV[i, 3]) - lift * (r[1] + r[3])) * s1
            + float(DERIV[i, 2] - 2.0 * lift * r[2]) * mid
        )
        odd.append(value if before is None else value + lift * both)
    return [even[0] + odd[0], even[1] + odd[1], even[2], even[1] - odd[1], even[0] - odd[0]]


def points(axis, q, j):
    if axis == 0:
        return [25 * i + 5 * q + j for i in range(5)]
    if axis == 1:
        return [25 * q + 5 * i + j for i in range(5)]
    return [25 * q + 5 * j + i for i in range(5)]


def modal_line(u):
    s0, s1, mid, d0, d1 = fold(u)
    out = []
    for k in range(5):
        m = [float(x) for x in MODAL[k]]
        out.append(m[0] * s0 + m[1] * s1 + m[2] * mid if k % 2 == 0 else m[0] * d0 + m[1] * d1)
    return out


def sensor(load, work):
    def first(q, carry):
        for j in range(5):
            pts = points(0, q, j)
            for i, value in zip(pts, modal_line([load(p) for p in pts])):
                work[i] = value
        return carry

    lax.fori_loop(0, 5, first, 0)

    def second(q, carry):
        total, high = carry
        plane = {}
        for c in range(5):
            for b, value in enumerate(modal_line([work[25 * q + 5 * b + c] for b in range(5)])):
                plane[b, c] = value
        low = jnp.zeros_like(total)
        edge = jnp.zeros_like(total)
        for b in range(5):
            line = modal_line([plane[b, c] for c in range(5)])
            squares = [x * x for x in line]
            if b < 4:
                low = low + ((squares[0] + squares[1]) + (squares[2] + squares[3]))
                edge = edge + squares[4]
            else:
                edge = edge + ((squares[0] + squares[1]) + (squares[2] + squares[3])) + squares[4]
        plane_total = low + edge
        return total + plane_total, high + jnp.where(q == 4, plane_total, edge)

    zero = jnp.zeros(work.shape[1:], jnp.float32)
    total, high = lax.fori_loop(0, 5, second, (zero, zero))
    level = jnp.log(jnp.maximum(high / (total + ENERGY_EPS), RATIO_FLOOR)) * (1.0 / math.log(10.0))
    ramp = jnp.clip((level - SENSOR_CENTRE) / SENSOR_WIDTH, -1.0, 1.0)
    return EPS_SCALE * 0.5 * (1.0 + jnp.sin(0.5 * math.pi * ramp))


def rolled(value, shift, axis):
    size = value.shape[axis]
    return pltpu.roll(value, shift % size, axis)


LOWER = [float((1.0 - x) / 2.0) for x in NODES]
UPPER = [float((1.0 + x) / 2.0) for x in NODES]


def along_lanes(line):
    lanes = line.shape[1]
    lane = lax.broadcasted_iota(jnp.int32, line.shape, 1)
    before = jnp.where(lane == 0, 0.0, rolled(line, 1, 1))
    after = jnp.where(lane == lanes - 1, 0.0, rolled(line, -1, 1))
    return jnp.maximum(line, before), jnp.maximum(line, after)


def interpolate(neighbours, nu):
    corner = {}
    for x in range(2):
        for y in range(2):
            line = jnp.maximum(
                jnp.maximum(neighbours[x][y], neighbours[x + 1][y]),
                jnp.maximum(neighbours[x][y + 1], neighbours[x + 1][y + 1]),
            )
            corner[x, y, 0], corner[x, y, 1] = along_lanes(line)
    lower, upper = LOWER, UPPER
    for a in range(5):
        face = {
            (y, z): lower[a] * corner[0, y, z] + upper[a] * corner[1, y, z]
            for y in range(2)
            for z in range(2)
        }
        for b in range(5):
            edge = [lower[b] * face[0, z] + upper[b] * face[1, z] for z in range(2)]
            for c in range(5):
                nu[25 * a + 5 * b + c] = lower[c] * edge[0] + upper[c] * edge[1]


def row_masks(axis, chords, spans, lanes):
    row = lax.broadcasted_iota(jnp.int32, (chords * spans, lanes), 0)
    if axis == 0:
        return row < spans, row >= (chords - 1) * spans
    place = row % spans
    return place == 0, place == spans - 1


def outer_rows(axis, chords, spans, last):
    if axis == 0:
        return pl.ds((chords - 1) * spans if last else 0, spans)
    return pl.ds(spans - 1 if last else 0, chords, spans)


def weights(axis, masks):
    low, high = masks[axis]
    return [
        jnp.where(low, float(HALF_LEFT[i]), jnp.where(high, float(HALF_RIGHT[i]), 0.0))
        for i in range(5)
    ]


def local_kernel(sizes, count, chords, spans, *refs):
    state_hbm = refs[0]
    nu, acc = refs[1:3]
    state, grad, around, work, eps_out, faces, outside, lifted, relay = refs[3:12]
    sends = (refs[12:16], refs[16:20])
    lands = (refs[20:24], refs[24:28])
    load_sem, eps_send, eps_recv, send_sem, recv_sem, relay_sem, pass_sem = refs[28:]
    rows, lanes = nu.shape[1:]
    chord_size, span_size = sizes
    me_c, me_s = lax.axis_index("chord"), lax.axis_index("span")
    mesh_id = pl.DeviceIdType.MESH

    def reachable(dx):
        if dx == 0:
            return None
        return me_c + 1 < chord_size if dx == 1 else me_c > 0

    def guarded(cond, run):
        if cond is None:
            run()
        else:
            pl.when(cond)(run)

    def partner(dx, dy):
        return (me_c + dx, lax.rem(me_s + dy + span_size, span_size))

    cut = chord_size // 2
    ends = ((cut - 1, 0, cut), (cut, chord_size - 1, cut - 1))
    twin = me_s + 1 - 2 * lax.rem(me_s, 2)
    detoured = lax.rem((me_s + 1) // 2, 2) == 1
    relaying = jnp.logical_not(detoured)

    offsets = [(dx, dy) for dx in (0, -1, 1) for dy in (-1, 0, 1) if (dx, dy) != (0, 0)]
    barrier = pltpu.get_barrier_semaphore()
    for dx, dy in offsets:

        def greet(dx=dx, dy=dy):
            pl.semaphore_signal(barrier, inc=1, device_id=partner(dx, dy), device_id_type=mesh_id)

        guarded(reachable(dx), greet)

    for source, through, target in ends:
        for here, ready, there in ((through, relaying, source), (target, detoured, through)):

            def greet_relay(there=there):
                pl.semaphore_signal(
                    barrier, inc=1, device_id=(there, twin), device_id_type=mesh_id
                )

            pl.when((me_c == here) & ready)(greet_relay)

    def load(v):
        return pltpu.make_async_copy(state_hbm.at[v], state.at[v], load_sem.at[v])

    for v in range(count):
        load(v).start()

    def eps_copy(dx, dy):
        slot = 3 * (dx + 1) + dy + 1
        return pltpu.make_async_remote_copy(
            src_ref=eps_out, dst_ref=around.at[1 - dx, 1 - dy],
            send_sem=eps_send.at[slot], recv_sem=eps_recv.at[8 - slot],
            device_id=partner(dx, dy), device_id_type=mesh_id,
        )

    ways = ((1, 0), (-1, 0), (0, 1), (0, -1))

    def message(stage, k, v):
        dx, dy = ways[k]
        return pltpu.make_async_remote_copy(
            src_ref=sends[stage][k].at[v], dst_ref=lands[stage][k].at[v],
            send_sem=send_sem.at[stage, k], recv_sem=recv_sem.at[stage, k, v],
            device_id=partner(dx, dy), device_id_type=mesh_id,
        )

    def sent(stage, k):
        dx, dy = ways[k]
        return pltpu.make_async_remote_copy(
            src_ref=sends[stage][k], dst_ref=lands[stage][k],
            send_sem=send_sem.at[stage, k], recv_sem=recv_sem.at[stage, k, 0],
            device_id=partner(dx, dy), device_id_type=mesh_id,
        )

    def detour(stage, k, v):
        return pltpu.make_async_remote_copy(
            src_ref=sends[stage][k].at[v], dst_ref=relay.at[stage, v],
            send_sem=send_sem.at[stage, k], recv_sem=relay_sem.at[stage, v],
            device_id=(ends[k][1], twin), device_id_type=mesh_id,
        )

    def onward(stage, k, v):
        return pltpu.make_async_remote_copy(
            src_ref=relay.at[stage, v], dst_ref=lands[stage][k].at[v],
            send_sem=pass_sem.at[stage], recv_sem=recv_sem.at[stage, k, v],
            device_id=(ends[k][2], twin), device_id_type=mesh_id,
        )

    def forward(stage, v):
        for k in range(2):

            def hand_on(k=k):
                detour(stage, k, v).wait_recv()
                onward(stage, k, v).start()

            pl.when((me_c == ends[k][1]) & relaying)(hand_on)

    def forwarded(stage):
        def wait():
            pltpu.make_async_remote_copy(
                src_ref=relay.at[stage], dst_ref=relay.at[stage],
                send_sem=pass_sem.at[stage], recv_sem=relay_sem.at[stage, 0],
                device_id=(me_c, twin), device_id_type=mesh_id,
            ).wait_send()

        pl.when(((me_c == ends[0][1]) | (me_c == ends[1][1])) & relaying)(wait)

    def launch(stage, axis, v):
        sign = 1.0 if stage == 0 else -1.0
        for k in (2 * axis, 2 * axis + 1):
            if axis == 1:
                message(stage, k, v).start()
                continue
            indirect = (me_c == ends[k][0]) & detoured
            direct = reachable(ways[k][0]) & jnp.logical_not(indirect)
            pl.when(direct)(lambda k=k: message(stage, k, v).start())
            pl.when(indirect)(lambda k=k: detour(stage, k, v).start())
        if axis == 0:
            for k in range(2):

                def mirror(k=k):
                    lands[stage][1 - k][v] = sign * sends[stage][k][v]

                pl.when(jnp.logical_not(reachable(ways[k][0])))(mirror)

    def arrived(stage, axis, v):
        for k in (2 * axis, 2 * axis + 1):
            guarded(reachable(-ways[k][0]), lambda k=k: message(stage, k, v).wait_recv())

    masks = [row_masks(axis, chords, spans, lanes) for axis in range(2)]
    outer = [[outer_rows(axis, chords, spans, last) for last in (False, True)] for axis in range(2)]

    def extract(stage, axis, v, f, ref, index):
        up, down = sends[stage][2 * axis], sends[stage][2 * axis + 1]
        down[v, f] = ref[index + (outer[axis][0],)]
        up[v, f] = ref[index[:-1] + (index[-1] + 1, outer[axis][1])]

    def gather(stage, axis, v, f, ref):
        up, down = lands[stage][2 * axis], lands[stage][2 * axis + 1]
        ref[axis, f, outer[axis][0]] = up[v, f]
        ref[axis, f, outer[axis][1]] = down[v, f]
        return ref[axis, f]

    def send_traces(axis, v):
        def body(q, carry):
            for j in range(5):
                f = 5 * q + j
                left, right = traces(fold([state[v, p] for p in points(axis, q, j)]))
                faces[axis, v, 2 * f] = left
                faces[axis, v, 2 * f + 1] = right
                extract(0, axis, v, f, faces, (axis, v, 2 * f))
            return carry

        lax.fori_loop(0, 5, body, 0)

    for f in range(25):
        lifted[0, f] = jnp.zeros((rows, lanes), jnp.float32)
    load(0).wait()
    eps = sensor(lambda p: state[0, p], work)
    eps_out[...] = eps
    around[1, 1] = eps
    send_traces(1, 0)
    send_traces(0, 0)
    sides = jnp.where(me_c > 0, 1, 0) + jnp.where(me_c + 1 < chord_size, 1, 0)
    turns = jnp.where(relaying, jnp.where((me_c == ends[0][1]) | (me_c == ends[1][1]), 1, 0), 0)
    turns += jnp.where(detoured, jnp.where((me_c == ends[0][0]) | (me_c == ends[1][0]), 1, 0), 0)
    pl.semaphore_wait(barrier, 2 + 3 * sides + turns)
    for dx, dy in offsets:
        guarded(reachable(dx), lambda dx=dx, dy=dy: eps_copy(dx, dy).start())
    launch(0, 0, 0)
    launch(0, 1, 0)

    def later_traces(v, carry):
        load(v).wait()
        for axis in range(2):
            send_traces(axis, v)
            launch(0, axis, v)
        return carry

    lax.fori_loop(1, count, later_traces, 0)

    lane = lax.broadcasted_iota(jnp.int32, (rows, lanes), 1)
    first, last = lane == 0, lane == lanes - 1

    def normal_gradient(v, carry):
        def body(q, carry):
            for j in range(5):
                pts = points(2, q, j)
                parts = fold([state[v, p] for p in pts])
                left, right = traces(parts)
                before = jnp.where(first, left, rolled(right, 1, 1))
                after = jnp.where(last, right, rolled(left, -1, 1))
                for p, value in zip(pts, slope(parts, before, after)):
                    grad[v, p] = value
            return carry

        lax.fori_loop(0, 5, body, 0, unroll=True)
        return carry

    lax.fori_loop(0, count, normal_gradient, 0)
    for v in range(3):
        forward(0, v)

    row = lax.broadcasted_iota(jnp.int32, (rows, lanes), 0)
    for dx, dy in offsets:
        guarded(reachable(-dx), lambda dx=dx, dy=dy: eps_copy(dx, dy).wait_recv())

    have_low = jnp.where(me_c > 0, spans, 0)
    have_high = jnp.where(me_c + 1 < chord_size, rows, rows - spans)
    low_s, high_s = masks[1]
    low_c, high_c = masks[0]
    column = []
    for x in range(3):
        mine, left, right = around[x, 1], around[x, 0], around[x, 2]
        column.append([
            jnp.where(low_s, rolled(left, 1 - spans, 0), rolled(mine, 1, 0)),
            mine,
            jnp.where(high_s, rolled(right, spans - 1, 0), rolled(mine, -1, 0)),
        ])
    closed_low = row < spans - have_low
    closed_high = row >= have_high
    neighbours = [[], [], []]
    for y in range(3):
        inner = column[1][y]
        below = jnp.where(low_c, rolled(column[0][y], spans, 0), rolled(inner, spans, 0))
        above = jnp.where(high_c, rolled(column[2][y], -spans, 0), rolled(inner, -spans, 0))
        neighbours[0].append(jnp.where(closed_low, 0.0, below))
        neighbours[1].append(inner)
        neighbours[2].append(jnp.where(closed_high, 0.0, above))
    interpolate(neighbours, nu)
    for v in range(3, count):
        forward(0, v)

    def flux(axis, v):
        low, high = masks[axis]
        step = spans if axis == 0 else 1

        def body(q, carry):
            for j in range(5):
                f = 5 * q + j
                pts = points(axis, q, j)
                parts = fold([state[v, p] for p in pts])
                left, right = faces[axis, v, 2 * f], faces[axis, v, 2 * f + 1]
                ghost = gather(0, axis, v, f, outside)
                before = jnp.where(low, ghost, rolled(right, step, 0))
                after = jnp.where(high, ghost, rolled(left, -step, 0))
                gradient = slope(parts, before, after)
                parts = fold([nu[p] * g for p, g in zip(pts, gradient)])
                left, right = traces(parts)
                work[2 * f] = left
                work[2 * f + 1] = right
                extract(1, axis, v, f, work, (2 * f,))
                before = jnp.where(low, 0.0, rolled(right, step, 0))
                after = jnp.where(high, 0.0, rolled(left, -step, 0))
                for p, value in zip(pts, slope(parts, before, after)):
                    if axis == 0:
                        acc[v, p] = value
                    else:
                        acc[v, p] += value
            return carry

        lax.fori_loop(0, 5, body, 0, unroll=True)

    def variable(v, carry):
        for axis in range(2):
            arrived(0, axis, v)
            flux(axis, v)
            launch(1, axis, v)
        return carry

    lax.fori_loop(0, count, variable, 0)

    def normal(v, carry):
        def body(q, carry):
            for j in range(5):
                pts = points(2, q, j)
                parts = fold([nu[p] * grad[v, p] for p in pts])
                left, right = traces(parts)
                before = jnp.where(first, -left, rolled(right, 1, 1))
                after = jnp.where(last, -right, rolled(left, -1, 1))
                for p, value in zip(pts, slope(parts, before, after)):
                    acc[v, p] += value
            return carry

        lax.fori_loop(0, 5, body, 0, unroll=True)
        return carry

    forward(1, 0)
    lax.fori_loop(0, count, normal, 0)
    for v in range(1, 3):
        forward(1, v)

    weight_c, weight_s = weights(0, masks), weights(1, masks)

    def correct(v, carry):
        pl.when(v + 3 < count)(lambda: forward(1, v + 3))
        for axis in range(2):
            arrived(1, axis, v)
        for f in range(25):
            for axis in range(2):
                gather(1, axis, v, f, lifted)
        for c in range(5):
            across = [lifted[0, 5 * b + c] for b in range(5)]
            for a in range(5):
                along = lifted[1, 5 * a + c]
                for b in range(5):
                    acc[v, 25 * a + 5 * b + c] += weight_c[a] * across[b] + weight_s[b] * along
        return carry

    lax.fori_loop(0, count, correct, 0)

    for dx, dy in offsets:
        guarded(reachable(dx), lambda dx=dx, dy=dy: eps_copy(dx, dy).wait_send())
    for stage in range(2):
        for k in range(4):
            guarded(reachable(ways[k][0]), lambda stage=stage, k=k: sent(stage, k).wait_send())
        forwarded(stage)


def shards(state):
    count, npts, chords, spans, lanes = state.shape
    rows = chords * spans
    flat = state.reshape(count, npts, rows, lanes)
    f32 = jnp.float32
    sizes = (lax.axis_size("chord"), lax.axis_size("span"))

    def message(n, k):
        return (n, 25, spans if k < 2 else chords, lanes)

    def full(*shape):
        return jax.ShapeDtypeStruct(shape, f32)

    vmem = pl.BlockSpec(memory_space=pltpu.VMEM)
    nu, residual = pl.pallas_call(
        functools.partial(local_kernel, sizes, count, chords, spans),
        in_specs=[pl.BlockSpec(memory_space=pltpu.HBM)],
        out_specs=[vmem, vmem],
        out_shape=[full(npts, rows, lanes), full(count, npts, rows, lanes)],
        scratch_shapes=[
            pltpu.VMEM(shape, f32)
            for shape in [
                (count, npts, rows, lanes),
                (count, npts, rows, lanes),
                (3, 3, rows, lanes),
                (npts, rows, lanes),
                (rows, lanes),
                (2, count, 50, rows, lanes),
                (2, 25, rows, lanes),
                (2, 25, rows, lanes),
                (2, *message(count, 0)),
            ]
            + [message(count, k) for k in range(4)] * 4
        ]
        + [
            pltpu.SemaphoreType.DMA((count,)),
            pltpu.SemaphoreType.DMA((9,)),
            pltpu.SemaphoreType.DMA((9,)),
            pltpu.SemaphoreType.DMA((2, 4)),
            pltpu.SemaphoreType.DMA((2, 4, count)),
            pltpu.SemaphoreType.DMA((2, count)),
            pltpu.SemaphoreType.DMA((2,)),
        ],
        compiler_params=pltpu.CompilerParams(
            collective_id=0, has_side_effects=True, vmem_limit_bytes=VMEM_BYTES
        ),
    )(flat)
    return residual.reshape(state.shape), nu.reshape(npts, chords, spans, lanes)


def solution(mesh):
    in_specs = (P(None, None, "chord", "span", None),)
    out_specs = (P(None, None, "chord", "span", None), P(None, "chord", "span", None))
    return jax.shard_map(shards, mesh=mesh, in_specs=in_specs, out_specs=out_specs, check_vma=False)
```

```python
import functools
import math

import jax
import jax.numpy as jnp
import numpy as np
from jax import lax
from jax.experimental import pallas as pl
from jax.experimental.pallas import tpu as pltpu
from jax.sharding import PartitionSpec as P

VMEM_BYTES = 52_500_000
EPS_SCALE = 0.01
SENSOR_CENTRE = -3.0
SENSOR_WIDTH = 1.5
RATIO_FLOOR = 1e-06
ENERGY_EPS = 1e-06
GAUSS_NODES = [-0.906179845938664, -0.5384693101056831, 0.0, 0.5384693101056831, 0.906179845938664]
GAUSS_WEIGHTS = [
    0.2369268850561891,
    0.4786286704993665,
    0.5688888888888889,
    0.4786286704993665,
    0.2369268850561891,
]


def legendre_values(points):
    values = [np.ones(points.shape), np.array(points)]
    for order in range(1, 5):
        values.append(
            ((2 * order + 1) * points * values[order] - order * values[order - 1]) / (order + 1)
        )
    return values


def line_tables():
    line_nodes = np.array(GAUSS_NODES)
    quadrature_weights = np.array(GAUSS_WEIGHTS)
    barycentric = np.array(
        [
            1.0 / np.prod([line_nodes[j] - line_nodes[k] for k in range(5) if k != j])
            for j in range(5)
        ]
    )
    derivative = np.zeros((5, 5))
    for i in range(5):
        for j in range(5):
            if i != j:
                derivative[i, j] = barycentric[j] / barycentric[i] / (line_nodes[i] - line_nodes[j])
        derivative[i, i] = -np.sum(derivative[i])
    left_values = np.ones(5)
    right_values = np.ones(5)
    for j in range(5):
        for k in range(5):
            if k != j:
                left_values[j] *= (-1.0 - line_nodes[k]) / (line_nodes[j] - line_nodes[k])
                right_values[j] *= (1.0 - line_nodes[k]) / (line_nodes[j] - line_nodes[k])
    legendre = legendre_values(line_nodes)
    fourth_slope = 7.0 * legendre[3] + 3.0 * legendre[1]
    fifth_slope = 9.0 * legendre[4] + 5.0 * legendre[2] + legendre[0]
    left_corr = 0.5 * (fourth_slope - fifth_slope)
    right_corr = 0.5 * (fourth_slope + fifth_slope)
    modal = np.zeros((5, 5))
    for k in range(5):
        modal[k, :] = quadrature_weights * math.sqrt((2 * k + 1) / 2.0) * legendre[k]
    return (line_nodes, derivative, left_values, right_values, left_corr, right_corr, modal)


NODES, DERIV, LEFT, RIGHT, LIFT_LEFT, LIFT_RIGHT, MODAL = line_tables()
HALF_LEFT = 0.5 * LIFT_LEFT
HALF_RIGHT = 0.5 * LIFT_RIGHT


def fold(u):
    return (u[0] + u[4], u[1] + u[3], u[2], u[0] - u[4], u[1] - u[3])


def traces(parts):
    s0, s1, mid, d0, d1 = parts
    r = [float(x) for x in RIGHT]
    even = 0.5 * (r[0] + r[4]) * s0 + 0.5 * (r[1] + r[3]) * s1 + r[2] * mid
    odd = 0.5 * (r[0] - r[4]) * d0 + 0.5 * (r[1] - r[3]) * d1
    return even - odd, even + odd


def slope(parts, before, after):
    s0, s1, mid, d0, d1 = parts
    h = [float(x) for x in HALF_LEFT]
    r = [float(x) for x in RIGHT]
    if before is not None:
        diff, both = before - after, before + after
    even, odd = [], []
    for i in range(3):
        lift = 0.5 * (h[i] + h[4 - i])
        value = (
            float(0.5 * (DERIV[i, 0] - DERIV[i, 4]) + lift * (r[0] - r[4])) * d0
            + float(0.5 * (DERIV[i, 1] - DERIV[i, 3]) + lift * (r[1] - r[3])) * d1
        )
        even.append(value if before is None else value + lift * diff)
    for i in range(2):
        lift = 0.5 * (h[i] - h[4 - i])
        value = (
            float(0.5 * (DERIV[i, 0] + DERIV[i, 4]) - lift * (r[0] + r[4])) * s0
            + float(0.5 * (DERIV[i, 1] + DERIV[i, 3]) - lift * (r[1] + r[3])) * s1
            + float(DERIV[i, 2] - 2.0 * lift * r[2]) * mid
        )
        odd.append(value if before is None else value + lift * both)
    return [even[0] + odd[0], even[1] + odd[1], even[2], even[1] - odd[1], even[0] - odd[0]]


def points(axis, q, j):
    if axis == 0:
        return [25 * i + 5 * q + j for i in range(5)]
    if axis == 1:
        return [25 * q + 5 * i + j for i in range(5)]
    return [25 * q + 5 * j + i for i in range(5)]


def modal_line(u):
    s0, s1, mid, d0, d1 = fold(u)
    out = []
    for k in range(5):
        m = [float(x) for x in MODAL[k]]
        out.append(m[0] * s0 + m[1] * s1 + m[2] * mid if k % 2 == 0 else m[0] * d0 + m[1] * d1)
    return out


def sensor(load, work):
    def first(q, carry):
        for j in range(5):
            pts = points(0, q, j)
            for i, value in zip(pts, modal_line([load(p) for p in pts])):
                work[i] = value
        return carry

    lax.fori_loop(0, 5, first, 0)

    def second(q, carry):
        total, high = carry
        plane = {}
        for c in range(5):
            for b, value in enumerate(modal_line([work[25 * q + 5 * b + c] for b in range(5)])):
                plane[b, c] = value
        low = jnp.zeros_like(total)
        edge = jnp.zeros_like(total)
        for b in range(5):
            line = modal_line([plane[b, c] for c in range(5)])
            squares = [x * x for x in line]
            if b < 4:
                low = low + ((squares[0] + squares[1]) + (squares[2] + squares[3]))
                edge = edge + squares[4]
            else:
                edge = edge + ((squares[0] + squares[1]) + (squares[2] + squares[3])) + squares[4]
        plane_total = low + edge
        return total + plane_total, high + jnp.where(q == 4, plane_total, edge)

    zero = jnp.zeros(work.shape[1:], jnp.float32)
    total, high = lax.fori_loop(0, 5, second, (zero, zero))
    level = jnp.log(jnp.maximum(high / (total + ENERGY_EPS), RATIO_FLOOR)) * (1.0 / math.log(10.0))
    ramp = jnp.clip((level - SENSOR_CENTRE) / SENSOR_WIDTH, -1.0, 1.0)
    return EPS_SCALE * 0.5 * (1.0 + jnp.sin(0.5 * math.pi * ramp))


def rolled(value, shift, axis):
    size = value.shape[axis]
    return pltpu.roll(value, shift % size, axis)


LOWER = [float((1.0 - x) / 2.0) for x in NODES]
UPPER = [float((1.0 + x) / 2.0) for x in NODES]


def along_lanes(line):
    lanes = line.shape[1]
    lane = lax.broadcasted_iota(jnp.int32, line.shape, 1)
    before = jnp.where(lane == 0, 0.0, rolled(line, 1, 1))
    after = jnp.where(lane == lanes - 1, 0.0, rolled(line, -1, 1))
    return jnp.maximum(line, before), jnp.maximum(line, after)


def interpolate(neighbours, nu):
    corner = {}
    for x in range(2):
        for y in range(2):
            line = jnp.maximum(
                jnp.maximum(neighbours[x][y], neighbours[x + 1][y]),
                jnp.maximum(neighbours[x][y + 1], neighbours[x + 1][y + 1]),
            )
            corner[x, y, 0], corner[x, y, 1] = along_lanes(line)
    lower, upper = LOWER, UPPER
    for a in range(5):
        face = {
            (y, z): lower[a] * corner[0, y, z] + upper[a] * corner[1, y, z]
            for y in range(2)
            for z in range(2)
        }
        for b in range(5):
            edge = [lower[b] * face[0, z] + upper[b] * face[1, z] for z in range(2)]
            for c in range(5):
                nu[25 * a + 5 * b + c] = lower[c] * edge[0] + upper[c] * edge[1]
    return corner


def row_masks(axis, chords, spans, lanes):
    row = lax.broadcasted_iota(jnp.int32, (chords * spans, lanes), 0)
    if axis == 0:
        return row < spans, row >= (chords - 1) * spans
    place = row % spans
    return place == 0, place == spans - 1


def outer_rows(axis, chords, spans, last):
    if axis == 0:
        return pl.ds((chords - 1) * spans if last else 0, spans)
    return pl.ds(spans - 1 if last else 0, chords, spans)


def weights(axis, masks):
    low, high = masks[axis]
    return [
        jnp.where(low, float(HALF_LEFT[i]), jnp.where(high, float(HALF_RIGHT[i]), 0.0))
        for i in range(5)
    ]


def local_kernel(sizes, count, chords, spans, *refs):
    state_hbm = refs[0]
    nu, acc = refs[1:3]
    state, grad, halo, work, faces, lifted, beta, spread, relay = refs[3:12]
    sends = (refs[12:16], refs[16:20])
    lands = (refs[20:24], refs[24:28])
    load_sem, eps_send, eps_recv, send_sem, recv_sem, relay_sem, pass_sem = refs[28:]
    rows, lanes = nu.shape[1:]
    chord_size, span_size = sizes
    me_c, me_s = lax.axis_index("chord"), lax.axis_index("span")
    mesh_id = pl.DeviceIdType.MESH

    def reachable(dx):
        if dx == 0:
            return None
        return me_c + 1 < chord_size if dx == 1 else me_c > 0

    def guarded(cond, run):
        if cond is None:
            run()
        else:
            pl.when(cond)(run)

    def partner(dx, dy):
        return (me_c + dx, lax.rem(me_s + dy + span_size, span_size))

    cut, final = chord_size // 2, chord_size - 1
    ends = ((cut - 1, cut), (cut, cut - 1))
    twin = me_s + 1 - 2 * lax.rem(me_s, 2)
    detoured = lax.rem((me_s + 1) // 2, 2) == 1
    relaying = jnp.logical_not(detoured)
    longer = 2
    routes = (
        ((0, True, 0, count - longer), (1, True, count - longer, count), (2, False, count - longer, count)),
        ((0, True, longer, count), (1, True, 0, longer), (2, False, 0, longer)),
    )

    def place(k, depth):
        return depth if k == 0 else final - depth

    def mate(twinned):
        return twin if twinned else me_s

    offsets = [(dx, dy) for dx in (0, -1, 1) for dy in (-1, 0, 1) if (dx, dy) != (0, 0)]
    for r in range(chords + 4):
        for q in range(spans + 4):
            halo[r, q] = jnp.zeros((1, lanes), jnp.float32)
    barrier = pltpu.get_barrier_semaphore()
    for dx, dy in offsets:

        def greet(dx=dx, dy=dy):
            pl.semaphore_signal(barrier, inc=1, device_id=partner(dx, dy), device_id_type=mesh_id)

        guarded(reachable(dx), greet)

    extra = 0
    for k, (source, target) in enumerate(ends):
        for depth, twinned, _, _ in routes[0]:
            through = place(k, depth)
            sender = detoured if twinned else relaying
            hops = [(target, sender, through, relaying)]
            if twinned:
                hops.append((through, relaying, source, sender))
            for here, ready, there, awaiting in hops:

                def greet_relay(there=there, twinned=twinned):
                    pl.semaphore_signal(
                        barrier, inc=1, device_id=(there, mate(twinned)), device_id_type=mesh_id
                    )

                pl.when((me_c == here) & ready)(greet_relay)
                extra += jnp.where((me_c == there) & awaiting, 1, 0)

    def load(v):
        return pltpu.make_async_copy(state_hbm.at[v], state.at[v], load_sem.at[v])

    for v in range(count):
        load(v).start()

    def layer(d, length, inside):
        if d == 0:
            return pl.ds(2, length)
        if inside:
            return pl.ds(length if d == 1 else 2, 2)
        return pl.ds(0 if d == 1 else length + 2, 2)

    def eps_copy(dx, dy):
        slot = 3 * (dx + 1) + dy + 1
        return pltpu.make_async_remote_copy(
            src_ref=halo.at[layer(dx, chords, True), layer(dy, spans, True)],
            dst_ref=halo.at[layer(dx, chords, False), layer(dy, spans, False)],
            send_sem=eps_send.at[slot], recv_sem=eps_recv.at[8 - slot],
            device_id=partner(dx, dy), device_id_type=mesh_id,
        )

    ways = ((1, 0), (-1, 0), (0, 1), (0, -1))

    def message(stage, k, v):
        dx, dy = ways[k]
        return pltpu.make_async_remote_copy(
            src_ref=sends[stage][k].at[v], dst_ref=lands[stage][k].at[v],
            send_sem=send_sem.at[stage, k], recv_sem=recv_sem.at[stage, k, v],
            device_id=partner(dx, dy), device_id_type=mesh_id,
        )

    def sent(stage, k):
        dx, dy = ways[k]
        return pltpu.make_async_remote_copy(
            src_ref=sends[stage][k], dst_ref=lands[stage][k],
            send_sem=send_sem.at[stage, k], recv_sem=recv_sem.at[stage, k, 0],
            device_id=partner(dx, dy), device_id_type=mesh_id,
        )

    def detour(stage, k, v, route):
        return pltpu.make_async_remote_copy(
            src_ref=sends[stage][k].at[v], dst_ref=relay.at[stage, v],
            send_sem=send_sem.at[stage, k], recv_sem=relay_sem.at[stage, v],
            device_id=(place(k, route[0]), mate(route[1])), device_id_type=mesh_id,
        )

    def onward(stage, k, v, route):
        return pltpu.make_async_remote_copy(
            src_ref=relay.at[stage, v], dst_ref=lands[stage][k].at[v],
            send_sem=pass_sem.at[stage, v], recv_sem=recv_sem.at[stage, k, v],
            device_id=(ends[k][1], mate(route[1])), device_id_type=mesh_id,
        )

    posts = [place(k, route[0]) for k in range(2) for route in routes[0]]
    on_post = functools.reduce(jnp.logical_or, [me_c == c for c in posts]) & relaying

    def each_relay(stage, variables, run):
        def roles():
            for k in range(2):
                for route in routes[stage]:

                    def role(k=k, route=route):
                        for v in variables:
                            if route[2] <= v < route[3]:
                                run(k, v, route)

                    pl.when(me_c == place(k, route[0]))(role)

        pl.when(on_post)(roles)

    def forward(stage, variables):
        def hand_on(k, v, route):
            detour(stage, k, v, route).wait_recv()
            onward(stage, k, v, route).start()

        each_relay(stage, variables, hand_on)

    def forwarded(stage):
        each_relay(
            stage, range(count), lambda k, v, route: onward(stage, k, v, route).wait_send()
        )

    def launch(stage, axis, v):
        for k in (2 * axis, 2 * axis + 1):
            if axis == 1:
                message(stage, k, v).start()
                continue
            at_cut = me_c == ends[k][0]

            def cross(k=k):
                direct = me_c == ends[k][0]
                for route in routes[stage]:
                    takes = (detoured if route[1] else relaying) & (v >= route[2]) & (v < route[3])
                    direct = direct & jnp.logical_not(takes)
                    pl.when(takes)(lambda route=route: detour(stage, k, v, route).start())
                pl.when(direct)(lambda: message(stage, k, v).start())

            pl.when(at_cut)(cross)
            pl.when(reachable(ways[k][0]) & jnp.logical_not(at_cut))(
                lambda k=k: message(stage, k, v).start()
            )
        if axis == 0:
            for k in range(2):

                def mirror(k=k):
                    if stage == 0:
                        lands[0][1 - k][v] = jnp.zeros(lands[0][1 - k].shape[1:], jnp.float32)
                    else:
                        lands[1][1 - k][v] = -sends[1][k][v]

                pl.when(jnp.logical_not(reachable(ways[k][0])))(mirror)

    def arrived(stage, axis, v):
        for k in (2 * axis, 2 * axis + 1):
            guarded(reachable(-ways[k][0]), lambda k=k: message(stage, k, v).wait_recv())

    masks = [row_masks(axis, chords, spans, lanes) for axis in range(2)]
    outer = [[outer_rows(axis, chords, spans, last) for last in (False, True)] for axis in range(2)]

    def extract(stage, axis, v, f, ref, index):
        up, down = sends[stage][2 * axis], sends[stage][2 * axis + 1]
        down[v, f] = ref[index + (outer[axis][0],)]
        up[v, f] = ref[index[:-1] + (index[-1] + 1, outer[axis][1])]

    def gather(stage, axis, v, f, ref):
        up, down = lands[stage][2 * axis], lands[stage][2 * axis + 1]
        ref[axis, f, outer[axis][0]] = up[v, f]
        ref[axis, f, outer[axis][1]] = down[v, f]
        return ref[axis, f]

    def send_traces(axis, v):
        def body(q, carry):
            for j in range(5):
                f = 5 * q + j
                left, right = traces(fold([state[v, p] for p in points(axis, q, j)]))
                faces[axis, v, 2 * f] = left
                faces[axis, v, 2 * f + 1] = right
                extract(0, axis, v, f, faces, (axis, v, 2 * f))
            return carry

        lax.fori_loop(0, 5, body, 0)

    load(0).wait()
    eps = sensor(lambda p: state[0, p], work)
    lifted[1, 0] = eps
    for r in range(rows):
        halo[2 + r // spans, 2 + r % spans] = lifted[1, 0, pl.ds(r, 1)]
    send_traces(1, 0)
    send_traces(0, 0)
    sides = jnp.where(me_c > 0, 1, 0) + jnp.where(me_c + 1 < chord_size, 1, 0)
    pl.semaphore_wait(barrier, 2 + 3 * sides + extra)
    for dx, dy in offsets:
        guarded(reachable(dx), lambda dx=dx, dy=dy: eps_copy(dx, dy).start())
    launch(0, 0, 0)
    launch(0, 1, 0)

    def later_traces(v, carry):
        load(v).wait()
        for axis in range(2):
            send_traces(axis, v)
            launch(0, axis, v)
        return carry

    lax.fori_loop(1, count, later_traces, 0)

    lane = lax.broadcasted_iota(jnp.int32, (rows, lanes), 1)
    first, last = lane == 0, lane == lanes - 1

    row = lax.broadcasted_iota(jnp.int32, (rows, lanes), 0)
    closed_low = row < spans - jnp.where(me_c > 0, spans, 0)
    closed_high = row >= jnp.where(me_c + 1 < chord_size, rows, rows - spans)

    def inner(axis, left, right):
        low, high = masks[axis]
        step = spans if axis == 0 else 1
        before = jnp.where(low, 0.0, rolled(right, step, 0))
        return before, jnp.where(high, 0.0, rolled(left, -step, 0))

    def local_gradients(v, carry):
        def body(q, carry):
            for j in range(5):
                f = 5 * q + j
                for axis in range(3):
                    pts = points(axis, q, j)
                    parts = fold([state[v, p] for p in pts])
                    if axis == 2:
                        left, right = traces(parts)
                        before = jnp.where(first, left, rolled(right, 1, 1))
                        after = jnp.where(last, right, rolled(left, -1, 1))
                    else:
                        left, right = faces[axis, v, 2 * f], faces[axis, v, 2 * f + 1]
                        before, after = inner(axis, left, right)
                    if axis == 0:
                        before = jnp.where(closed_low, left, before)
                        after = jnp.where(closed_high, right, after)
                    for p, value in zip(pts, slope(parts, before, after)):
                        grad[axis, v, p] = value
            return carry

        lax.fori_loop(0, 5, body, 0, unroll=True)
        return carry

    lax.fori_loop(0, count, local_gradients, 0)

    for dx, dy in offsets:
        guarded(reachable(-dx), lambda dx=dx, dy=dy: eps_copy(dx, dy).wait_recv())
    forward(0, range(count))

    def shifted(x, y, slot):
        for r in range(rows):
            lifted[1, slot, pl.ds(r, 1)] = halo[2 + x + r // spans, 2 + y + r % spans]
        return lifted[1, slot]

    near = {(x, y): shifted(x, y, 3 * x + y + 4) for x in (-1, 0, 1) for y in (-1, 0, 1)}
    neighbours = [[near[x, y] for y in (-1, 0, 1)] for x in (-1, 0, 1)]
    corner = interpolate(neighbours, nu)
    near_weight = sum(float(LEFT[i] * HALF_LEFT[i] * (1.0 - NODES[i]) / 2.0) for i in range(5))
    far_weight = sum(float(LEFT[i] * HALF_LEFT[i] * (1.0 + NODES[i]) / 2.0) for i in range(5))
    slot = 9
    for axis in range(2):
        low = masks[axis][0]
        sign = jnp.where(low, -1.0, 1.0)
        lines = []
        for t in (-1, 0, 1):
            beyond = []
            for d in (-2, 2):
                x, y = (d, t) if axis == 0 else (t, d)
                beyond.append(shifted(x, y, slot))
                slot += 1
            close = [near[d, t] if axis == 0 else near[t, d] for d in (-1, 1)]
            lines.append(jnp.maximum(jnp.where(low, *beyond), jnp.where(low, *close)))
        weight = {}
        for t in range(2):
            far = along_lanes(jnp.maximum(lines[t], lines[t + 1]))
            for z in range(2):
                if axis == 0:
                    shared = jnp.where(low, corner[0, t, z], corner[1, t, z])
                else:
                    shared = jnp.where(low, corner[t, 0, z], corner[t, 1, z])
                value = sign * (near_weight * shared + far_weight * far[z])
                if axis == 0:
                    value = jnp.where(closed_low | closed_high, 0.0, value)
                weight[t, z] = value
        for m in range(5):
            edge = [LOWER[m] * weight[0, z] + UPPER[m] * weight[1, z] for z in range(2)]
            for c in range(5):
                beta[axis, 5 * m + c] = LOWER[c] * edge[0] + UPPER[c] * edge[1]

    def flux(axis, v):
        def body(q, carry):
            for j in range(5):
                f = 5 * q + j
                values = []
                for p in points(axis, q, j):
                    values.append(nu[p] * grad[axis, v, p])
                    grad[axis, v, p] = values[-1]
                left, right = traces(fold(values))
                work[2 * f] = left
                work[2 * f + 1] = right
                extract(1, axis, v, f, work, (2 * f,))
            return carry

        lax.fori_loop(0, 5, body, 0, unroll=True)

    def fluxes(v, carry):
        for axis in range(2):
            flux(axis, v)
            launch(1, axis, v)
        return carry

    lax.fori_loop(0, count, fluxes, 0)
    def normal(v, carry):
        def body(q, carry):
            for j in range(5):
                pts = points(2, q, j)
                parts = fold([nu[p] * grad[2, v, p] for p in pts])
                left, right = traces(parts)
                before = jnp.where(first, -left, rolled(right, 1, 1))
                after = jnp.where(last, -right, rolled(left, -1, 1))
                for p, value in zip(pts, slope(parts, before, after)):
                    acc[v, p] = value
            return carry

        lax.fori_loop(0, 5, body, 0, unroll=True)
        return carry

    lax.fori_loop(0, count, normal, 0)
    forward(1, range(longer))

    lift = [weights(axis, masks) for axis in range(2)]
    for f in range(25):
        lifted[0, f] = jnp.zeros((rows, lanes), jnp.float32)
        for axis in range(2):
            for p, w in zip(points(axis, f // 5, f % 5), lift[axis]):
                spread[axis, p] = nu[p] * w

    def divergence(v, carry):
        for axis in range(2):
            arrived(0, axis, v)

        def body(q, carry):
            for j in range(5):
                f = 5 * q + j
                for axis in range(2):
                    pts = points(axis, q, j)
                    ghost = gather(0, axis, v, f, lifted)
                    parts = fold([grad[axis, v, p] + spread[axis, p] * ghost for p in pts])
                    before, after = inner(axis, *traces(parts))
                    for p, value in zip(pts, slope(parts, before, after)):
                        acc[v, p] += value
            return carry

        lax.fori_loop(0, 5, body, 0, unroll=True)
        for w in range(longer, count):
            pl.when(v == w - 1)(lambda w=w: forward(1, (w,)))
        return carry

    lax.fori_loop(0, count, divergence, 0)

    def correct(v, carry):
        for axis in range(2):
            arrived(1, axis, v)
        for f in range(25):
            for axis in range(2):
                gather(1, axis, v, f, lifted)

        def outer_flux(axis, f):
            own = jnp.where(masks[axis][0], faces[axis, v, 2 * f], faces[axis, v, 2 * f + 1])
            return lifted[axis, f] + beta[axis, f] * own

        for c in range(5):
            across = [outer_flux(0, 5 * b + c) for b in range(5)]
            for a in range(5):
                along = outer_flux(1, 5 * a + c)
                for b in range(5):
                    acc[v, 25 * a + 5 * b + c] += lift[0][a] * across[b] + lift[1][b] * along
        return carry

    lax.fori_loop(0, count, correct, 0)

    for dx, dy in offsets:
        guarded(reachable(dx), lambda dx=dx, dy=dy: eps_copy(dx, dy).wait_send())
    for stage in range(2):
        for k in range(4):
            guarded(reachable(ways[k][0]), lambda stage=stage, k=k: sent(stage, k).wait_send())
        forwarded(stage)


def shards(state):
    count, npts, chords, spans, lanes = state.shape
    rows = chords * spans
    flat = state.reshape(count, npts, rows, lanes)
    f32 = jnp.float32
    sizes = (lax.axis_size("chord"), lax.axis_size("span"))

    def message(n, k):
        return (n, 25, spans if k < 2 else chords, lanes)

    def full(*shape):
        return jax.ShapeDtypeStruct(shape, f32)

    vmem = pl.BlockSpec(memory_space=pltpu.VMEM)
    nu, residual = pl.pallas_call(
        functools.partial(local_kernel, sizes, count, chords, spans),
        in_specs=[pl.BlockSpec(memory_space=pltpu.HBM)],
        out_specs=[vmem, vmem],
        out_shape=[full(npts, rows, lanes), full(count, npts, rows, lanes)],
        scratch_shapes=[
            pltpu.VMEM(shape, f32)
            for shape in [
                (count, npts, rows, lanes),
                (3, count, npts, rows, lanes),
                (chords + 4, spans + 4, 1, lanes),
                (npts, rows, lanes),
                (2, count, 50, rows, lanes),
                (2, 25, rows, lanes),
                (2, 25, rows, lanes),
                (2, npts, rows, lanes),
                (2, *message(count, 0)),
            ]
            + [message(count, k) for k in range(4)] * 4
        ]
        + [
            pltpu.SemaphoreType.DMA((count,)),
            pltpu.SemaphoreType.DMA((9,)),
            pltpu.SemaphoreType.DMA((9,)),
            pltpu.SemaphoreType.DMA((2, 4)),
            pltpu.SemaphoreType.DMA((2, 4, count)),
            pltpu.SemaphoreType.DMA((2, count)),
            pltpu.SemaphoreType.DMA((2, count)),
        ],
        compiler_params=pltpu.CompilerParams(
            collective_id=0, has_side_effects=True, vmem_limit_bytes=VMEM_BYTES
        ),
    )(flat)
    return residual.reshape(state.shape), nu.reshape(npts, chords, spans, lanes)


def solution(mesh):
    in_specs = (P(None, None, "chord", "span", None),)
    out_specs = (P(None, None, "chord", "span", None), P(None, "chord", "span", None))
    return jax.shard_map(shards, mesh=mesh, in_specs=in_specs, out_specs=out_specs, check_vma=False)
```

```python
import functools
import math

import jax
import jax.numpy as jnp
import numpy as np
from jax import lax
from jax.experimental import pallas as pl
from jax.experimental.pallas import tpu as pltpu
from jax.sharding import PartitionSpec as P

VMEM_BYTES = 52_500_000
EPS_SCALE = 0.01
SENSOR_CENTRE = -3.0
SENSOR_WIDTH = 1.5
RATIO_FLOOR = 1e-06
ENERGY_EPS = 1e-06
GAUSS_NODES = [-0.906179845938664, -0.5384693101056831, 0.0, 0.5384693101056831, 0.906179845938664]
GAUSS_WEIGHTS = [
    0.2369268850561891,
    0.4786286704993665,
    0.5688888888888889,
    0.4786286704993665,
    0.2369268850561891,
]


def legendre_values(points):
    values = [np.ones(points.shape), np.array(points)]
    for order in range(1, 5):
        values.append(
            ((2 * order + 1) * points * values[order] - order * values[order - 1]) / (order + 1)
        )
    return values


def line_tables():
    line_nodes = np.array(GAUSS_NODES)
    quadrature_weights = np.array(GAUSS_WEIGHTS)
    barycentric = np.array(
        [
            1.0 / np.prod([line_nodes[j] - line_nodes[k] for k in range(5) if k != j])
            for j in range(5)
        ]
    )
    derivative = np.zeros((5, 5))
    for i in range(5):
        for j in range(5):
            if i != j:
                derivative[i, j] = barycentric[j] / barycentric[i] / (line_nodes[i] - line_nodes[j])
        derivative[i, i] = -np.sum(derivative[i])
    left_values = np.ones(5)
    right_values = np.ones(5)
    for j in range(5):
        for k in range(5):
            if k != j:
                left_values[j] *= (-1.0 - line_nodes[k]) / (line_nodes[j] - line_nodes[k])
                right_values[j] *= (1.0 - line_nodes[k]) / (line_nodes[j] - line_nodes[k])
    legendre = legendre_values(line_nodes)
    fourth_slope = 7.0 * legendre[3] + 3.0 * legendre[1]
    fifth_slope = 9.0 * legendre[4] + 5.0 * legendre[2] + legendre[0]
    left_corr = 0.5 * (fourth_slope - fifth_slope)
    right_corr = 0.5 * (fourth_slope + fifth_slope)
    modal = np.zeros((5, 5))
    for k in range(5):
        modal[k, :] = quadrature_weights * math.sqrt((2 * k + 1) / 2.0) * legendre[k]
    return (line_nodes, derivative, left_values, right_values, left_corr, right_corr, modal)


NODES, DERIV, LEFT, RIGHT, LIFT_LEFT, LIFT_RIGHT, MODAL = line_tables()
HALF_LEFT = 0.5 * LIFT_LEFT
HALF_RIGHT = 0.5 * LIFT_RIGHT


def fold(u):
    return (u[0] + u[4], u[1] + u[3], u[2], u[0] - u[4], u[1] - u[3])


def traces(parts):
    s0, s1, mid, d0, d1 = parts
    r = [float(x) for x in RIGHT]
    even = 0.5 * (r[0] + r[4]) * s0 + 0.5 * (r[1] + r[3]) * s1 + r[2] * mid
    odd = 0.5 * (r[0] - r[4]) * d0 + 0.5 * (r[1] - r[3]) * d1
    return even - odd, even + odd


def slope(parts, before, after):
    s0, s1, mid, d0, d1 = parts
    h = [float(x) for x in HALF_LEFT]
    r = [float(x) for x in RIGHT]
    if before is not None:
        diff, both = before - after, before + after
    even, odd = [], []
    for i in range(3):
        lift = 0.5 * (h[i] + h[4 - i])
        value = (
            float(0.5 * (DERIV[i, 0] - DERIV[i, 4]) + lift * (r[0] - r[4])) * d0
            + float(0.5 * (DERIV[i, 1] - DERIV[i, 3]) + lift * (r[1] - r[3])) * d1
        )
        even.append(value if before is None else value + lift * diff)
    for i in range(2):
        lift = 0.5 * (h[i] - h[4 - i])
        value = (
            float(0.5 * (DERIV[i, 0] + DERIV[i, 4]) - lift * (r[0] + r[4])) * s0
            + float(0.5 * (DERIV[i, 1] + DERIV[i, 3]) - lift * (r[1] + r[3])) * s1
            + float(DERIV[i, 2] - 2.0 * lift * r[2]) * mid
        )
        odd.append(value if before is None else value + lift * both)
    return [even[0] + odd[0], even[1] + odd[1], even[2], even[1] - odd[1], even[0] - odd[0]]


def points(axis, q, j):
    if axis == 0:
        return [25 * i + 5 * q + j for i in range(5)]
    if axis == 1:
        return [25 * q + 5 * i + j for i in range(5)]
    return [25 * q + 5 * j + i for i in range(5)]


def modal_line(u):
    s0, s1, mid, d0, d1 = fold(u)
    out = []
    for k in range(5):
        m = [float(x) for x in MODAL[k]]
        out.append(m[0] * s0 + m[1] * s1 + m[2] * mid if k % 2 == 0 else m[0] * d0 + m[1] * d1)
    return out


def sensor(load, work):
    def first(q, carry):
        for j in range(5):
            pts = points(0, q, j)
            for i, value in zip(pts, modal_line([load(p) for p in pts])):
                work[i] = value
        return carry

    lax.fori_loop(0, 5, first, 0)

    def second(q, carry):
        total, high = carry
        plane = {}
        for c in range(5):
            for b, value in enumerate(modal_line([work[25 * q + 5 * b + c] for b in range(5)])):
                plane[b, c] = value
        low = jnp.zeros_like(total)
        edge = jnp.zeros_like(total)
        for b in range(5):
            line = modal_line([plane[b, c] for c in range(5)])
            squares = [x * x for x in line]
            if b < 4:
                low = low + ((squares[0] + squares[1]) + (squares[2] + squares[3]))
                edge = edge + squares[4]
            else:
                edge = edge + ((squares[0] + squares[1]) + (squares[2] + squares[3])) + squares[4]
        plane_total = low + edge
        return total + plane_total, high + jnp.where(q == 4, plane_total, edge)

    zero = jnp.zeros(work.shape[1:], jnp.float32)
    total, high = lax.fori_loop(0, 5, second, (zero, zero))
    level = jnp.log(jnp.maximum(high / (total + ENERGY_EPS), RATIO_FLOOR)) * (1.0 / math.log(10.0))
    ramp = jnp.clip((level - SENSOR_CENTRE) / SENSOR_WIDTH, -1.0, 1.0)
    return EPS_SCALE * 0.5 * (1.0 + jnp.sin(0.5 * math.pi * ramp))


def rolled(value, shift, axis):
    size = value.shape[axis]
    return pltpu.roll(value, shift % size, axis)


LOWER = [float((1.0 - x) / 2.0) for x in NODES]
UPPER = [float((1.0 + x) / 2.0) for x in NODES]


def along_lanes(line):
    lanes = line.shape[1]
    lane = lax.broadcasted_iota(jnp.int32, line.shape, 1)
    before = jnp.where(lane == 0, 0.0, rolled(line, 1, 1))
    after = jnp.where(lane == lanes - 1, 0.0, rolled(line, -1, 1))
    return jnp.maximum(line, before), jnp.maximum(line, after)


def interpolate(neighbours, nu):
    corner = {}
    for x in range(2):
        for y in range(2):
            line = jnp.maximum(
                jnp.maximum(neighbours[x][y], neighbours[x + 1][y]),
                jnp.maximum(neighbours[x][y + 1], neighbours[x + 1][y + 1]),
            )
            corner[x, y, 0], corner[x, y, 1] = along_lanes(line)
    lower, upper = LOWER, UPPER
    for a in range(5):
        face = {
            (y, z): lower[a] * corner[0, y, z] + upper[a] * corner[1, y, z]
            for y in range(2)
            for z in range(2)
        }
        for b in range(5):
            edge = [lower[b] * face[0, z] + upper[b] * face[1, z] for z in range(2)]
            for c in range(5):
                nu[25 * a + 5 * b + c] = lower[c] * edge[0] + upper[c] * edge[1]
    return corner


def row_masks(axis, chords, spans, lanes):
    row = lax.broadcasted_iota(jnp.int32, (chords * spans, lanes), 0)
    if axis == 0:
        return row < spans, row >= (chords - 1) * spans
    place = row % spans
    return place == 0, place == spans - 1


def outer_rows(axis, chords, spans, last):
    if axis == 0:
        return pl.ds((chords - 1) * spans if last else 0, spans)
    return pl.ds(spans - 1 if last else 0, chords, spans)


def weights(axis, masks):
    low, high = masks[axis]
    return [
        jnp.where(low, float(HALF_LEFT[i]), jnp.where(high, float(HALF_RIGHT[i]), 0.0))
        for i in range(5)
    ]


def local_kernel(sizes, count, chords, spans, *refs):
    state_hbm = refs[0]
    nu, acc = refs[1:3]
    state, grad, halo, work, faces, lifted, beta, spread, relay = refs[3:12]
    sends = (refs[12:16], refs[16:20])
    lands = (refs[20:24], refs[24:28])
    load_sem, eps_send, eps_recv, send_sem, recv_sem, relay_sem, pass_sem = refs[28:]
    rows, lanes = nu.shape[1:]
    chord_size, span_size = sizes
    me_c, me_s = lax.axis_index("chord"), lax.axis_index("span")
    mesh_id = pl.DeviceIdType.MESH

    def reachable(dx):
        if dx == 0:
            return None
        return me_c + 1 < chord_size if dx == 1 else me_c > 0

    def guarded(cond, run):
        if cond is None:
            run()
        else:
            pl.when(cond)(run)

    def partner(dx, dy):
        return (me_c + dx, lax.rem(me_s + dy + span_size, span_size))

    cut, final = chord_size // 2, chord_size - 1
    ends = ((cut - 1, cut), (cut, cut - 1))
    twin = me_s + 1 - 2 * lax.rem(me_s, 2)
    detoured = lax.rem((me_s + 1) // 2, 2) == 1
    relaying = jnp.logical_not(detoured)
    longer = 2
    routes = (
        ((0, True, 0, longer), (1, True, longer, count), (2, False, longer, count)),
        ((0, True, 0, count),),
    )

    def place(k, depth):
        return depth if k == 0 else final - depth

    def mate(twinned):
        return twin if twinned else me_s

    offsets = [(dx, dy) for dx in (0, -1, 1) for dy in (-1, 0, 1) if (dx, dy) != (0, 0)]
    for r in range(chords + 4):
        for q in range(spans + 4):
            halo[r, q] = jnp.zeros((1, lanes), jnp.float32)
    barrier = pltpu.get_barrier_semaphore()
    for dx, dy in offsets:

        def greet(dx=dx, dy=dy):
            pl.semaphore_signal(barrier, inc=1, device_id=partner(dx, dy), device_id_type=mesh_id)

        guarded(reachable(dx), greet)

    extra = 0
    for k, (source, target) in enumerate(ends):
        for depth, twinned, _, _ in routes[0]:
            through = place(k, depth)
            sender = detoured if twinned else relaying
            hops = [(target, sender, through, relaying)]
            if twinned:
                hops.append((through, relaying, source, sender))
            for here, ready, there, awaiting in hops:

                def greet_relay(there=there, twinned=twinned):
                    pl.semaphore_signal(
                        barrier, inc=1, device_id=(there, mate(twinned)), device_id_type=mesh_id
                    )

                pl.when((me_c == here) & ready)(greet_relay)
                extra += jnp.where((me_c == there) & awaiting, 1, 0)

    def load(v):
        return pltpu.make_async_copy(state_hbm.at[v], state.at[v], load_sem.at[v])

    for v in range(count):
        load(v).start()

    def layer(d, length, inside):
        if d == 0:
            return pl.ds(2, length)
        if inside:
            return pl.ds(length if d == 1 else 2, 2)
        return pl.ds(0 if d == 1 else length + 2, 2)

    def eps_copy(dx, dy):
        slot = 3 * (dx + 1) + dy + 1
        return pltpu.make_async_remote_copy(
            src_ref=halo.at[layer(dx, chords, True), layer(dy, spans, True)],
            dst_ref=halo.at[layer(dx, chords, False), layer(dy, spans, False)],
            send_sem=eps_send.at[slot], recv_sem=eps_recv.at[8 - slot],
            device_id=partner(dx, dy), device_id_type=mesh_id,
        )

    ways = ((1, 0), (-1, 0), (0, 1), (0, -1))

    def message(stage, k, v):
        dx, dy = ways[k]
        return pltpu.make_async_remote_copy(
            src_ref=sends[stage][k].at[v], dst_ref=lands[stage][k].at[v],
            send_sem=send_sem.at[stage, k], recv_sem=recv_sem.at[stage, k, v],
            device_id=partner(dx, dy), device_id_type=mesh_id,
        )

    def sent(stage, k):
        dx, dy = ways[k]
        return pltpu.make_async_remote_copy(
            src_ref=sends[stage][k], dst_ref=lands[stage][k],
            send_sem=send_sem.at[stage, k], recv_sem=recv_sem.at[stage, k, 0],
            device_id=partner(dx, dy), device_id_type=mesh_id,
        )

    def detour(stage, k, v, route):
        return pltpu.make_async_remote_copy(
            src_ref=sends[stage][k].at[v], dst_ref=relay.at[stage, v],
            send_sem=send_sem.at[stage, k], recv_sem=relay_sem.at[stage, v],
            device_id=(place(k, route[0]), mate(route[1])), device_id_type=mesh_id,
        )

    def onward(stage, k, v, route):
        return pltpu.make_async_remote_copy(
            src_ref=relay.at[stage, v], dst_ref=lands[stage][k].at[v],
            send_sem=pass_sem.at[stage, v], recv_sem=recv_sem.at[stage, k, v],
            device_id=(ends[k][1], mate(route[1])), device_id_type=mesh_id,
        )

    posts = [place(k, route[0]) for k in range(2) for route in routes[0]]
    on_post = functools.reduce(jnp.logical_or, [me_c == c for c in posts]) & relaying

    def each_relay(stage, variables, run):
        def roles():
            for k in range(2):
                for route in routes[stage]:

                    def role(k=k, route=route):
                        for v in variables:
                            if route[2] <= v < route[3]:
                                run(k, v, route)

                    pl.when(me_c == place(k, route[0]))(role)

        pl.when(on_post)(roles)

    def forward(stage, variables):
        def hand_on(k, v, route):
            detour(stage, k, v, route).wait_recv()
            onward(stage, k, v, route).start()

        each_relay(stage, variables, hand_on)

    def forwarded(stage):
        each_relay(
            stage, range(count), lambda k, v, route: onward(stage, k, v, route).wait_send()
        )

    def launch(stage, axis, v):
        for k in (2 * axis, 2 * axis + 1):
            if axis == 1:
                message(stage, k, v).start()
                continue
            at_cut = me_c == ends[k][0]

            def cross(k=k):
                direct = me_c == ends[k][0]
                for route in routes[stage]:
                    takes = (detoured if route[1] else relaying) & (v >= route[2]) & (v < route[3])
                    direct = direct & jnp.logical_not(takes)
                    pl.when(takes)(lambda route=route: detour(stage, k, v, route).start())
                pl.when(direct)(lambda: message(stage, k, v).start())

            pl.when(at_cut)(cross)
            pl.when(reachable(ways[k][0]) & jnp.logical_not(at_cut))(
                lambda k=k: message(stage, k, v).start()
            )
        if axis == 0:
            for k in range(2):

                def mirror(k=k):
                    if stage == 0:
                        lands[0][1 - k][v] = jnp.zeros(lands[0][1 - k].shape[1:], jnp.float32)
                    else:
                        lands[1][1 - k][v] = -sends[1][k][v]

                pl.when(jnp.logical_not(reachable(ways[k][0])))(mirror)

    def arrived(stage, axis, v):
        for k in (2 * axis, 2 * axis + 1):
            guarded(reachable(-ways[k][0]), lambda k=k: message(stage, k, v).wait_recv())

    masks = [row_masks(axis, chords, spans, lanes) for axis in range(2)]
    outer = [[outer_rows(axis, chords, spans, last) for last in (False, True)] for axis in range(2)]

    def extract(stage, axis, v, f, ref, index):
        up, down = sends[stage][2 * axis], sends[stage][2 * axis + 1]
        down[v, f] = ref[index + (outer[axis][0],)]
        up[v, f] = ref[index[:-1] + (index[-1] + 1, outer[axis][1])]

    def gather(stage, axis, v, f, ref):
        up, down = lands[stage][2 * axis], lands[stage][2 * axis + 1]
        ref[axis, f, outer[axis][0]] = up[v, f]
        ref[axis, f, outer[axis][1]] = down[v, f]
        return ref[axis, f]

    def send_traces(axis, v):
        def body(q, carry):
            for j in range(5):
                f = 5 * q + j
                left, right = traces(fold([state[v, p] for p in points(axis, q, j)]))
                faces[axis, v, 2 * f] = left
                faces[axis, v, 2 * f + 1] = right
                extract(0, axis, v, f, faces, (axis, v, 2 * f))
            return carry

        lax.fori_loop(0, 5, body, 0)

    load(0).wait()
    eps = sensor(lambda p: state[0, p], work)
    lifted[1, 0] = eps
    for r in range(rows):
        halo[2 + r // spans, 2 + r % spans] = lifted[1, 0, pl.ds(r, 1)]
    send_traces(1, 0)
    send_traces(0, 0)
    sides = jnp.where(me_c > 0, 1, 0) + jnp.where(me_c + 1 < chord_size, 1, 0)
    pl.semaphore_wait(barrier, 2 + 3 * sides + extra)
    for dx, dy in offsets:
        guarded(reachable(dx), lambda dx=dx, dy=dy: eps_copy(dx, dy).start())
    launch(0, 0, 0)
    launch(0, 1, 0)

    def later_traces(v, carry):
        load(v).wait()
        for axis in range(2):
            send_traces(axis, v)
            launch(0, axis, v)
        return carry

    lax.fori_loop(1, count, later_traces, 0)

    lane = lax.broadcasted_iota(jnp.int32, (rows, lanes), 1)
    first, last = lane == 0, lane == lanes - 1

    row = lax.broadcasted_iota(jnp.int32, (rows, lanes), 0)
    closed_low = row < spans - jnp.where(me_c > 0, spans, 0)
    closed_high = row >= jnp.where(me_c + 1 < chord_size, rows, rows - spans)

    def inner(axis, left, right):
        low, high = masks[axis]
        step = spans if axis == 0 else 1
        before = jnp.where(low, 0.0, rolled(right, step, 0))
        return before, jnp.where(high, 0.0, rolled(left, -step, 0))

    def local_gradients(v, carry):
        def body(q, carry):
            for j in range(5):
                f = 5 * q + j
                for axis in range(3):
                    pts = points(axis, q, j)
                    parts = fold([state[v, p] for p in pts])
                    if axis == 2:
                        left, right = traces(parts)
                        before = jnp.where(first, left, rolled(right, 1, 1))
                        after = jnp.where(last, right, rolled(left, -1, 1))
                    else:
                        left, right = faces[axis, v, 2 * f], faces[axis, v, 2 * f + 1]
                        before, after = inner(axis, left, right)
                    if axis == 0:
                        before = jnp.where(closed_low, left, before)
                        after = jnp.where(closed_high, right, after)
                    for p, value in zip(pts, slope(parts, before, after)):
                        grad[axis, v, p] = value
            return carry

        lax.fori_loop(0, 5, body, 0, unroll=True)
        return carry

    lax.fori_loop(0, count, local_gradients, 0)

    for dx, dy in offsets:
        guarded(reachable(-dx), lambda dx=dx, dy=dy: eps_copy(dx, dy).wait_recv())
    forward(0, range(3))

    def shifted(x, y, slot):
        for r in range(rows):
            lifted[1, slot, pl.ds(r, 1)] = halo[2 + x + r // spans, 2 + y + r % spans]
        return lifted[1, slot]

    near = {(x, y): shifted(x, y, 3 * x + y + 4) for x in (-1, 0, 1) for y in (-1, 0, 1)}
    neighbours = [[near[x, y] for y in (-1, 0, 1)] for x in (-1, 0, 1)]
    corner = interpolate(neighbours, nu)
    near_weight = sum(float(LEFT[i] * HALF_LEFT[i] * (1.0 - NODES[i]) / 2.0) for i in range(5))
    far_weight = sum(float(LEFT[i] * HALF_LEFT[i] * (1.0 + NODES[i]) / 2.0) for i in range(5))
    slot = 9
    for axis in range(2):
        low = masks[axis][0]
        sign = jnp.where(low, -1.0, 1.0)
        lines = []
        for t in (-1, 0, 1):
            beyond = []
            for d in (-2, 2):
                x, y = (d, t) if axis == 0 else (t, d)
                beyond.append(shifted(x, y, slot))
                slot += 1
            close = [near[d, t] if axis == 0 else near[t, d] for d in (-1, 1)]
            lines.append(jnp.maximum(jnp.where(low, *beyond), jnp.where(low, *close)))
        weight = {}
        for t in range(2):
            far = along_lanes(jnp.maximum(lines[t], lines[t + 1]))
            for z in range(2):
                if axis == 0:
                    shared = jnp.where(low, corner[0, t, z], corner[1, t, z])
                else:
                    shared = jnp.where(low, corner[t, 0, z], corner[t, 1, z])
                value = sign * (near_weight * shared + far_weight * far[z])
                if axis == 0:
                    value = jnp.where(closed_low | closed_high, 0.0, value)
                weight[t, z] = value
        for m in range(5):
            edge = [LOWER[m] * weight[0, z] + UPPER[m] * weight[1, z] for z in range(2)]
            for c in range(5):
                beta[axis, 5 * m + c] = LOWER[c] * edge[0] + UPPER[c] * edge[1]

    def flux(axis, v):
        def body(q, carry):
            for j in range(5):
                f = 5 * q + j
                values = []
                for p in points(axis, q, j):
                    values.append(nu[p] * grad[axis, v, p])
                    grad[axis, v, p] = values[-1]
                left, right = traces(fold(values))
                work[2 * f] = left
                work[2 * f + 1] = right
                extract(1, axis, v, f, work, (2 * f,))
            return carry

        lax.fori_loop(0, 5, body, 0, unroll=True)

    def fluxes(v, carry):
        for axis in range(2):
            flux(axis, v)
            launch(1, axis, v)
        return carry

    lax.fori_loop(0, count, fluxes, 0)
    forward(0, range(3, count))
    def normal(v, carry):
        def body(q, carry):
            for j in range(5):
                pts = points(2, q, j)
                parts = fold([nu[p] * grad[2, v, p] for p in pts])
                left, right = traces(parts)
                before = jnp.where(first, -left, rolled(right, 1, 1))
                after = jnp.where(last, -right, rolled(left, -1, 1))
                for p, value in zip(pts, slope(parts, before, after)):
                    acc[v, p] = value
            return carry

        lax.fori_loop(0, 5, body, 0, unroll=True)
        return carry

    lax.fori_loop(0, count, normal, 0)
    forward(1, range(2))

    lift = [weights(axis, masks) for axis in range(2)]
    for f in range(25):
        lifted[0, f] = jnp.zeros((rows, lanes), jnp.float32)
        for axis in range(2):
            for p, w in zip(points(axis, f // 5, f % 5), lift[axis]):
                spread[axis, p] = nu[p] * w

    def divergence(v, carry):
        for axis in range(2):
            arrived(0, axis, v)

        def body(q, carry):
            for j in range(5):
                f = 5 * q + j
                for axis in range(2):
                    pts = points(axis, q, j)
                    ghost = gather(0, axis, v, f, lifted)
                    parts = fold([grad[axis, v, p] + spread[axis, p] * ghost for p in pts])
                    before, after = inner(axis, *traces(parts))
                    for p, value in zip(pts, slope(parts, before, after)):
                        acc[v, p] += value
            return carry

        lax.fori_loop(0, 5, body, 0, unroll=True)
        for w in range(2, count):
            pl.when(v == w - 1)(lambda w=w: forward(1, (w,)))
        return carry

    lax.fori_loop(0, count, divergence, 0)

    def correct(v, carry):
        for axis in range(2):
            arrived(1, axis, v)
        for f in range(25):
            for axis in range(2):
                gather(1, axis, v, f, lifted)

        def outer_flux(axis, f):
            own = jnp.where(masks[axis][0], faces[axis, v, 2 * f], faces[axis, v, 2 * f + 1])
            return lifted[axis, f] + beta[axis, f] * own

        for c in range(5):
            across = [outer_flux(0, 5 * b + c) for b in range(5)]
            for a in range(5):
                along = outer_flux(1, 5 * a + c)
                for b in range(5):
                    acc[v, 25 * a + 5 * b + c] += lift[0][a] * across[b] + lift[1][b] * along
        return carry

    lax.fori_loop(0, count, correct, 0)

    for dx, dy in offsets:
        guarded(reachable(dx), lambda dx=dx, dy=dy: eps_copy(dx, dy).wait_send())
    for stage in range(2):
        for k in range(4):
            guarded(reachable(ways[k][0]), lambda stage=stage, k=k: sent(stage, k).wait_send())
        forwarded(stage)


def write_kernel(nu, residual, nu_hbm, residual_hbm, sems):
    copies = [
        pltpu.make_async_copy(residual.at[v], residual_hbm.at[v], sems.at[v])
        for v in range(residual.shape[0])
    ]
    copies.append(pltpu.make_async_copy(nu, nu_hbm, sems.at[residual.shape[0]]))
    for copy in copies:
        copy.start()
    for copy in copies:
        copy.wait()


def shards(state):
    count, npts, chords, spans, lanes = state.shape
    rows = chords * spans
    flat = state.reshape(count, npts, rows, lanes)
    f32 = jnp.float32
    sizes = (lax.axis_size("chord"), lax.axis_size("span"))

    def message(n, k):
        return (n, 25, spans if k < 2 else chords, lanes)

    def full(*shape):
        return jax.ShapeDtypeStruct(shape, f32)

    vmem = pl.BlockSpec(memory_space=pltpu.VMEM)
    nu, residual = pl.pallas_call(
        functools.partial(local_kernel, sizes, count, chords, spans),
        in_specs=[pl.BlockSpec(memory_space=pltpu.HBM)],
        out_specs=[vmem, vmem],
        out_shape=[full(npts, rows, lanes), full(count, npts, rows, lanes)],
        scratch_shapes=[
            pltpu.VMEM(shape, f32)
            for shape in [
                (count, npts, rows, lanes),
                (3, count, npts, rows, lanes),
                (chords + 4, spans + 4, 1, lanes),
                (npts, rows, lanes),
                (2, count, 50, rows, lanes),
                (2, 25, rows, lanes),
                (2, 25, rows, lanes),
                (2, npts, rows, lanes),
                (2, *message(count, 0)),
            ]
            + [message(count, k) for k in range(4)] * 4
        ]
        + [
            pltpu.SemaphoreType.DMA((count,)),
            pltpu.SemaphoreType.DMA((9,)),
            pltpu.SemaphoreType.DMA((9,)),
            pltpu.SemaphoreType.DMA((2, 4)),
            pltpu.SemaphoreType.DMA((2, 4, count)),
            pltpu.SemaphoreType.DMA((2, count)),
            pltpu.SemaphoreType.DMA((2, count)),
        ],
        compiler_params=pltpu.CompilerParams(
            collective_id=0, has_side_effects=True, vmem_limit_bytes=VMEM_BYTES
        ),
    )(flat)
    hbm = pl.BlockSpec(memory_space=pltpu.HBM)
    nu, residual = pl.pallas_call(
        write_kernel,
        in_specs=[vmem, vmem],
        out_specs=[hbm, hbm],
        out_shape=[full(npts, rows, lanes), full(count, npts, rows, lanes)],
        scratch_shapes=[pltpu.SemaphoreType.DMA((count + 1,))],
        compiler_params=pltpu.CompilerParams(vmem_limit_bytes=1_000_000),
    )(nu, residual)
    return residual.reshape(state.shape), nu.reshape(npts, chords, spans, lanes)


def solution(mesh):
    in_specs = (P(None, None, "chord", "span", None),)
    out_specs = (P(None, None, "chord", "span", None), P(None, "chord", "span", None))
    return jax.shard_map(shards, mesh=mesh, in_specs=in_specs, out_specs=out_specs, check_vma=False)
```

```python
import functools
import math

import jax
import jax.numpy as jnp
import numpy as np
from jax import lax
from jax.experimental import pallas as pl
from jax.experimental.pallas import tpu as pltpu
from jax.sharding import PartitionSpec as P

VMEM_BYTES = 52_500_000
EPS_SCALE = 0.01
SENSOR_CENTRE = -3.0
SENSOR_WIDTH = 1.5
RATIO_FLOOR = 1e-06
ENERGY_EPS = 1e-06
GAUSS_NODES = [-0.906179845938664, -0.5384693101056831, 0.0, 0.5384693101056831, 0.906179845938664]
GAUSS_WEIGHTS = [
    0.2369268850561891,
    0.4786286704993665,
    0.5688888888888889,
    0.4786286704993665,
    0.2369268850561891,
]


def legendre_values(points):
    values = [np.ones(points.shape), np.array(points)]
    for order in range(1, 5):
        values.append(
            ((2 * order + 1) * points * values[order] - order * values[order - 1]) / (order + 1)
        )
    return values


def line_tables():
    line_nodes = np.array(GAUSS_NODES)
    quadrature_weights = np.array(GAUSS_WEIGHTS)
    barycentric = np.array(
        [
            1.0 / np.prod([line_nodes[j] - line_nodes[k] for k in range(5) if k != j])
            for j in range(5)
        ]
    )
    derivative = np.zeros((5, 5))
    for i in range(5):
        for j in range(5):
            if i != j:
                derivative[i, j] = barycentric[j] / barycentric[i] / (line_nodes[i] - line_nodes[j])
        derivative[i, i] = -np.sum(derivative[i])
    left_values = np.ones(5)
    right_values = np.ones(5)
    for j in range(5):
        for k in range(5):
            if k != j:
                left_values[j] *= (-1.0 - line_nodes[k]) / (line_nodes[j] - line_nodes[k])
                right_values[j] *= (1.0 - line_nodes[k]) / (line_nodes[j] - line_nodes[k])
    legendre = legendre_values(line_nodes)
    fourth_slope = 7.0 * legendre[3] + 3.0 * legendre[1]
    fifth_slope = 9.0 * legendre[4] + 5.0 * legendre[2] + legendre[0]
    left_corr = 0.5 * (fourth_slope - fifth_slope)
    right_corr = 0.5 * (fourth_slope + fifth_slope)
    modal = np.zeros((5, 5))
    for k in range(5):
        modal[k, :] = quadrature_weights * math.sqrt((2 * k + 1) / 2.0) * legendre[k]
    return (line_nodes, derivative, left_values, right_values, left_corr, right_corr, modal)


NODES, DERIV, LEFT, RIGHT, LIFT_LEFT, LIFT_RIGHT, MODAL = line_tables()
HALF_LEFT = 0.5 * LIFT_LEFT
HALF_RIGHT = 0.5 * LIFT_RIGHT


def fold(u):
    return (u[0] + u[4], u[1] + u[3], u[2], u[0] - u[4], u[1] - u[3])


def traces(parts):
    s0, s1, mid, d0, d1 = parts
    r = [float(x) for x in RIGHT]
    even = 0.5 * (r[0] + r[4]) * s0 + 0.5 * (r[1] + r[3]) * s1 + r[2] * mid
    odd = 0.5 * (r[0] - r[4]) * d0 + 0.5 * (r[1] - r[3]) * d1
    return even - odd, even + odd


def slope(parts, before, after):
    s0, s1, mid, d0, d1 = parts
    h = [float(x) for x in HALF_LEFT]
    r = [float(x) for x in RIGHT]
    if before is not None:
        diff, both = before - after, before + after
    even, odd = [], []
    for i in range(3):
        lift = 0.5 * (h[i] + h[4 - i])
        value = (
            float(0.5 * (DERIV[i, 0] - DERIV[i, 4]) + lift * (r[0] - r[4])) * d0
            + float(0.5 * (DERIV[i, 1] - DERIV[i, 3]) + lift * (r[1] - r[3])) * d1
        )
        even.append(value if before is None else value + lift * diff)
    for i in range(2):
        lift = 0.5 * (h[i] - h[4 - i])
        value = (
            float(0.5 * (DERIV[i, 0] + DERIV[i, 4]) - lift * (r[0] + r[4])) * s0
            + float(0.5 * (DERIV[i, 1] + DERIV[i, 3]) - lift * (r[1] + r[3])) * s1
            + float(DERIV[i, 2] - 2.0 * lift * r[2]) * mid
        )
        odd.append(value if before is None else value + lift * both)
    return [even[0] + odd[0], even[1] + odd[1], even[2], even[1] - odd[1], even[0] - odd[0]]


def points(axis, q, j):
    if axis == 0:
        return [25 * i + 5 * q + j for i in range(5)]
    if axis == 1:
        return [25 * q + 5 * i + j for i in range(5)]
    return [25 * q + 5 * j + i for i in range(5)]


def modal_line(u):
    s0, s1, mid, d0, d1 = fold(u)
    out = []
    for k in range(5):
        m = [float(x) for x in MODAL[k]]
        out.append(m[0] * s0 + m[1] * s1 + m[2] * mid if k % 2 == 0 else m[0] * d0 + m[1] * d1)
    return out


def sensor(load, work):
    def first(q, carry):
        for j in range(5):
            pts = points(0, q, j)
            for i, value in zip(pts, modal_line([load(p) for p in pts])):
                work[i] = value
        return carry

    lax.fori_loop(0, 5, first, 0)

    def second(q, carry):
        total, high = carry
        plane = {}
        for c in range(5):
            for b, value in enumerate(modal_line([work[25 * q + 5 * b + c] for b in range(5)])):
                plane[b, c] = value
        low = jnp.zeros_like(total)
        edge = jnp.zeros_like(total)
        for b in range(5):
            line = modal_line([plane[b, c] for c in range(5)])
            squares = [x * x for x in line]
            if b < 4:
                low = low + ((squares[0] + squares[1]) + (squares[2] + squares[3]))
                edge = edge + squares[4]
            else:
                edge = edge + ((squares[0] + squares[1]) + (squares[2] + squares[3])) + squares[4]
        plane_total = low + edge
        return total + plane_total, high + jnp.where(q == 4, plane_total, edge)

    zero = jnp.zeros(work.shape[1:], jnp.float32)
    total, high = lax.fori_loop(0, 5, second, (zero, zero))
    level = jnp.log(jnp.maximum(high / (total + ENERGY_EPS), RATIO_FLOOR)) * (1.0 / math.log(10.0))
    ramp = jnp.clip((level - SENSOR_CENTRE) / SENSOR_WIDTH, -1.0, 1.0)
    return EPS_SCALE * 0.5 * (1.0 + jnp.sin(0.5 * math.pi * ramp))


def rolled(value, shift, axis):
    size = value.shape[axis]
    return pltpu.roll(value, shift % size, axis)


LOWER = [float((1.0 - x) / 2.0) for x in NODES]
UPPER = [float((1.0 + x) / 2.0) for x in NODES]


def along_lanes(line):
    lanes = line.shape[1]
    lane = lax.broadcasted_iota(jnp.int32, line.shape, 1)
    before = jnp.where(lane == 0, 0.0, rolled(line, 1, 1))
    after = jnp.where(lane == lanes - 1, 0.0, rolled(line, -1, 1))
    return jnp.maximum(line, before), jnp.maximum(line, after)


def interpolate(neighbours, nu):
    corner = {}
    for x in range(2):
        for y in range(2):
            line = jnp.maximum(
                jnp.maximum(neighbours[x][y], neighbours[x + 1][y]),
                jnp.maximum(neighbours[x][y + 1], neighbours[x + 1][y + 1]),
            )
            corner[x, y, 0], corner[x, y, 1] = along_lanes(line)
    lower, upper = LOWER, UPPER
    for a in range(5):
        face = {
            (y, z): lower[a] * corner[0, y, z] + upper[a] * corner[1, y, z]
            for y in range(2)
            for z in range(2)
        }
        for b in range(5):
            edge = [lower[b] * face[0, z] + upper[b] * face[1, z] for z in range(2)]
            for c in range(5):
                nu[25 * a + 5 * b + c] = lower[c] * edge[0] + upper[c] * edge[1]
    return corner


def row_masks(axis, chords, spans, lanes):
    row = lax.broadcasted_iota(jnp.int32, (chords * spans, lanes), 0)
    if axis == 0:
        return row < spans, row >= (chords - 1) * spans
    place = row % spans
    return place == 0, place == spans - 1


def outer_rows(axis, chords, spans, last):
    if axis == 0:
        return pl.ds((chords - 1) * spans if last else 0, spans)
    return pl.ds(spans - 1 if last else 0, chords, spans)


def weights(axis, masks):
    low, high = masks[axis]
    return [
        jnp.where(low, float(HALF_LEFT[i]), jnp.where(high, float(HALF_RIGHT[i]), 0.0))
        for i in range(5)
    ]


def local_kernel(sizes, count, chords, spans, *refs):
    state_hbm = refs[0]
    nu, acc = refs[1:3]
    state, grad, halo, work, faces, lifted, beta, spread, relay = refs[3:12]
    sends = (refs[12:16], refs[16:20])
    lands = (refs[20:24], refs[24:28])
    load_sem, eps_send, eps_recv, send_sem, recv_sem, relay_sem, pass_sem = refs[28:]
    rows, lanes = nu.shape[1:]
    chord_size, span_size = sizes
    me_c, me_s = lax.axis_index("chord"), lax.axis_index("span")
    mesh_id = pl.DeviceIdType.MESH

    def reachable(dx):
        if dx == 0:
            return None
        return me_c + 1 < chord_size if dx == 1 else me_c > 0

    def guarded(cond, run):
        if cond is None:
            run()
        else:
            pl.when(cond)(run)

    def partner(dx, dy):
        return (me_c + dx, lax.rem(me_s + dy + span_size, span_size))

    cut, final = chord_size // 2, chord_size - 1
    ends = ((cut - 1, cut), (cut, cut - 1))
    twin = me_s + 1 - 2 * lax.rem(me_s, 2)
    detoured = lax.rem((me_s + 1) // 2, 2) == 1
    relaying = jnp.logical_not(detoured)
    longer = 2
    ghost_routes = (
        (0, True, 0, longer, 0), (1, True, longer, count, 0), (2, False, longer, count, 0),
    )
    near, shifted_from = (0, True, 0, count, 1), 1
    routes = ((ghost_routes, ghost_routes), ((near,), (near, (0, False, shifted_from, count, 2))))

    def place(k, depth):
        return depth if k == 0 else final - depth

    def mate(twinned):
        return twin if twinned else me_s

    offsets = [(dx, dy) for dx in (0, -1, 1) for dy in (-1, 0, 1) if (dx, dy) != (0, 0)]
    for r in range(chords + 4):
        for q in range(spans + 4):
            halo[r, q] = jnp.zeros((1, lanes), jnp.float32)
    barrier = pltpu.get_barrier_semaphore()
    for dx, dy in offsets:

        def greet(dx=dx, dy=dy):
            pl.semaphore_signal(barrier, inc=1, device_id=partner(dx, dy), device_id_type=mesh_id)

        guarded(reachable(dx), greet)

    extra = 0
    for k, (source, target) in enumerate(ends):
        for depth, twinned in sorted({r[:2] for stage in routes for r in stage[k]}):
            through = place(k, depth)
            sender = detoured if twinned else relaying
            hops = [(target, sender, through, relaying)]
            if twinned or abs(through - source) > 1:
                hops.append((through, relaying, source, sender))
            for here, ready, there, awaiting in hops:

                def greet_relay(there=there, twinned=twinned):
                    pl.semaphore_signal(
                        barrier, inc=1, device_id=(there, mate(twinned)), device_id_type=mesh_id
                    )

                pl.when((me_c == here) & ready)(greet_relay)
                extra += jnp.where((me_c == there) & awaiting, 1, 0)

    def load(v):
        return pltpu.make_async_copy(state_hbm.at[v], state.at[v], load_sem.at[v])

    for v in range(count):
        load(v).start()

    def layer(d, length, inside):
        if d == 0:
            return pl.ds(2, length)
        if inside:
            return pl.ds(length if d == 1 else 2, 2)
        return pl.ds(0 if d == 1 else length + 2, 2)

    def eps_copy(dx, dy):
        slot = 3 * (dx + 1) + dy + 1
        return pltpu.make_async_remote_copy(
            src_ref=halo.at[layer(dx, chords, True), layer(dy, spans, True)],
            dst_ref=halo.at[layer(dx, chords, False), layer(dy, spans, False)],
            send_sem=eps_send.at[slot], recv_sem=eps_recv.at[8 - slot],
            device_id=partner(dx, dy), device_id_type=mesh_id,
        )

    ways = ((1, 0), (-1, 0), (0, 1), (0, -1))

    def message(stage, k, v):
        dx, dy = ways[k]
        return pltpu.make_async_remote_copy(
            src_ref=sends[stage][k].at[v], dst_ref=lands[stage][k].at[v],
            send_sem=send_sem.at[stage, k], recv_sem=recv_sem.at[stage, k, v],
            device_id=partner(dx, dy), device_id_type=mesh_id,
        )

    def sent(stage, k):
        dx, dy = ways[k]
        return pltpu.make_async_remote_copy(
            src_ref=sends[stage][k], dst_ref=lands[stage][k],
            send_sem=send_sem.at[stage, k], recv_sem=recv_sem.at[stage, k, 0],
            device_id=partner(dx, dy), device_id_type=mesh_id,
        )

    def detour(stage, k, v, route):
        return pltpu.make_async_remote_copy(
            src_ref=sends[stage][k].at[v], dst_ref=relay.at[route[4], v],
            send_sem=send_sem.at[stage, k], recv_sem=relay_sem.at[route[4], v],
            device_id=(place(k, route[0]), mate(route[1])), device_id_type=mesh_id,
        )

    def onward(stage, k, v, route):
        return pltpu.make_async_remote_copy(
            src_ref=relay.at[route[4], v], dst_ref=lands[stage][k].at[v],
            send_sem=pass_sem.at[route[4], v], recv_sem=recv_sem.at[stage, k, v],
            device_id=(ends[k][1], mate(route[1])), device_id_type=mesh_id,
        )

    posts = [place(k, route[0]) for k in range(2) for route in ghost_routes]
    on_post = functools.reduce(jnp.logical_or, [me_c == c for c in posts]) & relaying

    def each_relay(stage, variables, run):
        def roles():
            for k in range(2):
                for route in routes[stage][k]:

                    def role(k=k, route=route):
                        for v in variables:
                            if route[2] <= v < route[3]:
                                run(k, v, route)

                    pl.when(me_c == place(k, route[0]))(role)

        pl.when(on_post)(roles)

    def forward(stage, variables):
        def hand_on(k, v, route):
            detour(stage, k, v, route).wait_recv()
            onward(stage, k, v, route).start()

        each_relay(stage, variables, hand_on)

    def forwarded(stage):
        each_relay(
            stage, range(count), lambda k, v, route: onward(stage, k, v, route).wait_send()
        )

    def launch(stage, axis, v):
        for k in (2 * axis, 2 * axis + 1):
            if axis == 1:
                message(stage, k, v).start()
                continue
            at_cut = me_c == ends[k][0]

            def cross(k=k):
                direct = me_c == ends[k][0]
                for route in routes[stage][k]:
                    takes = (detoured if route[1] else relaying) & (v >= route[2]) & (v < route[3])
                    direct = direct & jnp.logical_not(takes)
                    pl.when(takes)(lambda route=route: detour(stage, k, v, route).start())
                pl.when(direct)(lambda: message(stage, k, v).start())

            pl.when(at_cut)(cross)
            pl.when(reachable(ways[k][0]) & jnp.logical_not(at_cut))(
                lambda k=k: message(stage, k, v).start()
            )
        if axis == 0:
            for k in range(2):

                def mirror(k=k):
                    if stage == 0:
                        lands[0][1 - k][v] = jnp.zeros(lands[0][1 - k].shape[1:], jnp.float32)
                    else:
                        lands[1][1 - k][v] = -sends[1][k][v]

                pl.when(jnp.logical_not(reachable(ways[k][0])))(mirror)

    def arrived(stage, axis, v):
        for k in (2 * axis, 2 * axis + 1):
            guarded(reachable(-ways[k][0]), lambda k=k: message(stage, k, v).wait_recv())

    masks = [row_masks(axis, chords, spans, lanes) for axis in range(2)]
    outer = [[outer_rows(axis, chords, spans, last) for last in (False, True)] for axis in range(2)]

    def extract(stage, axis, v, f, ref, index):
        up, down = sends[stage][2 * axis], sends[stage][2 * axis + 1]
        down[v, f] = ref[index + (outer[axis][0],)]
        up[v, f] = ref[index[:-1] + (index[-1] + 1, outer[axis][1])]

    def gather(stage, axis, v, f, ref):
        up, down = lands[stage][2 * axis], lands[stage][2 * axis + 1]
        ref[axis, f, outer[axis][0]] = up[v, f]
        ref[axis, f, outer[axis][1]] = down[v, f]
        return ref[axis, f]

    def send_traces(axis, v):
        def body(q, carry):
            for j in range(5):
                f = 5 * q + j
                left, right = traces(fold([state[v, p] for p in points(axis, q, j)]))
                faces[axis, v, 2 * f] = left
                faces[axis, v, 2 * f + 1] = right
                extract(0, axis, v, f, faces, (axis, v, 2 * f))
            return carry

        lax.fori_loop(0, 5, body, 0)

    load(0).wait()
    eps = sensor(lambda p: state[0, p], work)
    lifted[1, 0] = eps
    for r in range(rows):
        halo[2 + r // spans, 2 + r % spans] = lifted[1, 0, pl.ds(r, 1)]
    send_traces(1, 0)
    send_traces(0, 0)
    sides = jnp.where(me_c > 0, 1, 0) + jnp.where(me_c + 1 < chord_size, 1, 0)
    pl.semaphore_wait(barrier, 2 + 3 * sides + extra)
    for dx, dy in offsets:
        guarded(reachable(dx), lambda dx=dx, dy=dy: eps_copy(dx, dy).start())
    launch(0, 0, 0)
    launch(0, 1, 0)

    def later_traces(v, carry):
        load(v).wait()
        for axis in range(2):
            send_traces(axis, v)
            launch(0, axis, v)
        return carry

    lax.fori_loop(1, count, later_traces, 0)

    lane = lax.broadcasted_iota(jnp.int32, (rows, lanes), 1)
    first, last = lane == 0, lane == lanes - 1

    row = lax.broadcasted_iota(jnp.int32, (rows, lanes), 0)
    closed_low = row < spans - jnp.where(me_c > 0, spans, 0)
    closed_high = row >= jnp.where(me_c + 1 < chord_size, rows, rows - spans)

    def inner(axis, left, right):
        low, high = masks[axis]
        step = spans if axis == 0 else 1
        before = jnp.where(low, 0.0, rolled(right, step, 0))
        return before, jnp.where(high, 0.0, rolled(left, -step, 0))

    def local_gradients(v, carry):
        def body(q, carry):
            for j in range(5):
                f = 5 * q + j
                for axis in range(3):
                    pts = points(axis, q, j)
                    parts = fold([state[v, p] for p in pts])
                    if axis == 2:
                        left, right = traces(parts)
                        before = jnp.where(first, left, rolled(right, 1, 1))
                        after = jnp.where(last, right, rolled(left, -1, 1))
                    else:
                        left, right = faces[axis, v, 2 * f], faces[axis, v, 2 * f + 1]
                        before, after = inner(axis, left, right)
                    if axis == 0:
                        before = jnp.where(closed_low, left, before)
                        after = jnp.where(closed_high, right, after)
                    for p, value in zip(pts, slope(parts, before, after)):
                        grad[axis, v, p] = value
            return carry

        lax.fori_loop(0, 5, body, 0, unroll=True)
        return carry

    lax.fori_loop(0, count, local_gradients, 0)

    for dx, dy in offsets:
        guarded(reachable(-dx), lambda dx=dx, dy=dy: eps_copy(dx, dy).wait_recv())
    forward(0, range(3))

    def shifted(x, y, slot):
        for r in range(rows):
            lifted[1, slot, pl.ds(r, 1)] = halo[2 + x + r // spans, 2 + y + r % spans]
        return lifted[1, slot]

    near = {(x, y): shifted(x, y, 3 * x + y + 4) for x in (-1, 0, 1) for y in (-1, 0, 1)}
    neighbours = [[near[x, y] for y in (-1, 0, 1)] for x in (-1, 0, 1)]
    corner = interpolate(neighbours, nu)
    def flux(axis, v):
        def body(q, carry):
            for j in range(5):
                f = 5 * q + j
                values = []
                for p in points(axis, q, j):
                    values.append(nu[p] * grad[axis, v, p])
                    grad[axis, v, p] = values[-1]
                left, right = traces(fold(values))
                work[2 * f] = left
                work[2 * f + 1] = right
                extract(1, axis, v, f, work, (2 * f,))
            return carry

        lax.fori_loop(0, 5, body, 0, unroll=True)

    def fluxes(v, carry):
        for axis in range(2):
            flux(axis, v)
            launch(1, axis, v)
        return carry

    lax.fori_loop(0, count, fluxes, 0)
    forward(0, range(3, count))

    near_weight = sum(float(LEFT[i] * HALF_LEFT[i] * (1.0 - NODES[i]) / 2.0) for i in range(5))
    far_weight = sum(float(LEFT[i] * HALF_LEFT[i] * (1.0 + NODES[i]) / 2.0) for i in range(5))
    slot = 9
    for axis in range(2):
        low = masks[axis][0]
        sign = jnp.where(low, -1.0, 1.0)
        lines = []
        for t in (-1, 0, 1):
            beyond = []
            for d in (-2, 2):
                x, y = (d, t) if axis == 0 else (t, d)
                beyond.append(shifted(x, y, slot))
                slot += 1
            close = [near[d, t] if axis == 0 else near[t, d] for d in (-1, 1)]
            lines.append(jnp.maximum(jnp.where(low, *beyond), jnp.where(low, *close)))
        weight = {}
        for t in range(2):
            far = along_lanes(jnp.maximum(lines[t], lines[t + 1]))
            for z in range(2):
                if axis == 0:
                    shared = jnp.where(low, corner[0, t, z], corner[1, t, z])
                else:
                    shared = jnp.where(low, corner[t, 0, z], corner[t, 1, z])
                value = sign * (near_weight * shared + far_weight * far[z])
                if axis == 0:
                    value = jnp.where(closed_low | closed_high, 0.0, value)
                weight[t, z] = value
        for m in range(5):
            edge = [LOWER[m] * weight[0, z] + UPPER[m] * weight[1, z] for z in range(2)]
            for c in range(5):
                beta[axis, 5 * m + c] = LOWER[c] * edge[0] + UPPER[c] * edge[1]
    def normal(v, carry):
        def body(q, carry):
            for j in range(5):
                pts = points(2, q, j)
                parts = fold([nu[p] * grad[2, v, p] for p in pts])
                left, right = traces(parts)
                before = jnp.where(first, -left, rolled(right, 1, 1))
                after = jnp.where(last, -right, rolled(left, -1, 1))
                for p, value in zip(pts, slope(parts, before, after)):
                    acc[v, p] = value
            return carry

        lax.fori_loop(0, 5, body, 0, unroll=True)
        return carry

    lax.fori_loop(0, count, normal, 0)

    lift = [weights(axis, masks) for axis in range(2)]
    for f in range(25):
        lifted[0, f] = jnp.zeros((rows, lanes), jnp.float32)
        for axis in range(2):
            for p, w in zip(points(axis, f // 5, f % 5), lift[axis]):
                spread[axis, p] = nu[p] * w

    def divergence(v, carry):
        for axis in range(2):
            arrived(0, axis, v)

        def body(q, carry):
            for j in range(5):
                f = 5 * q + j
                for axis in range(2):
                    pts = points(axis, q, j)
                    ghost = gather(0, axis, v, f, lifted)
                    parts = fold([grad[axis, v, p] + spread[axis, p] * ghost for p in pts])
                    before, after = inner(axis, *traces(parts))
                    for p, value in zip(pts, slope(parts, before, after)):
                        acc[v, p] += value
            return carry

        lax.fori_loop(0, 5, body, 0, unroll=True)
        pl.when(v == count - 2)(lambda: forward(1, range(count)))
        return carry

    lax.fori_loop(0, count, divergence, 0)

    def correct(v, carry):
        for axis in range(2):
            arrived(1, axis, v)
        for f in range(25):
            for axis in range(2):
                gather(1, axis, v, f, lifted)

        def outer_flux(axis, f):
            own = jnp.where(masks[axis][0], faces[axis, v, 2 * f], faces[axis, v, 2 * f + 1])
            return lifted[axis, f] + beta[axis, f] * own

        for c in range(5):
            across = [outer_flux(0, 5 * b + c) for b in range(5)]
            for a in range(5):
                along = outer_flux(1, 5 * a + c)
                for b in range(5):
                    acc[v, 25 * a + 5 * b + c] += lift[0][a] * across[b] + lift[1][b] * along
        return carry

    lax.fori_loop(0, count, correct, 0)

    for dx, dy in offsets:
        guarded(reachable(dx), lambda dx=dx, dy=dy: eps_copy(dx, dy).wait_send())
    for stage in range(2):
        for k in range(4):
            guarded(reachable(ways[k][0]), lambda stage=stage, k=k: sent(stage, k).wait_send())
        forwarded(stage)


def write_kernel(nu, residual, nu_hbm, residual_hbm, sems):
    copies = [
        pltpu.make_async_copy(residual.at[v], residual_hbm.at[v], sems.at[v])
        for v in range(residual.shape[0])
    ]
    copies.append(pltpu.make_async_copy(nu, nu_hbm, sems.at[residual.shape[0]]))
    for copy in copies:
        copy.start()
    for copy in copies:
        copy.wait()


def shards(state):
    count, npts, chords, spans, lanes = state.shape
    rows = chords * spans
    flat = state.reshape(count, npts, rows, lanes)
    f32 = jnp.float32
    sizes = (lax.axis_size("chord"), lax.axis_size("span"))

    def message(n, k):
        return (n, 25, spans if k < 2 else chords, lanes)

    def full(*shape):
        return jax.ShapeDtypeStruct(shape, f32)

    vmem = pl.BlockSpec(memory_space=pltpu.VMEM)
    nu, residual = pl.pallas_call(
        functools.partial(local_kernel, sizes, count, chords, spans),
        in_specs=[pl.BlockSpec(memory_space=pltpu.HBM)],
        out_specs=[vmem, vmem],
        out_shape=[full(npts, rows, lanes), full(count, npts, rows, lanes)],
        scratch_shapes=[
            pltpu.VMEM(shape, f32)
            for shape in [
                (count, npts, rows, lanes),
                (3, count, npts, rows, lanes),
                (chords + 4, spans + 4, 1, lanes),
                (npts, rows, lanes),
                (2, count, 50, rows, lanes),
                (2, 25, rows, lanes),
                (2, 25, rows, lanes),
                (2, npts, rows, lanes),
                (3, *message(count, 0)),
            ]
            + [message(count, k) for k in range(4)] * 4
        ]
        + [
            pltpu.SemaphoreType.DMA((count,)),
            pltpu.SemaphoreType.DMA((9,)),
            pltpu.SemaphoreType.DMA((9,)),
            pltpu.SemaphoreType.DMA((2, 4)),
            pltpu.SemaphoreType.DMA((2, 4, count)),
            pltpu.SemaphoreType.DMA((3, count)),
            pltpu.SemaphoreType.DMA((3, count)),
        ],
        compiler_params=pltpu.CompilerParams(
            collective_id=0, has_side_effects=True, vmem_limit_bytes=VMEM_BYTES
        ),
    )(flat)
    hbm = pl.BlockSpec(memory_space=pltpu.HBM)
    nu, residual = pl.pallas_call(
        write_kernel,
        in_specs=[vmem, vmem],
        out_specs=[hbm, hbm],
        out_shape=[full(npts, rows, lanes), full(count, npts, rows, lanes)],
        scratch_shapes=[pltpu.SemaphoreType.DMA((count + 1,))],
        compiler_params=pltpu.CompilerParams(vmem_limit_bytes=1_000_000),
    )(nu, residual)
    return residual.reshape(state.shape), nu.reshape(npts, chords, spans, lanes)


def solution(mesh):
    in_specs = (P(None, None, "chord", "span", None),)
    out_specs = (P(None, None, "chord", "span", None), P(None, "chord", "span", None))
    return jax.shard_map(shards, mesh=mesh, in_specs=in_specs, out_specs=out_specs, check_vma=False)
```

```python
import functools
import math

import jax
import jax.numpy as jnp
import numpy as np
from jax import lax
from jax.experimental import pallas as pl
from jax.experimental.pallas import tpu as pltpu
from jax.sharding import PartitionSpec as P

VMEM_BYTES = 52_500_000
EPS_SCALE = 0.01
SENSOR_CENTRE = -3.0
SENSOR_WIDTH = 1.5
RATIO_FLOOR = 1e-06
ENERGY_EPS = 1e-06
GAUSS_NODES = [-0.906179845938664, -0.5384693101056831, 0.0, 0.5384693101056831, 0.906179845938664]
GAUSS_WEIGHTS = [
    0.2369268850561891,
    0.4786286704993665,
    0.5688888888888889,
    0.4786286704993665,
    0.2369268850561891,
]


def legendre_values(points):
    values = [np.ones(points.shape), np.array(points)]
    for order in range(1, 5):
        values.append(
            ((2 * order + 1) * points * values[order] - order * values[order - 1]) / (order + 1)
        )
    return values


def line_tables():
    line_nodes = np.array(GAUSS_NODES)
    quadrature_weights = np.array(GAUSS_WEIGHTS)
    barycentric = np.array(
        [
            1.0 / np.prod([line_nodes[j] - line_nodes[k] for k in range(5) if k != j])
            for j in range(5)
        ]
    )
    derivative = np.zeros((5, 5))
    for i in range(5):
        for j in range(5):
            if i != j:
                derivative[i, j] = barycentric[j] / barycentric[i] / (line_nodes[i] - line_nodes[j])
        derivative[i, i] = -np.sum(derivative[i])
    left_values = np.ones(5)
    right_values = np.ones(5)
    for j in range(5):
        for k in range(5):
            if k != j:
                left_values[j] *= (-1.0 - line_nodes[k]) / (line_nodes[j] - line_nodes[k])
                right_values[j] *= (1.0 - line_nodes[k]) / (line_nodes[j] - line_nodes[k])
    legendre = legendre_values(line_nodes)
    fourth_slope = 7.0 * legendre[3] + 3.0 * legendre[1]
    fifth_slope = 9.0 * legendre[4] + 5.0 * legendre[2] + legendre[0]
    left_corr = 0.5 * (fourth_slope - fifth_slope)
    right_corr = 0.5 * (fourth_slope + fifth_slope)
    modal = np.zeros((5, 5))
    for k in range(5):
        modal[k, :] = quadrature_weights * math.sqrt((2 * k + 1) / 2.0) * legendre[k]
    return (line_nodes, derivative, left_values, right_values, left_corr, right_corr, modal)


NODES, DERIV, LEFT, RIGHT, LIFT_LEFT, LIFT_RIGHT, MODAL = line_tables()
HALF_LEFT = 0.5 * LIFT_LEFT
HALF_RIGHT = 0.5 * LIFT_RIGHT


def fold(u):
    return (u[0] + u[4], u[1] + u[3], u[2], u[0] - u[4], u[1] - u[3])


def traces(parts):
    s0, s1, mid, d0, d1 = parts
    r = [float(x) for x in RIGHT]
    even = 0.5 * (r[0] + r[4]) * s0 + 0.5 * (r[1] + r[3]) * s1 + r[2] * mid
    odd = 0.5 * (r[0] - r[4]) * d0 + 0.5 * (r[1] - r[3]) * d1
    return even - odd, even + odd


def slope(parts, before, after):
    s0, s1, mid, d0, d1 = parts
    h = [float(x) for x in HALF_LEFT]
    r = [float(x) for x in RIGHT]
    if before is not None:
        diff, both = before - after, before + after
    even, odd = [], []
    for i in range(3):
        lift = 0.5 * (h[i] + h[4 - i])
        value = (
            float(0.5 * (DERIV[i, 0] - DERIV[i, 4]) + lift * (r[0] - r[4])) * d0
            + float(0.5 * (DERIV[i, 1] - DERIV[i, 3]) + lift * (r[1] - r[3])) * d1
        )
        even.append(value if before is None else value + lift * diff)
    for i in range(2):
        lift = 0.5 * (h[i] - h[4 - i])
        value = (
            float(0.5 * (DERIV[i, 0] + DERIV[i, 4]) - lift * (r[0] + r[4])) * s0
            + float(0.5 * (DERIV[i, 1] + DERIV[i, 3]) - lift * (r[1] + r[3])) * s1
            + float(DERIV[i, 2] - 2.0 * lift * r[2]) * mid
        )
        odd.append(value if before is None else value + lift * both)
    return [even[0] + odd[0], even[1] + odd[1], even[2], even[1] - odd[1], even[0] - odd[0]]


def points(axis, q, j):
    if axis == 0:
        return [25 * i + 5 * q + j for i in range(5)]
    if axis == 1:
        return [25 * q + 5 * i + j for i in range(5)]
    return [25 * q + 5 * j + i for i in range(5)]


def modal_line(u):
    s0, s1, mid, d0, d1 = fold(u)
    out = []
    for k in range(5):
        m = [float(x) for x in MODAL[k]]
        out.append(m[0] * s0 + m[1] * s1 + m[2] * mid if k % 2 == 0 else m[0] * d0 + m[1] * d1)
    return out


def sensor(load, work):
    def first(q, carry):
        for j in range(5):
            pts = points(0, q, j)
            for i, value in zip(pts, modal_line([load(p) for p in pts])):
                work[i] = value
        return carry

    lax.fori_loop(0, 5, first, 0)

    def second(q, carry):
        total, high = carry
        plane = {}
        for c in range(5):
            for b, value in enumerate(modal_line([work[25 * q + 5 * b + c] for b in range(5)])):
                plane[b, c] = value
        low = jnp.zeros_like(total)
        edge = jnp.zeros_like(total)
        for b in range(5):
            line = modal_line([plane[b, c] for c in range(5)])
            squares = [x * x for x in line]
            if b < 4:
                low = low + ((squares[0] + squares[1]) + (squares[2] + squares[3]))
                edge = edge + squares[4]
            else:
                edge = edge + ((squares[0] + squares[1]) + (squares[2] + squares[3])) + squares[4]
        plane_total = low + edge
        return total + plane_total, high + jnp.where(q == 4, plane_total, edge)

    zero = jnp.zeros(work.shape[1:], jnp.float32)
    total, high = lax.fori_loop(0, 5, second, (zero, zero))
    level = jnp.log(jnp.maximum(high / (total + ENERGY_EPS), RATIO_FLOOR)) * (1.0 / math.log(10.0))
    ramp = jnp.clip((level - SENSOR_CENTRE) / SENSOR_WIDTH, -1.0, 1.0)
    return EPS_SCALE * 0.5 * (1.0 + jnp.sin(0.5 * math.pi * ramp))


def rolled(value, shift, axis):
    size = value.shape[axis]
    return pltpu.roll(value, shift % size, axis)


LOWER = [float((1.0 - x) / 2.0) for x in NODES]
UPPER = [float((1.0 + x) / 2.0) for x in NODES]


def along_lanes(line):
    lanes = line.shape[1]
    lane = lax.broadcasted_iota(jnp.int32, line.shape, 1)
    before = jnp.where(lane == 0, 0.0, rolled(line, 1, 1))
    after = jnp.where(lane == lanes - 1, 0.0, rolled(line, -1, 1))
    return jnp.maximum(line, before), jnp.maximum(line, after)


def interpolate(neighbours, nu):
    corner = {}
    for x in range(2):
        for y in range(2):
            line = jnp.maximum(
                jnp.maximum(neighbours[x][y], neighbours[x + 1][y]),
                jnp.maximum(neighbours[x][y + 1], neighbours[x + 1][y + 1]),
            )
            corner[x, y, 0], corner[x, y, 1] = along_lanes(line)
    lower, upper = LOWER, UPPER
    for a in range(5):
        face = {
            (y, z): lower[a] * corner[0, y, z] + upper[a] * corner[1, y, z]
            for y in range(2)
            for z in range(2)
        }
        for b in range(5):
            edge = [lower[b] * face[0, z] + upper[b] * face[1, z] for z in range(2)]
            for c in range(5):
                nu[25 * a + 5 * b + c] = lower[c] * edge[0] + upper[c] * edge[1]
    return corner


def row_masks(axis, chords, spans, lanes):
    row = lax.broadcasted_iota(jnp.int32, (chords * spans, lanes), 0)
    if axis == 0:
        return row < spans, row >= (chords - 1) * spans
    place = row % spans
    return place == 0, place == spans - 1


def outer_rows(axis, chords, spans, last):
    if axis == 0:
        return pl.ds((chords - 1) * spans if last else 0, spans)
    return pl.ds(spans - 1 if last else 0, chords, spans)


def weights(axis, masks):
    low, high = masks[axis]
    return [
        jnp.where(low, float(HALF_LEFT[i]), jnp.where(high, float(HALF_RIGHT[i]), 0.0))
        for i in range(5)
    ]


def local_kernel(sizes, count, chords, spans, *refs):
    state_hbm = refs[0]
    nu, acc = refs[1:3]
    state, grad, halo, work, faces, lifted, beta, spread, relay = refs[3:12]
    sends = (refs[12:16], refs[16:20])
    lands = (refs[20:24], refs[24:28])
    load_sem, eps_send, eps_recv, send_sem, recv_sem, relay_sem, pass_sem = refs[28:]
    rows, lanes = nu.shape[1:]
    chord_size, span_size = sizes
    me_c, me_s = lax.axis_index("chord"), lax.axis_index("span")
    mesh_id = pl.DeviceIdType.MESH

    def reachable(dx):
        if dx == 0:
            return None
        return me_c + 1 < chord_size if dx == 1 else me_c > 0

    def guarded(cond, run):
        if cond is None:
            run()
        else:
            pl.when(cond)(run)

    def partner(dx, dy):
        return (me_c + dx, lax.rem(me_s + dy + span_size, span_size))

    cut, final = chord_size // 2, chord_size - 1
    ends = ((cut - 1, cut), (cut, cut - 1))
    twin = me_s + 1 - 2 * lax.rem(me_s, 2)
    detoured = lax.rem((me_s + 1) // 2, 2) == 1
    relaying = jnp.logical_not(detoured)
    longer = 2
    ghost_routes = (
        (0, True, 0, longer, 0), (1, True, longer, count, 0), (2, False, longer, count, 0),
    )
    near, shifted_from = (0, True, 0, count, 1), 0
    fore_routes = ((0, True, 0, 1, 0), (1, True, 1, count, 0), (2, False, longer, count, 0))
    routes = ((fore_routes, ghost_routes), ((near,), (near, (0, False, shifted_from, count, 2))))

    def place(k, depth):
        return depth if k == 0 else final - depth

    def mate(twinned):
        return twin if twinned else me_s

    offsets = [(dx, dy) for dx in (0, -1, 1) for dy in (-1, 0, 1) if (dx, dy) != (0, 0)]
    def load(v):
        return pltpu.make_async_copy(state_hbm.at[v], state.at[v], load_sem.at[v])

    load(0).start()
    barrier = pltpu.get_barrier_semaphore()
    for dx, dy in offsets:

        def greet(dx=dx, dy=dy):
            pl.semaphore_signal(barrier, inc=1, device_id=partner(dx, dy), device_id_type=mesh_id)

        guarded(reachable(dx), greet)

    extra = 0
    for k, (source, target) in enumerate(ends):
        for depth, twinned in sorted({r[:2] for stage in routes for r in stage[k]}):
            through = place(k, depth)
            sender = detoured if twinned else relaying
            hops = [(target, sender, through, relaying)]
            if twinned or abs(through - source) > 1:
                hops.append((through, relaying, source, sender))
            for here, ready, there, awaiting in hops:

                def greet_relay(there=there, twinned=twinned):
                    pl.semaphore_signal(
                        barrier, inc=1, device_id=(there, mate(twinned)), device_id_type=mesh_id
                    )

                pl.when((me_c == here) & ready)(greet_relay)
                extra += jnp.where((me_c == there) & awaiting, 1, 0)

    for v in range(1, count):
        load(v).start()

    for dx, rows_out in ((-1, (0, 1)), (1, (chords + 2, chords + 3))):

        def close(rows_out=rows_out):
            for r in rows_out:
                for q in range(spans + 4):
                    halo[r, q] = jnp.zeros((1, lanes), jnp.float32)

        pl.when(jnp.logical_not(reachable(dx)))(close)

    def layer(d, length, inside):
        if d == 0:
            return pl.ds(2, length)
        if inside:
            return pl.ds(length if d == 1 else 2, 2)
        return pl.ds(0 if d == 1 else length + 2, 2)

    def eps_copy(dx, dy):
        slot = 3 * (dx + 1) + dy + 1
        return pltpu.make_async_remote_copy(
            src_ref=halo.at[layer(dx, chords, True), layer(dy, spans, True)],
            dst_ref=halo.at[layer(dx, chords, False), layer(dy, spans, False)],
            send_sem=eps_send.at[slot], recv_sem=eps_recv.at[8 - slot],
            device_id=partner(dx, dy), device_id_type=mesh_id,
        )

    ways = ((1, 0), (-1, 0), (0, 1), (0, -1))

    def message(stage, k, v):
        dx, dy = ways[k]
        return pltpu.make_async_remote_copy(
            src_ref=sends[stage][k].at[v], dst_ref=lands[stage][k].at[v],
            send_sem=send_sem.at[stage, k], recv_sem=recv_sem.at[stage, k, v],
            device_id=partner(dx, dy), device_id_type=mesh_id,
        )

    def sent(stage, k):
        dx, dy = ways[k]
        return pltpu.make_async_remote_copy(
            src_ref=sends[stage][k], dst_ref=lands[stage][k],
            send_sem=send_sem.at[stage, k], recv_sem=recv_sem.at[stage, k, 0],
            device_id=partner(dx, dy), device_id_type=mesh_id,
        )

    def detour(stage, k, v, route):
        return pltpu.make_async_remote_copy(
            src_ref=sends[stage][k].at[v], dst_ref=relay.at[route[4], v],
            send_sem=send_sem.at[stage, k], recv_sem=relay_sem.at[route[4], v],
            device_id=(place(k, route[0]), mate(route[1])), device_id_type=mesh_id,
        )

    def onward(stage, k, v, route):
        return pltpu.make_async_remote_copy(
            src_ref=relay.at[route[4], v], dst_ref=lands[stage][k].at[v],
            send_sem=pass_sem.at[route[4], v], recv_sem=recv_sem.at[stage, k, v],
            device_id=(ends[k][1], mate(route[1])), device_id_type=mesh_id,
        )

    posts = [place(k, route[0]) for k in range(2) for route in ghost_routes]
    on_post = functools.reduce(jnp.logical_or, [me_c == c for c in posts]) & relaying

    def each_relay(stage, variables, run):
        def roles():
            for k in range(2):
                for route in routes[stage][k]:

                    def role(k=k, route=route):
                        for v in variables:
                            if route[2] <= v < route[3]:
                                run(k, v, route)

                    pl.when(me_c == place(k, route[0]))(role)

        pl.when(on_post)(roles)

    def forward(stage, variables):
        def hand_on(k, v, route):
            detour(stage, k, v, route).wait_recv()
            onward(stage, k, v, route).start()

        each_relay(stage, variables, hand_on)

    def forwarded(stage):
        each_relay(
            stage, range(count), lambda k, v, route: onward(stage, k, v, route).wait_send()
        )

    def launch(stage, axis, v):
        for k in (2 * axis, 2 * axis + 1):
            if axis == 1:
                message(stage, k, v).start()
                continue
            at_cut = me_c == ends[k][0]

            def cross(k=k):
                direct = me_c == ends[k][0]
                for route in routes[stage][k]:
                    takes = (detoured if route[1] else relaying) & (v >= route[2]) & (v < route[3])
                    direct = direct & jnp.logical_not(takes)
                    pl.when(takes)(lambda route=route: detour(stage, k, v, route).start())
                pl.when(direct)(lambda: message(stage, k, v).start())

            pl.when(at_cut)(cross)
            pl.when(reachable(ways[k][0]) & jnp.logical_not(at_cut))(
                lambda k=k: message(stage, k, v).start()
            )
        if axis == 0:
            for k in range(2):

                def mirror(k=k):
                    if stage == 0:
                        lands[0][1 - k][v] = jnp.zeros(lands[0][1 - k].shape[1:], jnp.float32)
                    else:
                        lands[1][1 - k][v] = -sends[1][k][v]

                pl.when(jnp.logical_not(reachable(ways[k][0])))(mirror)

    def arrived(stage, axis, v):
        for k in (2 * axis, 2 * axis + 1):
            guarded(reachable(-ways[k][0]), lambda k=k: message(stage, k, v).wait_recv())

    masks = [row_masks(axis, chords, spans, lanes) for axis in range(2)]
    outer = [[outer_rows(axis, chords, spans, last) for last in (False, True)] for axis in range(2)]

    def extract(stage, axis, v, f, ref, index):
        up, down = sends[stage][2 * axis], sends[stage][2 * axis + 1]
        down[v, f] = ref[index + (outer[axis][0],)]
        up[v, f] = ref[index[:-1] + (index[-1] + 1, outer[axis][1])]

    def gather(stage, axis, v, f, ref):
        up, down = lands[stage][2 * axis], lands[stage][2 * axis + 1]
        ref[axis, f, outer[axis][0]] = up[v, f]
        ref[axis, f, outer[axis][1]] = down[v, f]
        return ref[axis, f]

    def send_traces(axis, v):
        def body(q, carry):
            for j in range(5):
                f = 5 * q + j
                left, right = traces(fold([state[v, p] for p in points(axis, q, j)]))
                faces[axis, v, 2 * f] = left
                faces[axis, v, 2 * f + 1] = right
                extract(0, axis, v, f, faces, (axis, v, 2 * f))
            return carry

        lax.fori_loop(0, 5, body, 0)

    load(0).wait()
    eps = sensor(lambda p: state[0, p], work)
    lifted[1, 0] = eps
    for r in range(rows):
        halo[2 + r // spans, 2 + r % spans] = lifted[1, 0, pl.ds(r, 1)]
    send_traces(1, 0)
    send_traces(0, 0)
    sides = jnp.where(me_c > 0, 1, 0) + jnp.where(me_c + 1 < chord_size, 1, 0)
    pl.semaphore_wait(barrier, 2 + 3 * sides + extra)
    for dx, dy in offsets:
        guarded(reachable(dx), lambda dx=dx, dy=dy: eps_copy(dx, dy).start())
    launch(0, 0, 0)
    launch(0, 1, 0)

    def later_traces(v, carry):
        load(v).wait()
        for axis in range(2):
            send_traces(axis, v)
            launch(0, axis, v)
        return carry

    lax.fori_loop(1, count, later_traces, 0)

    lane = lax.broadcasted_iota(jnp.int32, (rows, lanes), 1)
    first, last = lane == 0, lane == lanes - 1

    row = lax.broadcasted_iota(jnp.int32, (rows, lanes), 0)
    closed_low = row < spans - jnp.where(me_c > 0, spans, 0)
    closed_high = row >= jnp.where(me_c + 1 < chord_size, rows, rows - spans)

    def inner(axis, left, right):
        low, high = masks[axis]
        step = spans if axis == 0 else 1
        before = jnp.where(low, 0.0, rolled(right, step, 0))
        return before, jnp.where(high, 0.0, rolled(left, -step, 0))

    def local_gradients(v, carry):
        def body(q, carry):
            for j in range(5):
                f = 5 * q + j
                for axis in range(3):
                    pts = points(axis, q, j)
                    parts = fold([state[v, p] for p in pts])
                    if axis == 2:
                        left, right = traces(parts)
                        before = jnp.where(first, left, rolled(right, 1, 1))
                        after = jnp.where(last, right, rolled(left, -1, 1))
                    else:
                        left, right = faces[axis, v, 2 * f], faces[axis, v, 2 * f + 1]
                        before, after = inner(axis, left, right)
                    if axis == 0:
                        before = jnp.where(closed_low, left, before)
                        after = jnp.where(closed_high, right, after)
                    for p, value in zip(pts, slope(parts, before, after)):
                        grad[axis, v, p] = value
            return carry

        lax.fori_loop(0, 5, body, 0, unroll=True)
        return carry

    lax.fori_loop(0, count, local_gradients, 0)

    for dx, dy in offsets:
        guarded(reachable(-dx), lambda dx=dx, dy=dy: eps_copy(dx, dy).wait_recv())
    forward(0, range(3))

    def shifted(x, y, slot):
        for r in range(rows):
            lifted[1, slot, pl.ds(r, 1)] = halo[2 + x + r // spans, 2 + y + r % spans]
        return lifted[1, slot]

    near = {(x, y): shifted(x, y, 3 * x + y + 4) for x in (-1, 0, 1) for y in (-1, 0, 1)}
    neighbours = [[near[x, y] for y in (-1, 0, 1)] for x in (-1, 0, 1)]
    corner = interpolate(neighbours, nu)
    def flux(axis, v):
        def body(q, carry):
            for j in range(5):
                f = 5 * q + j
                values = []
                for p in points(axis, q, j):
                    values.append(nu[p] * grad[axis, v, p])
                    grad[axis, v, p] = values[-1]
                left, right = traces(fold(values))
                work[2 * f] = left
                work[2 * f + 1] = right
                extract(1, axis, v, f, work, (2 * f,))
            return carry

        lax.fori_loop(0, 5, body, 0, unroll=True)

    def fluxes(v, carry):
        for axis in range(2):
            flux(axis, v)
            launch(1, axis, v)
        return carry

    lax.fori_loop(0, count, fluxes, 0)
    forward(0, range(3, count))

    near_weight = sum(float(LEFT[i] * HALF_LEFT[i] * (1.0 - NODES[i]) / 2.0) for i in range(5))
    far_weight = sum(float(LEFT[i] * HALF_LEFT[i] * (1.0 + NODES[i]) / 2.0) for i in range(5))
    slot = 9
    for axis in range(2):
        low = masks[axis][0]
        sign = jnp.where(low, -1.0, 1.0)
        lines = []
        for t in (-1, 0, 1):
            beyond = []
            for d in (-2, 2):
                x, y = (d, t) if axis == 0 else (t, d)
                beyond.append(shifted(x, y, slot))
                slot += 1
            close = [near[d, t] if axis == 0 else near[t, d] for d in (-1, 1)]
            lines.append(jnp.maximum(jnp.where(low, *beyond), jnp.where(low, *close)))
        weight = {}
        for t in range(2):
            far = along_lanes(jnp.maximum(lines[t], lines[t + 1]))
            for z in range(2):
                if axis == 0:
                    shared = jnp.where(low, corner[0, t, z], corner[1, t, z])
                else:
                    shared = jnp.where(low, corner[t, 0, z], corner[t, 1, z])
                value = sign * (near_weight * shared + far_weight * far[z])
                if axis == 0:
                    value = jnp.where(closed_low | closed_high, 0.0, value)
                weight[t, z] = value
        for m in range(5):
            edge = [LOWER[m] * weight[0, z] + UPPER[m] * weight[1, z] for z in range(2)]
            for c in range(5):
                beta[axis, 5 * m + c] = LOWER[c] * edge[0] + UPPER[c] * edge[1]
    def normal(v, carry):
        def body(q, carry):
            for j in range(5):
                pts = points(2, q, j)
                parts = fold([nu[p] * grad[2, v, p] for p in pts])
                left, right = traces(parts)
                before = jnp.where(first, -left, rolled(right, 1, 1))
                after = jnp.where(last, -right, rolled(left, -1, 1))
                for p, value in zip(pts, slope(parts, before, after)):
                    acc[v, p] = value
            return carry

        lax.fori_loop(0, 5, body, 0, unroll=True)
        return carry

    lax.fori_loop(0, count, normal, 0)

    lift = [weights(axis, masks) for axis in range(2)]
    for f in range(25):
        lifted[0, f] = jnp.zeros((rows, lanes), jnp.float32)
        for axis in range(2):
            for p, w in zip(points(axis, f // 5, f % 5), lift[axis]):
                spread[axis, p] = nu[p] * w

    def divergence(v, carry):
        for axis in range(2):
            arrived(0, axis, v)

        def body(q, carry):
            for j in range(5):
                f = 5 * q + j
                for axis in range(2):
                    pts = points(axis, q, j)
                    ghost = gather(0, axis, v, f, lifted)
                    parts = fold([grad[axis, v, p] + spread[axis, p] * ghost for p in pts])
                    before, after = inner(axis, *traces(parts))
                    for p, value in zip(pts, slope(parts, before, after)):
                        acc[v, p] += value
            return carry

        lax.fori_loop(0, 5, body, 0, unroll=True)
        pl.when(v == count - 2)(lambda: forward(1, range(count)))
        return carry

    lax.fori_loop(0, count, divergence, 0)

    def correct(v, carry):
        for axis in range(2):
            arrived(1, axis, v)
        for f in range(25):
            for axis in range(2):
                gather(1, axis, v, f, lifted)

        def outer_flux(axis, f):
            own = jnp.where(masks[axis][0], faces[axis, v, 2 * f], faces[axis, v, 2 * f + 1])
            return lifted[axis, f] + beta[axis, f] * own

        for c in range(5):
            across = [outer_flux(0, 5 * b + c) for b in range(5)]
            for a in range(5):
                along = outer_flux(1, 5 * a + c)
                for b in range(5):
                    acc[v, 25 * a + 5 * b + c] += lift[0][a] * across[b] + lift[1][b] * along
        return carry

    lax.fori_loop(0, count, correct, 0)

    for dx, dy in offsets:
        guarded(reachable(dx), lambda dx=dx, dy=dy: eps_copy(dx, dy).wait_send())
    for stage in range(2):
        for k in range(4):
            guarded(reachable(ways[k][0]), lambda stage=stage, k=k: sent(stage, k).wait_send())
        forwarded(stage)


def write_kernel(nu, residual, nu_hbm, residual_hbm, sems):
    copies = [
        pltpu.make_async_copy(residual.at[v], residual_hbm.at[v], sems.at[v])
        for v in range(residual.shape[0])
    ]
    copies.append(pltpu.make_async_copy(nu, nu_hbm, sems.at[residual.shape[0]]))
    for copy in copies:
        copy.start()
    for copy in copies:
        copy.wait()


def shards(state):
    count, npts, chords, spans, lanes = state.shape
    rows = chords * spans
    flat = state.reshape(count, npts, rows, lanes)
    f32 = jnp.float32
    sizes = (lax.axis_size("chord"), lax.axis_size("span"))

    def message(n, k):
        return (n, 25, spans if k < 2 else chords, lanes)

    def full(*shape):
        return jax.ShapeDtypeStruct(shape, f32)

    vmem = pl.BlockSpec(memory_space=pltpu.VMEM)
    nu, residual = pl.pallas_call(
        functools.partial(local_kernel, sizes, count, chords, spans),
        in_specs=[pl.BlockSpec(memory_space=pltpu.HBM)],
        out_specs=[vmem, vmem],
        out_shape=[full(npts, rows, lanes), full(count, npts, rows, lanes)],
        scratch_shapes=[
            pltpu.VMEM(shape, f32)
            for shape in [
                (count, npts, rows, lanes),
                (3, count, npts, rows, lanes),
                (chords + 4, spans + 4, 1, lanes),
                (npts, rows, lanes),
                (2, count, 50, rows, lanes),
                (2, 25, rows, lanes),
                (2, 25, rows, lanes),
                (2, npts, rows, lanes),
                (3, *message(count, 0)),
            ]
            + [message(count, k) for k in range(4)] * 4
        ]
        + [
            pltpu.SemaphoreType.DMA((count,)),
            pltpu.SemaphoreType.DMA((9,)),
            pltpu.SemaphoreType.DMA((9,)),
            pltpu.SemaphoreType.DMA((2, 4)),
            pltpu.SemaphoreType.DMA((2, 4, count)),
            pltpu.SemaphoreType.DMA((3, count)),
            pltpu.SemaphoreType.DMA((3, count)),
        ],
        compiler_params=pltpu.CompilerParams(
            collective_id=0, has_side_effects=True, vmem_limit_bytes=VMEM_BYTES
        ),
    )(flat)
    hbm = pl.BlockSpec(memory_space=pltpu.HBM)
    nu, residual = pl.pallas_call(
        write_kernel,
        in_specs=[vmem, vmem],
        out_specs=[hbm, hbm],
        out_shape=[full(npts, rows, lanes), full(count, npts, rows, lanes)],
        scratch_shapes=[pltpu.SemaphoreType.DMA((count + 1,))],
        compiler_params=pltpu.CompilerParams(vmem_limit_bytes=1_000_000),
    )(nu, residual)
    return residual.reshape(state.shape), nu.reshape(npts, chords, spans, lanes)


def solution(mesh):
    in_specs = (P(None, None, "chord", "span", None),)
    out_specs = (P(None, None, "chord", "span", None), P(None, "chord", "span", None))
    return jax.shard_map(shards, mesh=mesh, in_specs=in_specs, out_specs=out_specs, check_vma=False)
```

```python
import functools
import math

import jax
import jax.numpy as jnp
import numpy as np
from jax import lax
from jax.experimental import pallas as pl
from jax.experimental.pallas import tpu as pltpu
from jax.sharding import PartitionSpec as P

VMEM_BYTES = 52_500_000
EPS_SCALE = 0.01
SENSOR_CENTRE = -3.0
SENSOR_WIDTH = 1.5
RATIO_FLOOR = 1e-06
ENERGY_EPS = 1e-06
GAUSS_NODES = [-0.906179845938664, -0.5384693101056831, 0.0, 0.5384693101056831, 0.906179845938664]
GAUSS_WEIGHTS = [
    0.2369268850561891,
    0.4786286704993665,
    0.5688888888888889,
    0.4786286704993665,
    0.2369268850561891,
]


def legendre_values(points):
    values = [np.ones(points.shape), np.array(points)]
    for order in range(1, 5):
        values.append(
            ((2 * order + 1) * points * values[order] - order * values[order - 1]) / (order + 1)
        )
    return values


def line_tables():
    line_nodes = np.array(GAUSS_NODES)
    quadrature_weights = np.array(GAUSS_WEIGHTS)
    barycentric = np.array(
        [
            1.0 / np.prod([line_nodes[j] - line_nodes[k] for k in range(5) if k != j])
            for j in range(5)
        ]
    )
    derivative = np.zeros((5, 5))
    for i in range(5):
        for j in range(5):
            if i != j:
                derivative[i, j] = barycentric[j] / barycentric[i] / (line_nodes[i] - line_nodes[j])
        derivative[i, i] = -np.sum(derivative[i])
    left_values = np.ones(5)
    right_values = np.ones(5)
    for j in range(5):
        for k in range(5):
            if k != j:
                left_values[j] *= (-1.0 - line_nodes[k]) / (line_nodes[j] - line_nodes[k])
                right_values[j] *= (1.0 - line_nodes[k]) / (line_nodes[j] - line_nodes[k])
    legendre = legendre_values(line_nodes)
    fourth_slope = 7.0 * legendre[3] + 3.0 * legendre[1]
    fifth_slope = 9.0 * legendre[4] + 5.0 * legendre[2] + legendre[0]
    left_corr = 0.5 * (fourth_slope - fifth_slope)
    right_corr = 0.5 * (fourth_slope + fifth_slope)
    modal = np.zeros((5, 5))
    for k in range(5):
        modal[k, :] = quadrature_weights * math.sqrt((2 * k + 1) / 2.0) * legendre[k]
    return (line_nodes, derivative, left_values, right_values, left_corr, right_corr, modal)


NODES, DERIV, LEFT, RIGHT, LIFT_LEFT, LIFT_RIGHT, MODAL = line_tables()
HALF_LEFT = 0.5 * LIFT_LEFT
HALF_RIGHT = 0.5 * LIFT_RIGHT


def fold(u):
    return (u[0] + u[4], u[1] + u[3], u[2], u[0] - u[4], u[1] - u[3])


def traces(parts):
    s0, s1, mid, d0, d1 = parts
    r = [float(x) for x in RIGHT]
    even = 0.5 * (r[0] + r[4]) * s0 + 0.5 * (r[1] + r[3]) * s1 + r[2] * mid
    odd = 0.5 * (r[0] - r[4]) * d0 + 0.5 * (r[1] - r[3]) * d1
    return even - odd, even + odd


def slope(parts, before, after):
    s0, s1, mid, d0, d1 = parts
    h = [float(x) for x in HALF_LEFT]
    r = [float(x) for x in RIGHT]
    if before is not None:
        diff, both = before - after, before + after
    even, odd = [], []
    for i in range(3):
        lift = 0.5 * (h[i] + h[4 - i])
        value = (
            float(0.5 * (DERIV[i, 0] - DERIV[i, 4]) + lift * (r[0] - r[4])) * d0
            + float(0.5 * (DERIV[i, 1] - DERIV[i, 3]) + lift * (r[1] - r[3])) * d1
        )
        even.append(value if before is None else value + lift * diff)
    for i in range(2):
        lift = 0.5 * (h[i] - h[4 - i])
        value = (
            float(0.5 * (DERIV[i, 0] + DERIV[i, 4]) - lift * (r[0] + r[4])) * s0
            + float(0.5 * (DERIV[i, 1] + DERIV[i, 3]) - lift * (r[1] + r[3])) * s1
            + float(DERIV[i, 2] - 2.0 * lift * r[2]) * mid
        )
        odd.append(value if before is None else value + lift * both)
    return [even[0] + odd[0], even[1] + odd[1], even[2], even[1] - odd[1], even[0] - odd[0]]


def points(axis, q, j):
    if axis == 0:
        return [25 * i + 5 * q + j for i in range(5)]
    if axis == 1:
        return [25 * q + 5 * i + j for i in range(5)]
    return [25 * q + 5 * j + i for i in range(5)]


def modal_line(u):
    s0, s1, mid, d0, d1 = fold(u)
    out = []
    for k in range(5):
        m = [float(x) for x in MODAL[k]]
        out.append(m[0] * s0 + m[1] * s1 + m[2] * mid if k % 2 == 0 else m[0] * d0 + m[1] * d1)
    return out


def sensor(load, work):
    def first(q, carry):
        for j in range(5):
            pts = points(0, q, j)
            for i, value in zip(pts, modal_line([load(p) for p in pts])):
                work[i] = value
        return carry

    lax.fori_loop(0, 5, first, 0)

    def second(q, carry):
        total, high = carry
        plane = {}
        for c in range(5):
            for b, value in enumerate(modal_line([work[25 * q + 5 * b + c] for b in range(5)])):
                plane[b, c] = value
        low = jnp.zeros_like(total)
        edge = jnp.zeros_like(total)
        for b in range(5):
            line = modal_line([plane[b, c] for c in range(5)])
            squares = [x * x for x in line]
            if b < 4:
                low = low + ((squares[0] + squares[1]) + (squares[2] + squares[3]))
                edge = edge + squares[4]
            else:
                edge = edge + ((squares[0] + squares[1]) + (squares[2] + squares[3])) + squares[4]
        plane_total = low + edge
        return total + plane_total, high + jnp.where(q == 4, plane_total, edge)

    zero = jnp.zeros(work.shape[1:], jnp.float32)
    total, high = lax.fori_loop(0, 5, second, (zero, zero))
    level = jnp.log(jnp.maximum(high / (total + ENERGY_EPS), RATIO_FLOOR)) * (1.0 / math.log(10.0))
    ramp = jnp.clip((level - SENSOR_CENTRE) / SENSOR_WIDTH, -1.0, 1.0)
    return EPS_SCALE * 0.5 * (1.0 + jnp.sin(0.5 * math.pi * ramp))


def rolled(value, shift, axis):
    size = value.shape[axis]
    return pltpu.roll(value, shift % size, axis)


LOWER = [float((1.0 - x) / 2.0) for x in NODES]
UPPER = [float((1.0 + x) / 2.0) for x in NODES]


def along_lanes(line):
    lanes = line.shape[1]
    lane = lax.broadcasted_iota(jnp.int32, line.shape, 1)
    before = jnp.where(lane == 0, 0.0, rolled(line, 1, 1))
    after = jnp.where(lane == lanes - 1, 0.0, rolled(line, -1, 1))
    return jnp.maximum(line, before), jnp.maximum(line, after)


def interpolate(neighbours, nu):
    corner = {}
    for x in range(2):
        for y in range(2):
            line = jnp.maximum(
                jnp.maximum(neighbours[x][y], neighbours[x + 1][y]),
                jnp.maximum(neighbours[x][y + 1], neighbours[x + 1][y + 1]),
            )
            corner[x, y, 0], corner[x, y, 1] = along_lanes(line)
    lower, upper = LOWER, UPPER
    for a in range(5):
        face = {
            (y, z): lower[a] * corner[0, y, z] + upper[a] * corner[1, y, z]
            for y in range(2)
            for z in range(2)
        }
        for b in range(5):
            edge = [lower[b] * face[0, z] + upper[b] * face[1, z] for z in range(2)]
            for c in range(5):
                nu[25 * a + 5 * b + c] = lower[c] * edge[0] + upper[c] * edge[1]
    return corner


def row_masks(axis, chords, spans, lanes):
    row = lax.broadcasted_iota(jnp.int32, (chords * spans, lanes), 0)
    if axis == 0:
        return row < spans, row >= (chords - 1) * spans
    place = row % spans
    return place == 0, place == spans - 1


def outer_rows(axis, chords, spans, last):
    if axis == 0:
        return pl.ds((chords - 1) * spans if last else 0, spans)
    return pl.ds(spans - 1 if last else 0, chords, spans)


def weights(axis, masks):
    low, high = masks[axis]
    return [
        jnp.where(low, float(HALF_LEFT[i]), jnp.where(high, float(HALF_RIGHT[i]), 0.0))
        for i in range(5)
    ]


def local_kernel(sizes, count, chords, spans, *refs):
    state_hbm = refs[0]
    nu, acc = refs[1:3]
    state, grad, halo, work, faces, lifted, beta, spread, relay = refs[3:12]
    sends = (refs[12:16], refs[16:20])
    lands = (refs[20:24], refs[24:28])
    load_sem, eps_send, eps_recv, send_sem, recv_sem, relay_sem, pass_sem = refs[28:]
    rows, lanes = nu.shape[1:]
    chord_size, span_size = sizes
    me_c, me_s = lax.axis_index("chord"), lax.axis_index("span")
    mesh_id = pl.DeviceIdType.MESH

    def reachable(dx):
        if dx == 0:
            return None
        return me_c + 1 < chord_size if dx == 1 else me_c > 0

    def guarded(cond, run):
        if cond is None:
            run()
        else:
            pl.when(cond)(run)

    def partner(dx, dy):
        return (me_c + dx, lax.rem(me_s + dy + span_size, span_size))

    cut, final = chord_size // 2, chord_size - 1
    ends = ((cut - 1, cut), (cut, cut - 1))
    twin = me_s + 1 - 2 * lax.rem(me_s, 2)
    detoured = lax.rem((me_s + 1) // 2, 2) == 1
    relaying = jnp.logical_not(detoured)
    longer = 2
    ghost_routes = (
        (0, True, 0, longer, 0), (1, True, longer, count, 0), (2, False, longer, count, 0),
    )
    near, shifted_from = (0, True, 0, count, 1), 0
    fore_routes = ((0, True, 0, 1, 0), (1, True, 1, count, 0), (2, False, longer, count, 0))
    routes = ((fore_routes, ghost_routes), ((near,), (near, (0, False, shifted_from, count, 2))))

    def place(k, depth):
        return depth if k == 0 else final - depth

    def mate(twinned):
        return twin if twinned else me_s

    offsets = [(dx, dy) for dx in (0, -1, 1) for dy in (-1, 0, 1) if (dx, dy) != (0, 0)]
    def load(v):
        return pltpu.make_async_copy(state_hbm.at[v], state.at[v], load_sem.at[v])

    load(0).start()
    barrier = pltpu.get_barrier_semaphore()
    for dx, dy in offsets:

        def greet(dx=dx, dy=dy):
            pl.semaphore_signal(barrier, inc=1, device_id=partner(dx, dy), device_id_type=mesh_id)

        guarded(reachable(dx), greet)

    extra = 0
    for k, (source, target) in enumerate(ends):
        for depth, twinned in sorted({r[:2] for stage in routes for r in stage[k]}):
            through = place(k, depth)
            sender = detoured if twinned else relaying
            hops = [(target, sender, through, relaying)]
            if twinned or abs(through - source) > 1:
                hops.append((through, relaying, source, sender))
            for here, ready, there, awaiting in hops:

                def greet_relay(there=there, twinned=twinned):
                    pl.semaphore_signal(
                        barrier, inc=1, device_id=(there, mate(twinned)), device_id_type=mesh_id
                    )

                pl.when((me_c == here) & ready)(greet_relay)
                extra += jnp.where((me_c == there) & awaiting, 1, 0)

    for v in range(1, count):
        load(v).start()

    for dx, rows_out in ((-1, (0, 1)), (1, (chords + 2, chords + 3))):

        def close(rows_out=rows_out):
            for r in rows_out:
                for q in range(spans + 4):
                    halo[r, q] = jnp.zeros((1, lanes), jnp.float32)

        pl.when(jnp.logical_not(reachable(dx)))(close)

    def layer(d, length, inside):
        if d == 0:
            return pl.ds(2, length)
        if inside:
            return pl.ds(length if d == 1 else 2, 2)
        return pl.ds(0 if d == 1 else length + 2, 2)

    def eps_copy(dx, dy):
        return pltpu.make_async_remote_copy(
            src_ref=halo.at[layer(dx, chords, True), layer(dy, spans, True)],
            dst_ref=halo.at[layer(dx, chords, False), layer(dy, spans, False)],
            send_sem=eps_send.at[dx + 1], recv_sem=eps_recv.at[1 - dx],
            device_id=partner(dx, dy), device_id_type=mesh_id,
        )

    def eps_group(dx):
        part = halo.at[pl.ds(0, chords), pl.ds(0, 4)] if dx == 0 else halo.at[pl.ds(0, 2)]
        return pltpu.make_async_remote_copy(
            src_ref=part, dst_ref=part, send_sem=eps_send.at[dx + 1], recv_sem=eps_recv.at[dx + 1],
            device_id=partner(dx, 1), device_id_type=mesh_id,
        )

    ways = ((1, 0), (-1, 0), (0, 1), (0, -1))

    def message(stage, k, v):
        dx, dy = ways[k]
        return pltpu.make_async_remote_copy(
            src_ref=sends[stage][k].at[v], dst_ref=lands[stage][k].at[v],
            send_sem=send_sem.at[stage, k], recv_sem=recv_sem.at[stage, k, v],
            device_id=partner(dx, dy), device_id_type=mesh_id,
        )

    def sent(stage, k):
        dx, dy = ways[k]
        return pltpu.make_async_remote_copy(
            src_ref=sends[stage][k], dst_ref=lands[stage][k],
            send_sem=send_sem.at[stage, k], recv_sem=recv_sem.at[stage, k, 0],
            device_id=partner(dx, dy), device_id_type=mesh_id,
        )

    def detour(stage, k, v, route):
        return pltpu.make_async_remote_copy(
            src_ref=sends[stage][k].at[v], dst_ref=relay.at[route[4], v],
            send_sem=send_sem.at[stage, k], recv_sem=relay_sem.at[route[4], v],
            device_id=(place(k, route[0]), mate(route[1])), device_id_type=mesh_id,
        )

    def onward(stage, k, v, route):
        return pltpu.make_async_remote_copy(
            src_ref=relay.at[route[4], v], dst_ref=lands[stage][k].at[v],
            send_sem=pass_sem.at[route[4], v], recv_sem=recv_sem.at[stage, k, v],
            device_id=(ends[k][1], mate(route[1])), device_id_type=mesh_id,
        )

    posts = [place(k, route[0]) for k in range(2) for route in ghost_routes]
    on_post = functools.reduce(jnp.logical_or, [me_c == c for c in posts]) & relaying

    def each_relay(stage, variables, run):
        def roles():
            for k in range(2):
                for route in routes[stage][k]:

                    def role(k=k, route=route):
                        for v in variables:
                            if route[2] <= v < route[3]:
                                run(k, v, route)

                    pl.when(me_c == place(k, route[0]))(role)

        pl.when(on_post)(roles)

    def forward(stage, variables):
        def hand_on(k, v, route):
            detour(stage, k, v, route).wait_recv()
            onward(stage, k, v, route).start()

        each_relay(stage, variables, hand_on)

    def forwarded(stage):
        each_relay(
            stage, range(count), lambda k, v, route: onward(stage, k, v, route).wait_send()
        )

    def launch(stage, axis, v):
        for k in (2 * axis, 2 * axis + 1):
            if axis == 1:
                message(stage, k, v).start()
                continue
            at_cut = me_c == ends[k][0]

            def cross(k=k):
                direct = me_c == ends[k][0]
                for route in routes[stage][k]:
                    takes = (detoured if route[1] else relaying) & (v >= route[2]) & (v < route[3])
                    direct = direct & jnp.logical_not(takes)
                    pl.when(takes)(lambda route=route: detour(stage, k, v, route).start())
                pl.when(direct)(lambda: message(stage, k, v).start())

            pl.when(at_cut)(cross)
            pl.when(reachable(ways[k][0]) & jnp.logical_not(at_cut))(
                lambda k=k: message(stage, k, v).start()
            )
        if axis == 0:
            for k in range(2):

                def mirror(k=k):
                    if stage == 0:
                        lands[0][1 - k][v] = jnp.zeros(lands[0][1 - k].shape[1:], jnp.float32)
                    else:
                        lands[1][1 - k][v] = -sends[1][k][v]

                pl.when(jnp.logical_not(reachable(ways[k][0])))(mirror)

    def arrived(stage, axis, v):
        for k in (2 * axis, 2 * axis + 1):
            guarded(reachable(-ways[k][0]), lambda k=k: message(stage, k, v).wait_recv())

    masks = [row_masks(axis, chords, spans, lanes) for axis in range(2)]
    outer = [[outer_rows(axis, chords, spans, last) for last in (False, True)] for axis in range(2)]

    def extract(stage, axis, v, f, ref, index):
        up, down = sends[stage][2 * axis], sends[stage][2 * axis + 1]
        down[v, f] = ref[index + (outer[axis][0],)]
        up[v, f] = ref[index[:-1] + (index[-1] + 1, outer[axis][1])]

    def gather(stage, axis, v, f, ref):
        up, down = lands[stage][2 * axis], lands[stage][2 * axis + 1]
        ref[axis, f, outer[axis][0]] = up[v, f]
        ref[axis, f, outer[axis][1]] = down[v, f]
        return ref[axis, f]

    def send_traces(axis, v):
        def body(q, carry):
            for j in range(5):
                f = 5 * q + j
                left, right = traces(fold([state[v, p] for p in points(axis, q, j)]))
                faces[axis, v, 2 * f] = left
                faces[axis, v, 2 * f + 1] = right
                extract(0, axis, v, f, faces, (axis, v, 2 * f))
            return carry

        lax.fori_loop(0, 5, body, 0)

    load(0).wait()
    eps = sensor(lambda p: state[0, p], work)
    lifted[1, 0] = eps
    for r in range(rows):
        halo[2 + r // spans, 2 + r % spans] = lifted[1, 0, pl.ds(r, 1)]
    send_traces(1, 0)
    send_traces(0, 0)
    sides = jnp.where(me_c > 0, 1, 0) + jnp.where(me_c + 1 < chord_size, 1, 0)
    pl.semaphore_wait(barrier, 2 + 3 * sides + extra)
    for dx, dy in offsets:
        guarded(reachable(dx), lambda dx=dx, dy=dy: eps_copy(dx, dy).start())
    launch(0, 0, 0)
    launch(0, 1, 0)

    def later_traces(v, carry):
        load(v).wait()
        for axis in range(2):
            send_traces(axis, v)
            launch(0, axis, v)
        return carry

    lax.fori_loop(1, count, later_traces, 0)

    lane = lax.broadcasted_iota(jnp.int32, (rows, lanes), 1)
    first, last = lane == 0, lane == lanes - 1

    row = lax.broadcasted_iota(jnp.int32, (rows, lanes), 0)
    closed_low = row < spans - jnp.where(me_c > 0, spans, 0)
    closed_high = row >= jnp.where(me_c + 1 < chord_size, rows, rows - spans)

    def inner(axis, left, right):
        low, high = masks[axis]
        step = spans if axis == 0 else 1
        before = jnp.where(low, 0.0, rolled(right, step, 0))
        return before, jnp.where(high, 0.0, rolled(left, -step, 0))

    def local_gradients(v, carry):
        def body(q, carry):
            for j in range(5):
                f = 5 * q + j
                for axis in range(3):
                    pts = points(axis, q, j)
                    parts = fold([state[v, p] for p in pts])
                    if axis == 2:
                        left, right = traces(parts)
                        before = jnp.where(first, left, rolled(right, 1, 1))
                        after = jnp.where(last, right, rolled(left, -1, 1))
                    else:
                        left, right = faces[axis, v, 2 * f], faces[axis, v, 2 * f + 1]
                        before, after = inner(axis, left, right)
                    if axis == 0:
                        before = jnp.where(closed_low, left, before)
                        after = jnp.where(closed_high, right, after)
                    for p, value in zip(pts, slope(parts, before, after)):
                        grad[axis, v, p] = value
            return carry

        lax.fori_loop(0, 5, body, 0, unroll=True)
        return carry

    lax.fori_loop(0, count, local_gradients, 0)

    for dx in (0, -1, 1):
        guarded(reachable(dx), lambda dx=dx: eps_group(dx).wait_recv())
    forward(0, range(3))

    def shifted(x, y, slot):
        for r in range(rows):
            lifted[1, slot, pl.ds(r, 1)] = halo[2 + x + r // spans, 2 + y + r % spans]
        return lifted[1, slot]

    near = {(x, y): shifted(x, y, 3 * x + y + 4) for x in (-1, 0, 1) for y in (-1, 0, 1)}
    neighbours = [[near[x, y] for y in (-1, 0, 1)] for x in (-1, 0, 1)]
    corner = interpolate(neighbours, nu)
    def flux(axis, v):
        def body(q, carry):
            for j in range(5):
                f = 5 * q + j
                values = []
                for p in points(axis, q, j):
                    values.append(nu[p] * grad[axis, v, p])
                    grad[axis, v, p] = values[-1]
                left, right = traces(fold(values))
                work[2 * f] = left
                work[2 * f + 1] = right
                extract(1, axis, v, f, work, (2 * f,))
            return carry

        lax.fori_loop(0, 5, body, 0, unroll=True)

    def fluxes(v, carry):
        for axis in range(2):
            flux(axis, v)
            launch(1, axis, v)
        return carry

    lax.fori_loop(0, count, fluxes, 0)
    forward(0, range(3, count))

    near_weight = sum(float(LEFT[i] * HALF_LEFT[i] * (1.0 - NODES[i]) / 2.0) for i in range(5))
    far_weight = sum(float(LEFT[i] * HALF_LEFT[i] * (1.0 + NODES[i]) / 2.0) for i in range(5))
    slot = 9
    for axis in range(2):
        low = masks[axis][0]
        sign = jnp.where(low, -1.0, 1.0)
        lines = []
        for t in (-1, 0, 1):
            beyond = []
            for d in (-2, 2):
                x, y = (d, t) if axis == 0 else (t, d)
                beyond.append(shifted(x, y, slot))
                slot += 1
            close = [near[d, t] if axis == 0 else near[t, d] for d in (-1, 1)]
            lines.append(jnp.maximum(jnp.where(low, *beyond), jnp.where(low, *close)))
        weight = {}
        for t in range(2):
            far = along_lanes(jnp.maximum(lines[t], lines[t + 1]))
            for z in range(2):
                if axis == 0:
                    shared = jnp.where(low, corner[0, t, z], corner[1, t, z])
                else:
                    shared = jnp.where(low, corner[t, 0, z], corner[t, 1, z])
                value = sign * (near_weight * shared + far_weight * far[z])
                if axis == 0:
                    value = jnp.where(closed_low | closed_high, 0.0, value)
                weight[t, z] = value
        for m in range(5):
            edge = [LOWER[m] * weight[0, z] + UPPER[m] * weight[1, z] for z in range(2)]
            for c in range(5):
                beta[axis, 5 * m + c] = LOWER[c] * edge[0] + UPPER[c] * edge[1]
    def normal(v, carry):
        def body(q, carry):
            for j in range(5):
                pts = points(2, q, j)
                parts = fold([nu[p] * grad[2, v, p] for p in pts])
                left, right = traces(parts)
                before = jnp.where(first, -left, rolled(right, 1, 1))
                after = jnp.where(last, -right, rolled(left, -1, 1))
                for p, value in zip(pts, slope(parts, before, after)):
                    acc[v, p] = value
            return carry

        lax.fori_loop(0, 5, body, 0, unroll=True)
        return carry

    lax.fori_loop(0, count, normal, 0)

    lift = [weights(axis, masks) for axis in range(2)]
    for f in range(25):
        lifted[0, f] = jnp.zeros((rows, lanes), jnp.float32)
        for axis in range(2):
            for p, w in zip(points(axis, f // 5, f % 5), lift[axis]):
                spread[axis, p] = nu[p] * w

    for axis in (1, 0):

        def divergence(v, carry):
            arrived(0, axis, v)

            def body(q, carry):
                for j in range(5):
                    f = 5 * q + j
                    pts = points(axis, q, j)
                    ghost = gather(0, axis, v, f, lifted)
                    parts = fold([grad[axis, v, p] + spread[axis, p] * ghost for p in pts])
                    before, after = inner(axis, *traces(parts))
                    for p, value in zip(pts, slope(parts, before, after)):
                        acc[v, p] += value
                return carry

            lax.fori_loop(0, 5, body, 0, unroll=True)
            if axis == 0:
                pl.when(v == count - 3)(lambda: forward(1, range(count)))
            return carry

        lax.fori_loop(0, count, divergence, 0)

    def correct(v, carry):
        for axis in range(2):
            arrived(1, axis, v)
        for f in range(25):
            for axis in range(2):
                gather(1, axis, v, f, lifted)

        def outer_flux(axis, f):
            own = jnp.where(masks[axis][0], faces[axis, v, 2 * f], faces[axis, v, 2 * f + 1])
            return lifted[axis, f] + beta[axis, f] * own

        for c in range(5):
            across = [outer_flux(0, 5 * b + c) for b in range(5)]
            for a in range(5):
                along = outer_flux(1, 5 * a + c)
                for b in range(5):
                    acc[v, 25 * a + 5 * b + c] += lift[0][a] * across[b] + lift[1][b] * along
        return carry

    lax.fori_loop(0, count, correct, 0)

    for dx in (0, -1, 1):
        guarded(reachable(dx), lambda dx=dx: eps_group(dx).wait_send())
    for stage in range(2):
        for k in range(4):
            guarded(reachable(ways[k][0]), lambda stage=stage, k=k: sent(stage, k).wait_send())
        forwarded(stage)


def write_kernel(nu, residual, nu_hbm, residual_hbm, sems):
    copies = [
        pltpu.make_async_copy(residual.at[v], residual_hbm.at[v], sems.at[v])
        for v in range(residual.shape[0])
    ]
    copies.append(pltpu.make_async_copy(nu, nu_hbm, sems.at[residual.shape[0]]))
    for copy in copies:
        copy.start()
    for copy in copies:
        copy.wait()


def shards(state):
    count, npts, chords, spans, lanes = state.shape
    rows = chords * spans
    flat = state.reshape(count, npts, rows, lanes)
    f32 = jnp.float32
    sizes = (lax.axis_size("chord"), lax.axis_size("span"))

    def message(n, k):
        return (n, 25, spans if k < 2 else chords, lanes)

    def full(*shape):
        return jax.ShapeDtypeStruct(shape, f32)

    vmem = pl.BlockSpec(memory_space=pltpu.VMEM)
    nu, residual = pl.pallas_call(
        functools.partial(local_kernel, sizes, count, chords, spans),
        in_specs=[pl.BlockSpec(memory_space=pltpu.HBM)],
        out_specs=[vmem, vmem],
        out_shape=[full(npts, rows, lanes), full(count, npts, rows, lanes)],
        scratch_shapes=[
            pltpu.VMEM(shape, f32)
            for shape in [
                (count, npts, rows, lanes),
                (3, count, npts, rows, lanes),
                (chords + 4, spans + 4, 1, lanes),
                (npts, rows, lanes),
                (2, count, 50, rows, lanes),
                (2, 25, rows, lanes),
                (2, 25, rows, lanes),
                (2, npts, rows, lanes),
                (3, *message(count, 0)),
            ]
            + [message(count, k) for k in range(4)] * 4
        ]
        + [
            pltpu.SemaphoreType.DMA((count,)),
            pltpu.SemaphoreType.DMA((3,)),
            pltpu.SemaphoreType.DMA((3,)),
            pltpu.SemaphoreType.DMA((2, 4)),
            pltpu.SemaphoreType.DMA((2, 4, count)),
            pltpu.SemaphoreType.DMA((3, count)),
            pltpu.SemaphoreType.DMA((3, count)),
        ],
        compiler_params=pltpu.CompilerParams(
            collective_id=0, has_side_effects=True, vmem_limit_bytes=VMEM_BYTES
        ),
    )(flat)
    hbm = pl.BlockSpec(memory_space=pltpu.HBM)
    nu, residual = pl.pallas_call(
        write_kernel,
        in_specs=[vmem, vmem],
        out_specs=[hbm, hbm],
        out_shape=[full(npts, rows, lanes), full(count, npts, rows, lanes)],
        scratch_shapes=[pltpu.SemaphoreType.DMA((count + 1,))],
        compiler_params=pltpu.CompilerParams(vmem_limit_bytes=1_000_000),
    )(nu, residual)
    return residual.reshape(state.shape), nu.reshape(npts, chords, spans, lanes)


def solution(mesh):
    in_specs = (P(None, None, "chord", "span", None),)
    out_specs = (P(None, None, "chord", "span", None), P(None, "chord", "span", None))
    return jax.shard_map(shards, mesh=mesh, in_specs=in_specs, out_specs=out_specs, check_vma=False)
```

```python
import functools
import math

import jax
import jax.numpy as jnp
import numpy as np
from jax import lax
from jax.experimental import pallas as pl
from jax.experimental.pallas import tpu as pltpu
from jax.sharding import PartitionSpec as P

VMEM_BYTES = 52_500_000
EPS_SCALE = 0.01
SENSOR_CENTRE = -3.0
SENSOR_WIDTH = 1.5
RATIO_FLOOR = 1e-06
ENERGY_EPS = 1e-06
GAUSS_NODES = [-0.906179845938664, -0.5384693101056831, 0.0, 0.5384693101056831, 0.906179845938664]
GAUSS_WEIGHTS = [
    0.2369268850561891,
    0.4786286704993665,
    0.5688888888888889,
    0.4786286704993665,
    0.2369268850561891,
]


def legendre_values(points):
    values = [np.ones(points.shape), np.array(points)]
    for order in range(1, 5):
        values.append(
            ((2 * order + 1) * points * values[order] - order * values[order - 1]) / (order + 1)
        )
    return values


def line_tables():
    line_nodes = np.array(GAUSS_NODES)
    quadrature_weights = np.array(GAUSS_WEIGHTS)
    barycentric = np.array(
        [
            1.0 / np.prod([line_nodes[j] - line_nodes[k] for k in range(5) if k != j])
            for j in range(5)
        ]
    )
    derivative = np.zeros((5, 5))
    for i in range(5):
        for j in range(5):
            if i != j:
                derivative[i, j] = barycentric[j] / barycentric[i] / (line_nodes[i] - line_nodes[j])
        derivative[i, i] = -np.sum(derivative[i])
    left_values = np.ones(5)
    right_values = np.ones(5)
    for j in range(5):
        for k in range(5):
            if k != j:
                left_values[j] *= (-1.0 - line_nodes[k]) / (line_nodes[j] - line_nodes[k])
                right_values[j] *= (1.0 - line_nodes[k]) / (line_nodes[j] - line_nodes[k])
    legendre = legendre_values(line_nodes)
    fourth_slope = 7.0 * legendre[3] + 3.0 * legendre[1]
    fifth_slope = 9.0 * legendre[4] + 5.0 * legendre[2] + legendre[0]
    left_corr = 0.5 * (fourth_slope - fifth_slope)
    right_corr = 0.5 * (fourth_slope + fifth_slope)
    modal = np.zeros((5, 5))
    for k in range(5):
        modal[k, :] = quadrature_weights * math.sqrt((2 * k + 1) / 2.0) * legendre[k]
    return (line_nodes, derivative, left_values, right_values, left_corr, right_corr, modal)


NODES, DERIV, LEFT, RIGHT, LIFT_LEFT, LIFT_RIGHT, MODAL = line_tables()
HALF_LEFT = 0.5 * LIFT_LEFT
HALF_RIGHT = 0.5 * LIFT_RIGHT


def fold(u):
    return (u[0] + u[4], u[1] + u[3], u[2], u[0] - u[4], u[1] - u[3])


def traces(parts):
    s0, s1, mid, d0, d1 = parts
    r = [float(x) for x in RIGHT]
    even = 0.5 * (r[0] + r[4]) * s0 + 0.5 * (r[1] + r[3]) * s1 + r[2] * mid
    odd = 0.5 * (r[0] - r[4]) * d0 + 0.5 * (r[1] - r[3]) * d1
    return even - odd, even + odd


def slope(parts, before, after):
    s0, s1, mid, d0, d1 = parts
    h = [float(x) for x in HALF_LEFT]
    r = [float(x) for x in RIGHT]
    if before is not None:
        diff, both = before - after, before + after
    even, odd = [], []
    for i in range(3):
        lift = 0.5 * (h[i] + h[4 - i])
        value = (
            float(0.5 * (DERIV[i, 0] - DERIV[i, 4]) + lift * (r[0] - r[4])) * d0
            + float(0.5 * (DERIV[i, 1] - DERIV[i, 3]) + lift * (r[1] - r[3])) * d1
        )
        even.append(value if before is None else value + lift * diff)
    for i in range(2):
        lift = 0.5 * (h[i] - h[4 - i])
        value = (
            float(0.5 * (DERIV[i, 0] + DERIV[i, 4]) - lift * (r[0] + r[4])) * s0
            + float(0.5 * (DERIV[i, 1] + DERIV[i, 3]) - lift * (r[1] + r[3])) * s1
            + float(DERIV[i, 2] - 2.0 * lift * r[2]) * mid
        )
        odd.append(value if before is None else value + lift * both)
    return [even[0] + odd[0], even[1] + odd[1], even[2], even[1] - odd[1], even[0] - odd[0]]


def points(axis, q, j):
    if axis == 0:
        return [25 * i + 5 * q + j for i in range(5)]
    if axis == 1:
        return [25 * q + 5 * i + j for i in range(5)]
    return [25 * q + 5 * j + i for i in range(5)]


def modal_line(u):
    s0, s1, mid, d0, d1 = fold(u)
    out = []
    for k in range(5):
        m = [float(x) for x in MODAL[k]]
        out.append(m[0] * s0 + m[1] * s1 + m[2] * mid if k % 2 == 0 else m[0] * d0 + m[1] * d1)
    return out


def sensor(load, work):
    def first(q, carry):
        for j in range(5):
            pts = points(0, q, j)
            for i, value in zip(pts, modal_line([load(p) for p in pts])):
                work[i] = value
        return carry

    lax.fori_loop(0, 5, first, 0)

    def second(q, carry):
        total, high = carry
        plane = {}
        for c in range(5):
            for b, value in enumerate(modal_line([work[25 * q + 5 * b + c] for b in range(5)])):
                plane[b, c] = value
        low = jnp.zeros_like(total)
        edge = jnp.zeros_like(total)
        for b in range(5):
            line = modal_line([plane[b, c] for c in range(5)])
            squares = [x * x for x in line]
            if b < 4:
                low = low + ((squares[0] + squares[1]) + (squares[2] + squares[3]))
                edge = edge + squares[4]
            else:
                edge = edge + ((squares[0] + squares[1]) + (squares[2] + squares[3])) + squares[4]
        plane_total = low + edge
        return total + plane_total, high + jnp.where(q == 4, plane_total, edge)

    zero = jnp.zeros(work.shape[1:], jnp.float32)
    total, high = lax.fori_loop(0, 5, second, (zero, zero))
    level = jnp.log(jnp.maximum(high / (total + ENERGY_EPS), RATIO_FLOOR)) * (1.0 / math.log(10.0))
    ramp = jnp.clip((level - SENSOR_CENTRE) / SENSOR_WIDTH, -1.0, 1.0)
    return EPS_SCALE * 0.5 * (1.0 + jnp.sin(0.5 * math.pi * ramp))


def rolled(value, shift, axis):
    size = value.shape[axis]
    return pltpu.roll(value, shift % size, axis)


LOWER = [float((1.0 - x) / 2.0) for x in NODES]
UPPER = [float((1.0 + x) / 2.0) for x in NODES]


def along_lanes(line):
    lanes = line.shape[1]
    lane = lax.broadcasted_iota(jnp.int32, line.shape, 1)
    before = jnp.where(lane == 0, 0.0, rolled(line, 1, 1))
    after = jnp.where(lane == lanes - 1, 0.0, rolled(line, -1, 1))
    return jnp.maximum(line, before), jnp.maximum(line, after)


def interpolate(neighbours, nu):
    corner = {}
    for x in range(2):
        for y in range(2):
            line = jnp.maximum(
                jnp.maximum(neighbours[x][y], neighbours[x + 1][y]),
                jnp.maximum(neighbours[x][y + 1], neighbours[x + 1][y + 1]),
            )
            corner[x, y, 0], corner[x, y, 1] = along_lanes(line)
    lower, upper = LOWER, UPPER
    for a in range(5):
        face = {
            (y, z): lower[a] * corner[0, y, z] + upper[a] * corner[1, y, z]
            for y in range(2)
            for z in range(2)
        }
        for b in range(5):
            edge = [lower[b] * face[0, z] + upper[b] * face[1, z] for z in range(2)]
            for c in range(5):
                nu[25 * a + 5 * b + c] = lower[c] * edge[0] + upper[c] * edge[1]
    return corner


def row_masks(axis, chords, spans, lanes):
    row = lax.broadcasted_iota(jnp.int32, (chords * spans, lanes), 0)
    if axis == 0:
        return row < spans, row >= (chords - 1) * spans
    place = row % spans
    return place == 0, place == spans - 1


def outer_rows(axis, chords, spans, last):
    if axis == 0:
        return pl.ds((chords - 1) * spans if last else 0, spans)
    return pl.ds(spans - 1 if last else 0, chords, spans)


def weights(axis, masks):
    low, high = masks[axis]
    return [
        jnp.where(low, float(HALF_LEFT[i]), jnp.where(high, float(HALF_RIGHT[i]), 0.0))
        for i in range(5)
    ]


def local_kernel(sizes, count, chords, spans, *refs):
    state_hbm = refs[0]
    nu, acc = refs[1:3]
    state, grad, halo, work, faces, lifted, beta, spread, relay = refs[3:12]
    sends = (refs[12:16], refs[16:20])
    lands = (refs[20:24], refs[24:28])
    load_sem, eps_send, eps_recv, send_sem, recv_sem, relay_sem, pass_sem = refs[28:]
    rows, lanes = nu.shape[1:]
    chord_size, span_size = sizes
    me_c, me_s = lax.axis_index("chord"), lax.axis_index("span")
    mesh_id = pl.DeviceIdType.MESH

    def reachable(dx):
        if dx == 0:
            return None
        return me_c + 1 < chord_size if dx == 1 else me_c > 0

    def guarded(cond, run):
        if cond is None:
            run()
        else:
            pl.when(cond)(run)

    def partner(dx, dy):
        return (me_c + dx, lax.rem(me_s + dy + span_size, span_size))

    cut, final = chord_size // 2, chord_size - 1
    ends = ((cut - 1, cut), (cut, cut - 1))
    twin = me_s + 1 - 2 * lax.rem(me_s, 2)
    detoured = lax.rem((me_s + 1) // 2, 2) == 1
    relaying = jnp.logical_not(detoured)
    longer = 2
    ghost_routes = (
        (0, True, 0, longer, 0), (1, True, longer, count, 0), (2, False, longer, count, 0),
    )
    near, shifted_from = (0, True, 0, count, 1), 0
    fore_routes = ((0, True, 0, 1, 0), (1, True, 1, count, 0), (2, False, longer, count, 0))
    routes = ((fore_routes, ghost_routes), ((near,), (near, (0, False, shifted_from, count, 2))))

    def place(k, depth):
        return depth if k == 0 else final - depth

    def mate(twinned):
        return twin if twinned else me_s

    offsets = [(dx, dy) for dx in (0, -1, 1) for dy in (-1, 0, 1) if (dx, dy) != (0, 0)]
    def load(v):
        return pltpu.make_async_copy(state_hbm.at[v], state.at[v], load_sem.at[v])

    load(0).start()
    barrier = pltpu.get_barrier_semaphore()
    for dx, dy in offsets:

        def greet(dx=dx, dy=dy):
            pl.semaphore_signal(barrier, inc=1, device_id=partner(dx, dy), device_id_type=mesh_id)

        guarded(reachable(dx), greet)

    extra = 0
    for k, (source, target) in enumerate(ends):
        for depth, twinned in sorted({r[:2] for stage in routes for r in stage[k]}):
            through = place(k, depth)
            sender = detoured if twinned else relaying
            hops = [(target, sender, through, relaying)]
            if twinned or abs(through - source) > 1:
                hops.append((through, relaying, source, sender))
            for here, ready, there, awaiting in hops:

                def greet_relay(there=there, twinned=twinned):
                    pl.semaphore_signal(
                        barrier, inc=1, device_id=(there, mate(twinned)), device_id_type=mesh_id
                    )

                pl.when((me_c == here) & ready)(greet_relay)
                extra += jnp.where((me_c == there) & awaiting, 1, 0)

    for v in range(1, count):
        load(v).start()

    for dx, rows_out in ((-1, (0, 1)), (1, (chords + 2, chords + 3))):

        def close(rows_out=rows_out):
            for r in rows_out:
                for q in range(spans + 4):
                    halo[r, q] = jnp.zeros((1, lanes), jnp.float32)

        pl.when(jnp.logical_not(reachable(dx)))(close)

    def layer(d, length, inside):
        if d == 0:
            return pl.ds(2, length)
        if inside:
            return pl.ds(length if d == 1 else 2, 2)
        return pl.ds(0 if d == 1 else length + 2, 2)

    def eps_copy(dx, dy):
        return pltpu.make_async_remote_copy(
            src_ref=halo.at[layer(dx, chords, True), layer(dy, spans, True)],
            dst_ref=halo.at[layer(dx, chords, False), layer(dy, spans, False)],
            send_sem=eps_send.at[dx + 1], recv_sem=eps_recv.at[1 - dx],
            device_id=partner(dx, dy), device_id_type=mesh_id,
        )

    def eps_group(dx):
        part = halo.at[pl.ds(0, chords), pl.ds(0, 4)] if dx == 0 else halo.at[pl.ds(0, 2)]
        return pltpu.make_async_remote_copy(
            src_ref=part, dst_ref=part, send_sem=eps_send.at[dx + 1], recv_sem=eps_recv.at[dx + 1],
            device_id=partner(dx, 1), device_id_type=mesh_id,
        )

    ways = ((1, 0), (-1, 0), (0, 1), (0, -1))

    def message(stage, k, v):
        dx, dy = ways[k]
        return pltpu.make_async_remote_copy(
            src_ref=sends[stage][k].at[v], dst_ref=lands[stage][k].at[v],
            send_sem=send_sem.at[stage, k], recv_sem=recv_sem.at[stage, min(k, 2), v],
            device_id=partner(dx, dy), device_id_type=mesh_id,
        )

    def sent(stage, k):
        dx, dy = ways[k]
        return pltpu.make_async_remote_copy(
            src_ref=sends[stage][k], dst_ref=lands[stage][k],
            send_sem=send_sem.at[stage, k], recv_sem=recv_sem.at[stage, k, 0],
            device_id=partner(dx, dy), device_id_type=mesh_id,
        )

    def detour(stage, k, v, route):
        return pltpu.make_async_remote_copy(
            src_ref=sends[stage][k].at[v], dst_ref=relay.at[route[4], v],
            send_sem=send_sem.at[stage, k], recv_sem=relay_sem.at[route[4], v],
            device_id=(place(k, route[0]), mate(route[1])), device_id_type=mesh_id,
        )

    def onward(stage, k, v, route):
        return pltpu.make_async_remote_copy(
            src_ref=relay.at[route[4], v], dst_ref=lands[stage][k].at[v],
            send_sem=pass_sem.at[route[4], v], recv_sem=recv_sem.at[stage, k, v],
            device_id=(ends[k][1], mate(route[1])), device_id_type=mesh_id,
        )

    posts = [place(k, route[0]) for k in range(2) for route in ghost_routes]
    on_post = functools.reduce(jnp.logical_or, [me_c == c for c in posts]) & relaying

    def each_relay(stage, variables, run):
        def roles():
            for k in range(2):
                for route in routes[stage][k]:

                    def role(k=k, route=route):
                        for v in variables:
                            if route[2] <= v < route[3]:
                                run(k, v, route)

                    pl.when(me_c == place(k, route[0]))(role)

        pl.when(on_post)(roles)

    def forward(stage, variables):
        def hand_on(k, v, route):
            detour(stage, k, v, route).wait_recv()
            onward(stage, k, v, route).start()

        each_relay(stage, variables, hand_on)

    def forwarded(stage):
        each_relay(
            stage, range(count), lambda k, v, route: onward(stage, k, v, route).wait_send()
        )

    def launch(stage, axis, v):
        for k in (2 * axis, 2 * axis + 1):
            if axis == 1:
                message(stage, k, v).start()
                continue
            at_cut = me_c == ends[k][0]

            def cross(k=k):
                direct = me_c == ends[k][0]
                for route in routes[stage][k]:
                    takes = (detoured if route[1] else relaying) & (v >= route[2]) & (v < route[3])
                    direct = direct & jnp.logical_not(takes)
                    pl.when(takes)(lambda route=route: detour(stage, k, v, route).start())
                pl.when(direct)(lambda: message(stage, k, v).start())

            pl.when(at_cut)(cross)
            pl.when(reachable(ways[k][0]) & jnp.logical_not(at_cut))(
                lambda k=k: message(stage, k, v).start()
            )
        if axis == 0:
            for k in range(2):

                def mirror(k=k):
                    if stage == 0:
                        lands[0][1 - k][v] = jnp.zeros(lands[0][1 - k].shape[1:], jnp.float32)
                    else:
                        lands[1][1 - k][v] = -sends[1][k][v]

                pl.when(jnp.logical_not(reachable(ways[k][0])))(mirror)

    def arrived(stage, axis, v):
        if axis == 1:
            both = sends[stage][2].at[pl.ds(0, 2)]
            pltpu.make_async_remote_copy(
                src_ref=both, dst_ref=both, send_sem=send_sem.at[stage, 2],
                recv_sem=recv_sem.at[stage, 2, v],
                device_id=partner(0, 1), device_id_type=mesh_id,
            ).wait_recv()
            return
        for k in range(2):
            guarded(reachable(-ways[k][0]), lambda k=k: message(stage, k, v).wait_recv())

    masks = [row_masks(axis, chords, spans, lanes) for axis in range(2)]
    outer = [[outer_rows(axis, chords, spans, last) for last in (False, True)] for axis in range(2)]

    def extract(stage, axis, v, f, ref, index):
        up, down = sends[stage][2 * axis], sends[stage][2 * axis + 1]
        down[v, f] = ref[index + (outer[axis][0],)]
        up[v, f] = ref[index[:-1] + (index[-1] + 1, outer[axis][1])]

    def gather(stage, axis, v, f, ref):
        up, down = lands[stage][2 * axis], lands[stage][2 * axis + 1]
        ref[axis, f, outer[axis][0]] = up[v, f]
        ref[axis, f, outer[axis][1]] = down[v, f]
        return ref[axis, f]

    def send_traces(axis, v):
        def body(q, carry):
            for j in range(5):
                f = 5 * q + j
                left, right = traces(fold([state[v, p] for p in points(axis, q, j)]))
                faces[axis, v, 2 * f] = left
                faces[axis, v, 2 * f + 1] = right
                extract(0, axis, v, f, faces, (axis, v, 2 * f))
            return carry

        lax.fori_loop(0, 5, body, 0)

    load(0).wait()
    eps = sensor(lambda p: state[0, p], work)
    lifted[1, 0] = eps
    for r in range(rows):
        halo[2 + r // spans, 2 + r % spans] = lifted[1, 0, pl.ds(r, 1)]
    send_traces(1, 0)
    send_traces(0, 0)
    sides = jnp.where(me_c > 0, 1, 0) + jnp.where(me_c + 1 < chord_size, 1, 0)
    pl.semaphore_wait(barrier, 2 + 3 * sides + extra)
    for dx, dy in offsets:
        guarded(reachable(dx), lambda dx=dx, dy=dy: eps_copy(dx, dy).start())
    launch(0, 0, 0)
    launch(0, 1, 0)

    def later_traces(v, carry):
        load(v).wait()
        for axis in range(2):
            send_traces(axis, v)
            launch(0, axis, v)
        return carry

    lax.fori_loop(1, count, later_traces, 0)

    lane = lax.broadcasted_iota(jnp.int32, (rows, lanes), 1)
    first, last = lane == 0, lane == lanes - 1

    row = lax.broadcasted_iota(jnp.int32, (rows, lanes), 0)
    closed_low = row < spans - jnp.where(me_c > 0, spans, 0)
    closed_high = row >= jnp.where(me_c + 1 < chord_size, rows, rows - spans)

    def inner(axis, left, right):
        low, high = masks[axis]
        step = spans if axis == 0 else 1
        before = jnp.where(low, 0.0, rolled(right, step, 0))
        return before, jnp.where(high, 0.0, rolled(left, -step, 0))

    def local_gradients(v, carry):
        def body(q, carry):
            for j in range(5):
                f = 5 * q + j
                for axis in range(3):
                    pts = points(axis, q, j)
                    parts = fold([state[v, p] for p in pts])
                    if axis == 2:
                        left, right = traces(parts)
                        before = jnp.where(first, left, rolled(right, 1, 1))
                        after = jnp.where(last, right, rolled(left, -1, 1))
                    else:
                        left, right = faces[axis, v, 2 * f], faces[axis, v, 2 * f + 1]
                        before, after = inner(axis, left, right)
                    if axis == 0:
                        before = jnp.where(closed_low, left, before)
                        after = jnp.where(closed_high, right, after)
                    for p, value in zip(pts, slope(parts, before, after)):
                        grad[axis, v, p] = value
            return carry

        lax.fori_loop(0, 5, body, 0, unroll=True)
        return carry

    lax.fori_loop(0, count, local_gradients, 0)

    for dx in (0, -1, 1):
        guarded(reachable(dx), lambda dx=dx: eps_group(dx).wait_recv())
    forward(0, range(3))

    def shifted(x, y, slot):
        for r in range(rows):
            lifted[1, slot, pl.ds(r, 1)] = halo[2 + x + r // spans, 2 + y + r % spans]
        return lifted[1, slot]

    near = {(x, y): shifted(x, y, 3 * x + y + 4) for x in (-1, 0, 1) for y in (-1, 0, 1)}
    neighbours = [[near[x, y] for y in (-1, 0, 1)] for x in (-1, 0, 1)]
    corner = interpolate(neighbours, nu)
    def flux(axis, v):
        def body(q, carry):
            for j in range(5):
                f = 5 * q + j
                values = []
                for p in points(axis, q, j):
                    values.append(nu[p] * grad[axis, v, p])
                    grad[axis, v, p] = values[-1]
                left, right = traces(fold(values))
                work[2 * f] = left
                work[2 * f + 1] = right
                extract(1, axis, v, f, work, (2 * f,))
            return carry

        lax.fori_loop(0, 5, body, 0, unroll=True)

    def fluxes(v, carry):
        for axis in (1, 0):
            flux(axis, v)
            launch(1, axis, v)
        return carry

    lax.fori_loop(0, count, fluxes, 0)
    forward(0, range(3, count))

    near_weight = sum(float(LEFT[i] * HALF_LEFT[i] * (1.0 - NODES[i]) / 2.0) for i in range(5))
    far_weight = sum(float(LEFT[i] * HALF_LEFT[i] * (1.0 + NODES[i]) / 2.0) for i in range(5))
    slot = 9
    for axis in range(2):
        low = masks[axis][0]
        sign = jnp.where(low, -1.0, 1.0)
        lines = []
        for t in (-1, 0, 1):
            beyond = []
            for d in (-2, 2):
                x, y = (d, t) if axis == 0 else (t, d)
                beyond.append(shifted(x, y, slot))
                slot += 1
            close = [near[d, t] if axis == 0 else near[t, d] for d in (-1, 1)]
            lines.append(jnp.maximum(jnp.where(low, *beyond), jnp.where(low, *close)))
        weight = {}
        for t in range(2):
            far = along_lanes(jnp.maximum(lines[t], lines[t + 1]))
            for z in range(2):
                if axis == 0:
                    shared = jnp.where(low, corner[0, t, z], corner[1, t, z])
                else:
                    shared = jnp.where(low, corner[t, 0, z], corner[t, 1, z])
                value = sign * (near_weight * shared + far_weight * far[z])
                if axis == 0:
                    value = jnp.where(closed_low | closed_high, 0.0, value)
                weight[t, z] = value
        for m in range(5):
            edge = [LOWER[m] * weight[0, z] + UPPER[m] * weight[1, z] for z in range(2)]
            for c in range(5):
                beta[axis, 5 * m + c] = LOWER[c] * edge[0] + UPPER[c] * edge[1]
    def normal(v, carry):
        def body(q, carry):
            for j in range(5):
                pts = points(2, q, j)
                parts = fold([nu[p] * grad[2, v, p] for p in pts])
                left, right = traces(parts)
                before = jnp.where(first, -left, rolled(right, 1, 1))
                after = jnp.where(last, -right, rolled(left, -1, 1))
                for p, value in zip(pts, slope(parts, before, after)):
                    acc[v, p] = value
            return carry

        lax.fori_loop(0, 5, body, 0, unroll=True)
        return carry

    lax.fori_loop(0, count, normal, 0)

    lift = [weights(axis, masks) for axis in range(2)]
    for f in range(25):
        lifted[0, f] = jnp.zeros((rows, lanes), jnp.float32)
        for axis in range(2):
            for p, w in zip(points(axis, f // 5, f % 5), lift[axis]):
                spread[axis, p] = nu[p] * w

    for axis in (1, 0):

        def divergence(v, carry):
            arrived(0, axis, v)

            def body(q, carry):
                for j in range(5):
                    f = 5 * q + j
                    pts = points(axis, q, j)
                    ghost = gather(0, axis, v, f, lifted)
                    parts = fold([grad[axis, v, p] + spread[axis, p] * ghost for p in pts])
                    before, after = inner(axis, *traces(parts))
                    for p, value in zip(pts, slope(parts, before, after)):
                        acc[v, p] += value
                return carry

            lax.fori_loop(0, 5, body, 0, unroll=True)
            if axis == 0:
                pl.when(v == count - 3)(lambda: forward(1, range(count)))
            return carry

        lax.fori_loop(0, count, divergence, 0)

    def correct(v, carry):
        for axis in range(2):
            arrived(1, axis, v)
        for f in range(25):
            for axis in range(2):
                gather(1, axis, v, f, lifted)

        def outer_flux(axis, f):
            own = jnp.where(masks[axis][0], faces[axis, v, 2 * f], faces[axis, v, 2 * f + 1])
            return lifted[axis, f] + beta[axis, f] * own

        for c in range(5):
            across = [outer_flux(0, 5 * b + c) for b in range(5)]
            for a in range(5):
                along = outer_flux(1, 5 * a + c)
                for b in range(5):
                    acc[v, 25 * a + 5 * b + c] += lift[0][a] * across[b] + lift[1][b] * along
        return carry

    lax.fori_loop(0, count, correct, 0)

    for dx in (0, -1, 1):
        guarded(reachable(dx), lambda dx=dx: eps_group(dx).wait_send())
    for stage in range(2):
        for k in range(4):
            guarded(reachable(ways[k][0]), lambda stage=stage, k=k: sent(stage, k).wait_send())
        forwarded(stage)


def write_kernel(nu, residual, nu_hbm, residual_hbm, sems):
    copies = [
        pltpu.make_async_copy(residual.at[v], residual_hbm.at[v], sems.at[v])
        for v in range(residual.shape[0])
    ]
    copies.append(pltpu.make_async_copy(nu, nu_hbm, sems.at[residual.shape[0]]))
    for copy in copies:
        copy.start()
    for copy in copies:
        copy.wait()


def shards(state):
    count, npts, chords, spans, lanes = state.shape
    rows = chords * spans
    flat = state.reshape(count, npts, rows, lanes)
    f32 = jnp.float32
    sizes = (lax.axis_size("chord"), lax.axis_size("span"))

    def message(n, k):
        return (n, 25, spans if k < 2 else chords, lanes)

    def full(*shape):
        return jax.ShapeDtypeStruct(shape, f32)

    vmem = pl.BlockSpec(memory_space=pltpu.VMEM)
    nu, residual = pl.pallas_call(
        functools.partial(local_kernel, sizes, count, chords, spans),
        in_specs=[pl.BlockSpec(memory_space=pltpu.HBM)],
        out_specs=[vmem, vmem],
        out_shape=[full(npts, rows, lanes), full(count, npts, rows, lanes)],
        scratch_shapes=[
            pltpu.VMEM(shape, f32)
            for shape in [
                (count, npts, rows, lanes),
                (3, count, npts, rows, lanes),
                (chords + 4, spans + 4, 1, lanes),
                (npts, rows, lanes),
                (2, count, 50, rows, lanes),
                (2, 25, rows, lanes),
                (2, 25, rows, lanes),
                (2, npts, rows, lanes),
                (3, *message(count, 0)),
            ]
            + [message(count, k) for k in range(4)] * 4
        ]
        + [
            pltpu.SemaphoreType.DMA((count,)),
            pltpu.SemaphoreType.DMA((3,)),
            pltpu.SemaphoreType.DMA((3,)),
            pltpu.SemaphoreType.DMA((2, 4)),
            pltpu.SemaphoreType.DMA((2, 3, count)),
            pltpu.SemaphoreType.DMA((3, count)),
            pltpu.SemaphoreType.DMA((3, count)),
        ],
        compiler_params=pltpu.CompilerParams(
            collective_id=0, has_side_effects=True, vmem_limit_bytes=VMEM_BYTES
        ),
    )(flat)
    hbm = pl.BlockSpec(memory_space=pltpu.HBM)
    nu, residual = pl.pallas_call(
        write_kernel,
        in_specs=[vmem, vmem],
        out_specs=[hbm, hbm],
        out_shape=[full(npts, rows, lanes), full(count, npts, rows, lanes)],
        scratch_shapes=[pltpu.SemaphoreType.DMA((count + 1,))],
        compiler_params=pltpu.CompilerParams(vmem_limit_bytes=1_000_000),
    )(nu, residual)
    return residual.reshape(state.shape), nu.reshape(npts, chords, spans, lanes)


def solution(mesh):
    in_specs = (P(None, None, "chord", "span", None),)
    out_specs = (P(None, None, "chord", "span", None), P(None, "chord", "span", None))
    return jax.shard_map(shards, mesh=mesh, in_specs=in_specs, out_specs=out_specs, check_vma=False)
```

```python
import functools
import math

import jax
import jax.numpy as jnp
import numpy as np
from jax import lax
from jax.experimental import pallas as pl
from jax.experimental.pallas import tpu as pltpu
from jax.sharding import PartitionSpec as P

VMEM_BYTES = 52_500_000
EPS_SCALE = 0.01
SENSOR_CENTRE = -3.0
SENSOR_WIDTH = 1.5
RATIO_FLOOR = 1e-06
ENERGY_EPS = 1e-06
GAUSS_NODES = [-0.906179845938664, -0.5384693101056831, 0.0, 0.5384693101056831, 0.906179845938664]
GAUSS_WEIGHTS = [
    0.2369268850561891,
    0.4786286704993665,
    0.5688888888888889,
    0.4786286704993665,
    0.2369268850561891,
]


def legendre_values(points):
    values = [np.ones(points.shape), np.array(points)]
    for order in range(1, 5):
        values.append(
            ((2 * order + 1) * points * values[order] - order * values[order - 1]) / (order + 1)
        )
    return values


def line_tables():
    line_nodes = np.array(GAUSS_NODES)
    quadrature_weights = np.array(GAUSS_WEIGHTS)
    barycentric = np.array(
        [
            1.0 / np.prod([line_nodes[j] - line_nodes[k] for k in range(5) if k != j])
            for j in range(5)
        ]
    )
    derivative = np.zeros((5, 5))
    for i in range(5):
        for j in range(5):
            if i != j:
                derivative[i, j] = barycentric[j] / barycentric[i] / (line_nodes[i] - line_nodes[j])
        derivative[i, i] = -np.sum(derivative[i])
    left_values = np.ones(5)
    right_values = np.ones(5)
    for j in range(5):
        for k in range(5):
            if k != j:
                left_values[j] *= (-1.0 - line_nodes[k]) / (line_nodes[j] - line_nodes[k])
                right_values[j] *= (1.0 - line_nodes[k]) / (line_nodes[j] - line_nodes[k])
    legendre = legendre_values(line_nodes)
    fourth_slope = 7.0 * legendre[3] + 3.0 * legendre[1]
    fifth_slope = 9.0 * legendre[4] + 5.0 * legendre[2] + legendre[0]
    left_corr = 0.5 * (fourth_slope - fifth_slope)
    right_corr = 0.5 * (fourth_slope + fifth_slope)
    modal = np.zeros((5, 5))
    for k in range(5):
        modal[k, :] = quadrature_weights * math.sqrt((2 * k + 1) / 2.0) * legendre[k]
    return (line_nodes, derivative, left_values, right_values, left_corr, right_corr, modal)


NODES, DERIV, LEFT, RIGHT, LIFT_LEFT, LIFT_RIGHT, MODAL = line_tables()
HALF_LEFT = 0.5 * LIFT_LEFT
HALF_RIGHT = 0.5 * LIFT_RIGHT


def fold(u):
    return (u[0] + u[4], u[1] + u[3], u[2], u[0] - u[4], u[1] - u[3])


def traces(parts):
    s0, s1, mid, d0, d1 = parts
    r = [float(x) for x in RIGHT]
    even = 0.5 * (r[0] + r[4]) * s0 + 0.5 * (r[1] + r[3]) * s1 + r[2] * mid
    odd = 0.5 * (r[0] - r[4]) * d0 + 0.5 * (r[1] - r[3]) * d1
    return even - odd, even + odd


def slope(parts, before, after):
    s0, s1, mid, d0, d1 = parts
    h = [float(x) for x in HALF_LEFT]
    r = [float(x) for x in RIGHT]
    if before is not None:
        diff, both = before - after, before + after
    even, odd = [], []
    for i in range(3):
        lift = 0.5 * (h[i] + h[4 - i])
        value = (
            float(0.5 * (DERIV[i, 0] - DERIV[i, 4]) + lift * (r[0] - r[4])) * d0
            + float(0.5 * (DERIV[i, 1] - DERIV[i, 3]) + lift * (r[1] - r[3])) * d1
        )
        even.append(value if before is None else value + lift * diff)
    for i in range(2):
        lift = 0.5 * (h[i] - h[4 - i])
        value = (
            float(0.5 * (DERIV[i, 0] + DERIV[i, 4]) - lift * (r[0] + r[4])) * s0
            + float(0.5 * (DERIV[i, 1] + DERIV[i, 3]) - lift * (r[1] + r[3])) * s1
            + float(DERIV[i, 2] - 2.0 * lift * r[2]) * mid
        )
        odd.append(value if before is None else value + lift * both)
    return [even[0] + odd[0], even[1] + odd[1], even[2], even[1] - odd[1], even[0] - odd[0]]


def points(axis, q, j):
    if axis == 0:
        return [25 * i + 5 * q + j for i in range(5)]
    if axis == 1:
        return [25 * q + 5 * i + j for i in range(5)]
    return [25 * q + 5 * j + i for i in range(5)]


def modal_line(u):
    s0, s1, mid, d0, d1 = fold(u)
    out = []
    for k in range(5):
        m = [float(x) for x in MODAL[k]]
        out.append(m[0] * s0 + m[1] * s1 + m[2] * mid if k % 2 == 0 else m[0] * d0 + m[1] * d1)
    return out


def sensor(load, work):
    def first(q, carry):
        for j in range(5):
            pts = points(0, q, j)
            for i, value in zip(pts, modal_line([load(p) for p in pts])):
                work[i] = value
        return carry

    lax.fori_loop(0, 5, first, 0)

    def second(q, carry):
        total, high = carry
        plane = {}
        for c in range(5):
            for b, value in enumerate(modal_line([work[25 * q + 5 * b + c] for b in range(5)])):
                plane[b, c] = value
        low = jnp.zeros_like(total)
        edge = jnp.zeros_like(total)
        for b in range(5):
            line = modal_line([plane[b, c] for c in range(5)])
            squares = [x * x for x in line]
            if b < 4:
                low = low + ((squares[0] + squares[1]) + (squares[2] + squares[3]))
                edge = edge + squares[4]
            else:
                edge = edge + ((squares[0] + squares[1]) + (squares[2] + squares[3])) + squares[4]
        plane_total = low + edge
        return total + plane_total, high + jnp.where(q == 4, plane_total, edge)

    zero = jnp.zeros(work.shape[1:], jnp.float32)
    total, high = lax.fori_loop(0, 5, second, (zero, zero))
    level = jnp.log(jnp.maximum(high / (total + ENERGY_EPS), RATIO_FLOOR)) * (1.0 / math.log(10.0))
    ramp = jnp.clip((level - SENSOR_CENTRE) / SENSOR_WIDTH, -1.0, 1.0)
    return EPS_SCALE * 0.5 * (1.0 + jnp.sin(0.5 * math.pi * ramp))


def rolled(value, shift, axis):
    size = value.shape[axis]
    return pltpu.roll(value, shift % size, axis)


LOWER = [float((1.0 - x) / 2.0) for x in NODES]
UPPER = [float((1.0 + x) / 2.0) for x in NODES]


def along_lanes(line):
    lanes = line.shape[1]
    lane = lax.broadcasted_iota(jnp.int32, line.shape, 1)
    before = jnp.where(lane == 0, 0.0, rolled(line, 1, 1))
    after = jnp.where(lane == lanes - 1, 0.0, rolled(line, -1, 1))
    return jnp.maximum(line, before), jnp.maximum(line, after)


def interpolate(neighbours, nu):
    corner = {}
    for x in range(2):
        for y in range(2):
            line = jnp.maximum(
                jnp.maximum(neighbours[x][y], neighbours[x + 1][y]),
                jnp.maximum(neighbours[x][y + 1], neighbours[x + 1][y + 1]),
            )
            corner[x, y, 0], corner[x, y, 1] = along_lanes(line)
    lower, upper = LOWER, UPPER
    for a in range(5):
        face = {
            (y, z): lower[a] * corner[0, y, z] + upper[a] * corner[1, y, z]
            for y in range(2)
            for z in range(2)
        }
        for b in range(5):
            edge = [lower[b] * face[0, z] + upper[b] * face[1, z] for z in range(2)]
            for c in range(5):
                nu[25 * a + 5 * b + c] = lower[c] * edge[0] + upper[c] * edge[1]
    return corner


def row_masks(axis, chords, spans, lanes):
    row = lax.broadcasted_iota(jnp.int32, (chords * spans, lanes), 0)
    if axis == 0:
        return row < spans, row >= (chords - 1) * spans
    place = row % spans
    return place == 0, place == spans - 1


def outer_rows(axis, chords, spans, last):
    if axis == 0:
        return pl.ds((chords - 1) * spans if last else 0, spans)
    return pl.ds(spans - 1 if last else 0, chords, spans)


def weights(axis, masks):
    low, high = masks[axis]
    return [
        jnp.where(low, float(HALF_LEFT[i]), jnp.where(high, float(HALF_RIGHT[i]), 0.0))
        for i in range(5)
    ]


def local_kernel(sizes, count, chords, spans, *refs):
    state_hbm = refs[0]
    nu, acc = refs[1:3]
    state, grad, halo, work, faces, lifted, beta, spread, relay = refs[3:12]
    sends = (refs[12:16], refs[16:20])
    lands = (refs[20:24], refs[24:28])
    load_sem, eps_send, eps_recv, send_sem, recv_sem, relay_sem, pass_sem = refs[28:]
    rows, lanes = nu.shape[1:]
    chord_size, span_size = sizes
    me_c, me_s = lax.axis_index("chord"), lax.axis_index("span")
    mesh_id = pl.DeviceIdType.MESH

    def reachable(dx):
        if dx == 0:
            return None
        return me_c + 1 < chord_size if dx == 1 else me_c > 0

    def guarded(cond, run):
        if cond is None:
            run()
        else:
            pl.when(cond)(run)

    def partner(dx, dy):
        return (me_c + dx, lax.rem(me_s + dy + span_size, span_size))

    cut, final = chord_size // 2, chord_size - 1
    ends = ((cut - 1, cut), (cut, cut - 1))
    twin = me_s + 1 - 2 * lax.rem(me_s, 2)
    detoured = lax.rem((me_s + 1) // 2, 2) == 1
    relaying = jnp.logical_not(detoured)
    longer = 2
    ghost_routes = (
        (0, True, 0, longer, 0), (1, True, longer, count, 0), (2, False, longer, count, 0),
    )
    near, shifted_from = (0, True, 0, count, 1), 0
    fore_routes = ((0, True, 0, 1, 0), (1, True, 1, count, 0), (2, False, longer, count, 0))
    routes = ((fore_routes, ghost_routes), ((near,), (near, (0, False, shifted_from, count, 2))))

    def place(k, depth):
        return depth if k == 0 else final - depth

    def mate(twinned):
        return twin if twinned else me_s

    offsets = [(dx, dy) for dx in (0, -1, 1) for dy in (-1, 0, 1) if (dx, dy) != (0, 0)]
    def load(v):
        return pltpu.make_async_copy(state_hbm.at[v], state.at[v], load_sem.at[v])

    load(0).start()
    barrier = pltpu.get_barrier_semaphore()
    for dx, dy in offsets:

        def greet(dx=dx, dy=dy):
            pl.semaphore_signal(barrier, inc=1, device_id=partner(dx, dy), device_id_type=mesh_id)

        guarded(reachable(dx), greet)

    extra = 0
    for k, (source, target) in enumerate(ends):
        for depth, twinned in sorted({r[:2] for stage in routes for r in stage[k]}):
            through = place(k, depth)
            sender = detoured if twinned else relaying
            hops = [(target, sender, through, relaying)]
            if twinned or abs(through - source) > 1:
                hops.append((through, relaying, source, sender))
            for here, ready, there, awaiting in hops:

                def greet_relay(there=there, twinned=twinned):
                    pl.semaphore_signal(
                        barrier, inc=1, device_id=(there, mate(twinned)), device_id_type=mesh_id
                    )

                pl.when((me_c == here) & ready)(greet_relay)
                extra += jnp.where((me_c == there) & awaiting, 1, 0)

    for v in range(1, count):
        load(v).start()

    for dx, rows_out in ((-1, (0, 1)), (1, (chords + 2, chords + 3))):

        def close(rows_out=rows_out):
            for r in rows_out:
                for q in range(spans + 4):
                    halo[r, q] = jnp.zeros((1, lanes), jnp.float32)

        pl.when(jnp.logical_not(reachable(dx)))(close)

    def layer(d, length, inside):
        if d == 0:
            return pl.ds(2, length)
        if inside:
            return pl.ds(length if d == 1 else 2, 2)
        return pl.ds(0 if d == 1 else length + 2, 2)

    def eps_copy(dx, dy):
        return pltpu.make_async_remote_copy(
            src_ref=halo.at[layer(dx, chords, True), layer(dy, spans, True)],
            dst_ref=halo.at[layer(dx, chords, False), layer(dy, spans, False)],
            send_sem=eps_send.at[dx + 1], recv_sem=eps_recv.at[1 - dx],
            device_id=partner(dx, dy), device_id_type=mesh_id,
        )

    def eps_group(dx):
        part = halo.at[pl.ds(0, chords), pl.ds(0, 4)] if dx == 0 else halo.at[pl.ds(0, 2)]
        return pltpu.make_async_remote_copy(
            src_ref=part, dst_ref=part, send_sem=eps_send.at[dx + 1], recv_sem=eps_recv.at[dx + 1],
            device_id=partner(dx, 1), device_id_type=mesh_id,
        )

    ways = ((1, 0), (-1, 0), (0, 1), (0, -1))

    def message(stage, k, v):
        dx, dy = ways[k]
        return pltpu.make_async_remote_copy(
            src_ref=sends[stage][k].at[v], dst_ref=lands[stage][k].at[v],
            send_sem=send_sem.at[stage, k], recv_sem=recv_sem.at[stage, min(k, 2), v],
            device_id=partner(dx, dy), device_id_type=mesh_id,
        )

    def sent(stage, k):
        dx, dy = ways[k]
        return pltpu.make_async_remote_copy(
            src_ref=sends[stage][k], dst_ref=lands[stage][k],
            send_sem=send_sem.at[stage, k], recv_sem=recv_sem.at[stage, k, 0],
            device_id=partner(dx, dy), device_id_type=mesh_id,
        )

    def detour(stage, k, v, route):
        return pltpu.make_async_remote_copy(
            src_ref=sends[stage][k].at[v], dst_ref=relay.at[route[4], v],
            send_sem=send_sem.at[stage, k], recv_sem=relay_sem.at[route[4], v],
            device_id=(place(k, route[0]), mate(route[1])), device_id_type=mesh_id,
        )

    def onward(stage, k, v, route):
        return pltpu.make_async_remote_copy(
            src_ref=relay.at[route[4], v], dst_ref=lands[stage][k].at[v],
            send_sem=pass_sem.at[route[4]], recv_sem=recv_sem.at[stage, k, v],
            device_id=(ends[k][1], mate(route[1])), device_id_type=mesh_id,
        )

    posts = [place(k, route[0]) for k in range(2) for route in ghost_routes]
    on_post = functools.reduce(jnp.logical_or, [me_c == c for c in posts]) & relaying

    def each_relay(stage, variables, run):
        def roles():
            for k in range(2):
                for route in routes[stage][k]:

                    def role(k=k, route=route):
                        for v in variables:
                            if route[2] <= v < route[3]:
                                run(k, v, route)

                    pl.when(me_c == place(k, route[0]))(role)

        pl.when(on_post)(roles)

    def forward(stage, variables):
        def hand_on(k, v, route):
            detour(stage, k, v, route).wait_recv()
            onward(stage, k, v, route).start()

        each_relay(stage, variables, hand_on)

    def forwarded(stage):
        def drained(k, v, route):
            if v == route[2]:
                sent_on = relay.at[route[4], pl.ds(v, route[3] - v)]
                pltpu.make_async_remote_copy(
                    src_ref=sent_on, dst_ref=sent_on, send_sem=pass_sem.at[route[4]],
                    recv_sem=relay_sem.at[route[4], v],
                    device_id=(ends[k][1], mate(route[1])), device_id_type=mesh_id,
                ).wait_send()

        each_relay(stage, range(count), drained)

    def launch(stage, axis, v):
        for k in (2 * axis, 2 * axis + 1):
            if axis == 1:
                message(stage, k, v).start()
                continue
            at_cut = me_c == ends[k][0]

            def cross(k=k):
                direct = me_c == ends[k][0]
                for route in routes[stage][k]:
                    takes = (detoured if route[1] else relaying) & (v >= route[2]) & (v < route[3])
                    direct = direct & jnp.logical_not(takes)
                    pl.when(takes)(lambda route=route: detour(stage, k, v, route).start())
                pl.when(direct)(lambda: message(stage, k, v).start())

            pl.when(at_cut)(cross)
            pl.when(reachable(ways[k][0]) & jnp.logical_not(at_cut))(
                lambda k=k: message(stage, k, v).start()
            )
        if axis == 0:
            for k in range(2):

                def mirror(k=k):
                    if stage == 0:
                        lands[0][1 - k][v] = jnp.zeros(lands[0][1 - k].shape[1:], jnp.float32)
                    else:
                        lands[1][1 - k][v] = -sends[1][k][v]

                pl.when(jnp.logical_not(reachable(ways[k][0])))(mirror)

    def arrived(stage, axis, v):
        if axis == 1:
            both = sends[stage][2].at[pl.ds(0, 2)]
            pltpu.make_async_remote_copy(
                src_ref=both, dst_ref=both, send_sem=send_sem.at[stage, 2],
                recv_sem=recv_sem.at[stage, 2, v],
                device_id=partner(0, 1), device_id_type=mesh_id,
            ).wait_recv()
            return
        for k in range(2):
            guarded(reachable(-ways[k][0]), lambda k=k: message(stage, k, v).wait_recv())

    masks = [row_masks(axis, chords, spans, lanes) for axis in range(2)]
    outer = [[outer_rows(axis, chords, spans, last) for last in (False, True)] for axis in range(2)]

    def extract(stage, axis, v, f, ref, index):
        up, down = sends[stage][2 * axis], sends[stage][2 * axis + 1]
        down[v, f] = ref[index + (outer[axis][0],)]
        up[v, f] = ref[index[:-1] + (index[-1] + 1, outer[axis][1])]

    def gather(stage, axis, v, f, ref):
        up, down = lands[stage][2 * axis], lands[stage][2 * axis + 1]
        ref[axis, f, outer[axis][0]] = up[v, f]
        ref[axis, f, outer[axis][1]] = down[v, f]
        return ref[axis, f]

    def send_traces(axis, v):
        def body(q, carry):
            for j in range(5):
                f = 5 * q + j
                left, right = traces(fold([state[v, p] for p in points(axis, q, j)]))
                faces[axis, v, 2 * f] = left
                faces[axis, v, 2 * f + 1] = right
                extract(0, axis, v, f, faces, (axis, v, 2 * f))
            return carry

        lax.fori_loop(0, 5, body, 0)

    load(0).wait()
    eps = sensor(lambda p: state[0, p], work)
    lifted[1, 0] = eps
    for r in range(rows):
        halo[2 + r // spans, 2 + r % spans] = lifted[1, 0, pl.ds(r, 1)]
    send_traces(1, 0)
    send_traces(0, 0)
    sides = jnp.where(me_c > 0, 1, 0) + jnp.where(me_c + 1 < chord_size, 1, 0)
    pl.semaphore_wait(barrier, 2 + 3 * sides + extra)
    for dx, dy in offsets:
        guarded(reachable(dx), lambda dx=dx, dy=dy: eps_copy(dx, dy).start())
    launch(0, 0, 0)
    launch(0, 1, 0)

    def later_traces(v, carry):
        load(v).wait()
        for axis in range(2):
            send_traces(axis, v)
            launch(0, axis, v)
        return carry

    lax.fori_loop(1, count, later_traces, 0)

    lane = lax.broadcasted_iota(jnp.int32, (rows, lanes), 1)
    first, last = lane == 0, lane == lanes - 1

    row = lax.broadcasted_iota(jnp.int32, (rows, lanes), 0)
    closed_low = row < spans - jnp.where(me_c > 0, spans, 0)
    closed_high = row >= jnp.where(me_c + 1 < chord_size, rows, rows - spans)

    def inner(axis, left, right):
        low, high = masks[axis]
        step = spans if axis == 0 else 1
        before = jnp.where(low, 0.0, rolled(right, step, 0))
        return before, jnp.where(high, 0.0, rolled(left, -step, 0))

    def local_gradients(v, carry):
        def body(q, carry):
            for j in range(5):
                f = 5 * q + j
                for axis in range(3):
                    pts = points(axis, q, j)
                    parts = fold([state[v, p] for p in pts])
                    if axis == 2:
                        left, right = traces(parts)
                        before = jnp.where(first, left, rolled(right, 1, 1))
                        after = jnp.where(last, right, rolled(left, -1, 1))
                    else:
                        left, right = faces[axis, v, 2 * f], faces[axis, v, 2 * f + 1]
                        before, after = inner(axis, left, right)
                    if axis == 0:
                        before = jnp.where(closed_low, left, before)
                        after = jnp.where(closed_high, right, after)
                    for p, value in zip(pts, slope(parts, before, after)):
                        grad[axis, v, p] = value
            return carry

        lax.fori_loop(0, 5, body, 0, unroll=True)
        return carry

    lax.fori_loop(0, count, local_gradients, 0)

    for dx in (0, -1, 1):
        guarded(reachable(dx), lambda dx=dx: eps_group(dx).wait_recv())
    forward(0, range(3))

    def shifted(x, y, slot):
        for r in range(rows):
            lifted[1, slot, pl.ds(r, 1)] = halo[2 + x + r // spans, 2 + y + r % spans]
        return lifted[1, slot]

    near = {(x, y): shifted(x, y, 3 * x + y + 4) for x in (-1, 0, 1) for y in (-1, 0, 1)}
    neighbours = [[near[x, y] for y in (-1, 0, 1)] for x in (-1, 0, 1)]
    corner = interpolate(neighbours, nu)
    def flux(axis, v):
        def body(q, carry):
            for j in range(5):
                f = 5 * q + j
                values = []
                for p in points(axis, q, j):
                    values.append(nu[p] * grad[axis, v, p])
                    grad[axis, v, p] = values[-1]
                left, right = traces(fold(values))
                work[2 * f] = left
                work[2 * f + 1] = right
                extract(1, axis, v, f, work, (2 * f,))
            return carry

        lax.fori_loop(0, 5, body, 0, unroll=True)

    def fluxes(v, carry):
        for axis in (1, 0):
            flux(axis, v)
            launch(1, axis, v)
        return carry

    lax.fori_loop(0, count, fluxes, 0)
    forward(0, range(3, count))

    near_weight = sum(float(LEFT[i] * HALF_LEFT[i] * (1.0 - NODES[i]) / 2.0) for i in range(5))
    far_weight = sum(float(LEFT[i] * HALF_LEFT[i] * (1.0 + NODES[i]) / 2.0) for i in range(5))
    slot = 9
    for axis in range(2):
        low = masks[axis][0]
        sign = jnp.where(low, -1.0, 1.0)
        lines = []
        for t in (-1, 0, 1):
            beyond = []
            for d in (-2, 2):
                x, y = (d, t) if axis == 0 else (t, d)
                beyond.append(shifted(x, y, slot))
                slot += 1
            close = [near[d, t] if axis == 0 else near[t, d] for d in (-1, 1)]
            lines.append(jnp.maximum(jnp.where(low, *beyond), jnp.where(low, *close)))
        weight = {}
        for t in range(2):
            far = along_lanes(jnp.maximum(lines[t], lines[t + 1]))
            for z in range(2):
                if axis == 0:
                    shared = jnp.where(low, corner[0, t, z], corner[1, t, z])
                else:
                    shared = jnp.where(low, corner[t, 0, z], corner[t, 1, z])
                value = sign * (near_weight * shared + far_weight * far[z])
                if axis == 0:
                    value = jnp.where(closed_low | closed_high, 0.0, value)
                weight[t, z] = value
        for m in range(5):
            edge = [LOWER[m] * weight[0, z] + UPPER[m] * weight[1, z] for z in range(2)]
            for c in range(5):
                beta[axis, 5 * m + c] = LOWER[c] * edge[0] + UPPER[c] * edge[1]
    def normal(v, carry):
        def body(q, carry):
            for j in range(5):
                pts = points(2, q, j)
                parts = fold([nu[p] * grad[2, v, p] for p in pts])
                left, right = traces(parts)
                before = jnp.where(first, -left, rolled(right, 1, 1))
                after = jnp.where(last, -right, rolled(left, -1, 1))
                for p, value in zip(pts, slope(parts, before, after)):
                    acc[v, p] = value
            return carry

        lax.fori_loop(0, 5, body, 0, unroll=True)
        return carry

    lax.fori_loop(0, count, normal, 0)

    lift = [weights(axis, masks) for axis in range(2)]
    for f in range(25):
        lifted[0, f] = jnp.zeros((rows, lanes), jnp.float32)
        for axis in range(2):
            for p, w in zip(points(axis, f // 5, f % 5), lift[axis]):
                spread[axis, p] = nu[p] * w

    for axis in (1, 0):

        def divergence(v, carry):
            arrived(0, axis, v)

            def body(q, carry):
                for j in range(5):
                    f = 5 * q + j
                    pts = points(axis, q, j)
                    ghost = gather(0, axis, v, f, lifted)
                    parts = fold([grad[axis, v, p] + spread[axis, p] * ghost for p in pts])
                    before, after = inner(axis, *traces(parts))
                    for p, value in zip(pts, slope(parts, before, after)):
                        acc[v, p] += value
                return carry

            lax.fori_loop(0, 5, body, 0, unroll=True)
            if axis == 0:
                pl.when(v == count - 3)(lambda: forward(1, range(count)))
            return carry

        lax.fori_loop(0, count, divergence, 0)

    def correct(v, carry):
        for axis in range(2):
            arrived(1, axis, v)
        for f in range(25):
            for axis in range(2):
                gather(1, axis, v, f, lifted)

        def outer_flux(axis, f):
            own = jnp.where(masks[axis][0], faces[axis, v, 2 * f], faces[axis, v, 2 * f + 1])
            return lifted[axis, f] + beta[axis, f] * own

        for c in range(5):
            across = [outer_flux(0, 5 * b + c) for b in range(5)]
            for a in range(5):
                along = outer_flux(1, 5 * a + c)
                for b in range(5):
                    acc[v, 25 * a + 5 * b + c] += lift[0][a] * across[b] + lift[1][b] * along
        return carry

    lax.fori_loop(0, count, correct, 0)

    for dx in (0, -1, 1):
        guarded(reachable(dx), lambda dx=dx: eps_group(dx).wait_send())
    for stage in range(2):
        for k in range(4):
            guarded(reachable(ways[k][0]), lambda stage=stage, k=k: sent(stage, k).wait_send())
        forwarded(stage)


def write_kernel(nu, residual, nu_hbm, residual_hbm, sems):
    copies = [
        pltpu.make_async_copy(residual.at[v], residual_hbm.at[v], sems.at[v])
        for v in range(residual.shape[0])
    ]
    copies.append(pltpu.make_async_copy(nu, nu_hbm, sems.at[residual.shape[0]]))
    for copy in copies:
        copy.start()
    for copy in copies:
        copy.wait()


def shards(state):
    count, npts, chords, spans, lanes = state.shape
    rows = chords * spans
    flat = state.reshape(count, npts, rows, lanes)
    f32 = jnp.float32
    sizes = (lax.axis_size("chord"), lax.axis_size("span"))

    def message(n, k):
        return (n, 25, spans if k < 2 else chords, lanes)

    def full(*shape):
        return jax.ShapeDtypeStruct(shape, f32)

    vmem = pl.BlockSpec(memory_space=pltpu.VMEM)
    nu, residual = pl.pallas_call(
        functools.partial(local_kernel, sizes, count, chords, spans),
        in_specs=[pl.BlockSpec(memory_space=pltpu.HBM)],
        out_specs=[vmem, vmem],
        out_shape=[full(npts, rows, lanes), full(count, npts, rows, lanes)],
        scratch_shapes=[
            pltpu.VMEM(shape, f32)
            for shape in [
                (count, npts, rows, lanes),
                (3, count, npts, rows, lanes),
                (chords + 4, spans + 4, 1, lanes),
                (npts, rows, lanes),
                (2, count, 50, rows, lanes),
                (2, 25, rows, lanes),
                (2, 25, rows, lanes),
                (2, npts, rows, lanes),
                (3, *message(count, 0)),
            ]
            + [message(count, k) for k in range(4)] * 4
        ]
        + [
            pltpu.SemaphoreType.DMA((count,)),
            pltpu.SemaphoreType.DMA((3,)),
            pltpu.SemaphoreType.DMA((3,)),
            pltpu.SemaphoreType.DMA((2, 4)),
            pltpu.SemaphoreType.DMA((2, 3, count)),
            pltpu.SemaphoreType.DMA((3, count)),
            pltpu.SemaphoreType.DMA((3,)),
        ],
        compiler_params=pltpu.CompilerParams(
            collective_id=0, has_side_effects=True, vmem_limit_bytes=VMEM_BYTES
        ),
    )(flat)
    hbm = pl.BlockSpec(memory_space=pltpu.HBM)
    nu, residual = pl.pallas_call(
        write_kernel,
        in_specs=[vmem, vmem],
        out_specs=[hbm, hbm],
        out_shape=[full(npts, rows, lanes), full(count, npts, rows, lanes)],
        scratch_shapes=[pltpu.SemaphoreType.DMA((count + 1,))],
        compiler_params=pltpu.CompilerParams(vmem_limit_bytes=1_000_000),
    )(nu, residual)
    return residual.reshape(state.shape), nu.reshape(npts, chords, spans, lanes)


def solution(mesh):
    in_specs = (P(None, None, "chord", "span", None),)
    out_specs = (P(None, None, "chord", "span", None), P(None, "chord", "span", None))
    return jax.shard_map(shards, mesh=mesh, in_specs=in_specs, out_specs=out_specs, check_vma=False)
```
